32 devices in a mesh: fsdp: 8 (over z, x), tensor: 4 (over y, core).
Axes of the slice: x: 2, y: 2, z: 4, core: 2. Of those that a mesh axis runs over, the one named last changes fastest.
Arguments:
- layer_input: bfloat16 [8192, 2048], P('fsdp'), may hold values from -6 to 6
- out_grad: bfloat16 [8192, 2048], P('fsdp'), may hold values from -6 to 6
- segment_ids: int32 [8192], P('fsdp'), may hold values from 0 to 8191, as said below
- query_weight: float32 [2048, 2048], P('fsdp', 'tensor'), may hold values from -0.125 to 0.125
- key_weight: float32 [2048, 1024], P('fsdp', 'tensor'), may hold values from -0.125 to 0.125
- value_matrix: float32 [2048, 1024], P('fsdp', 'tensor'), may hold values from -0.125 to 0.125
- output_weight: float32 [2048, 2048], P('fsdp', 'tensor'), may hold values from -0.5 to 0.5
- gate_up_weight: float32 [2, 2048, 6144], P(None, 'fsdp', 'tensor'), may hold values from -0.125 to 0.125
- down_weight: float32 [2048, 6144], P('fsdp', 'tensor'), may hold values from -0.15625 to 0.15625
- norm_gains: float32 [2, 2048], P(None, 'fsdp'), may hold values from 0.5 to 1.5
- headnorm_gains: float32 [2, 128], P(None, 'fsdp'), may hold values from 0.5 to 1.5
- query_weight_mean: float32 [2048, 2048], P('fsdp', 'tensor'), may hold values from -112 to 112
- key_weight_first_moment: float32 [2048, 1024], P('fsdp', 'tensor'), may hold values from -128 to 128
- value_weight_first_moment: float32 [2048, 1024], P('fsdp', 'tensor'), may hold values from -256 to 256
- output_weight_mean: float32 [2048, 2048], P('fsdp', 'tensor'), may hold values from -24 to 24
- gate_up_weight_mean: float32 [2, 2048, 6144], P(None, 'fsdp', 'tensor'), may hold values from -40 to 40
- down_weight_mean: float32 [2048, 6144], P('fsdp', 'tensor'), may hold values from -32 to 32
- norm_gains_mean: float32 [2, 2048], P(None, 'fsdp'), may hold values from -128 to 128
- headnorm_gains_mean: float32 [2, 128], P(None, 'fsdp'), may hold values from -448 to 448
- query_weight_square: float32 [2048, 2048], P('fsdp', 'tensor'), may hold values from 401.408 to 4014.08
- key_weight_second_moment: float32 [2048, 1024], P('fsdp', 'tensor'), may hold values from 704.512 to 7045.12
- value_weight_second_moment: float32 [2048, 1024], P('fsdp', 'tensor'), may hold values from 1966.08 to 19660.8
- output_weight_square: float32 [2048, 2048], P('fsdp', 'tensor'), may hold values from 19.6608 to 196.608
- gate_up_weight_square: float32 [2, 2048, 6144], P(None, 'fsdp', 'tensor'), may hold values from 58.968 to 589.68
- down_weight_square: float32 [2048, 6144], P('fsdp', 'tensor'), may hold values from 44.2368 to 442.368
- norm_gains_square: float32 [2, 2048], P(None, 'fsdp'), may hold values from 491.52 to 4915.2
- headnorm_gains_square: float32 [2, 128], P(None, 'fsdp'), may hold values from 6422.528 to 64225.28
Outputs:
- layer_output: float32 [8192, 2048], P('fsdp')
- input_grad: float32 [8192, 2048], P('fsdp')
- query_weight_grad: float32 [2048, 2048], P('fsdp', 'tensor')
- key_weight_grad: float32 [2048, 1024], P('fsdp', 'tensor')
- value_weight_grad: float32 [2048, 1024], P('fsdp', 'tensor')
- output_weight_grad: float32 [2048, 2048], P('fsdp', 'tensor')
- gate_up_weight_grad: float32 [2, 2048, 6144], P(None, 'fsdp', 'tensor')
- down_weight_grad: float32 [2048, 6144], P('fsdp', 'tensor')
- norm_gains_grad: float32 [2, 2048], P(None, 'fsdp')
- headnorm_gains_grad: float32 [2, 128], P(None, 'fsdp')
- query_weight_step: float32 [2048, 2048], P('fsdp', 'tensor')
- key_weight_step: float32 [2048, 1024], P('fsdp', 'tensor')
- value_weight_step: float32 [2048, 1024], P('fsdp', 'tensor')
- output_weight_step: float32 [2048, 2048], P('fsdp', 'tensor')
- gate_up_weight_step: float32 [2, 2048, 6144], P(None, 'fsdp', 'tensor')
- down_weight_step: float32 [2048, 6144], P('fsdp', 'tensor')
- norm_gains_step: float32 [2, 2048], P(None, 'fsdp')
- headnorm_gains_step: float32 [2, 128], P(None, 'fsdp')
- query_weight_mean_next: float32 [2048, 2048], P('fsdp', 'tensor')
- key_weight_mean_next: float32 [2048, 1024], P('fsdp', 'tensor')
- value_weight_mean_next: float32 [2048, 1024], P('fsdp', 'tensor')
- output_weight_mean_next: float32 [2048, 2048], P('fsdp', 'tensor')
- gate_up_weight_mean_next: float32 [2, 2048, 6144], P(None, 'fsdp', 'tensor')
- down_weight_mean_next: float32 [2048, 6144], P('fsdp', 'tensor')
- norm_gains_mean_next: float32 [2, 2048], P(None, 'fsdp')
- headnorm_gains_mean_next: float32 [2, 128], P(None, 'fsdp')
- query_weight_square_next: float32 [2048, 2048], P('fsdp', 'tensor')
- key_weight_square_next: float32 [2048, 1024], P('fsdp', 'tensor')
- value_weight_square_next: float32 [2048, 1024], P('fsdp', 'tensor')
- output_weight_square_next: float32 [2048, 2048], P('fsdp', 'tensor')
- gate_up_weight_square_next: float32 [2, 2048, 6144], P(None, 'fsdp', 'tensor')
- down_weight_square_next: float32 [2048, 6144], P('fsdp', 'tensor')
- norm_gains_square_next: float32 [2, 2048], P(None, 'fsdp')
- headnorm_gains_square_next: float32 [2, 128], P(None, 'fsdp')
The draws below stay inside these ranges and needn't reach their ends.
Inputs may be any that keep to these rules, and one draw needn't show every extreme that they name: `segment_ids`: segment ids never fall; the tokens of one segment lie within one aligned block of 1024 tokens; in at least one block a single segment fills all 1024 tokens.
All inputs are finite; a program needn't handle non-finite values.
Results may differ from the reference program's by a relative error of at most 0.015.
The reference program's roundings to bfloat16 on the way count: a program that leaves them out, or rounds other values in their place, can miss the bound.
Values may be sent and summed in bfloat16 or wider, within the bound.
A program may use at most 256 MiB of HBM per device.

```python
import math
import jax
import jax.numpy as jnp
from jax import lax

MODEL_WIDTH = 2048
QUERY_HEADS = 16
KEY_VALUE_HEADS = 8
HEAD_SIZE = 128
FF = 6144
TOK_DEV = 1024
ADAM_STEP = 3
TOKENS = 8192


def draw_segment_ids(key, part):
    shard_count = TOKENS // TOK_DEV
    key_cut = jax.random.fold_in(key, 31)
    key_rate = jax.random.fold_in(key, 32)
    key_long = jax.random.fold_in(key, 33)
    cut_rate = jax.random.randint(key_rate, (shard_count, 1), 1, 9)
    long_shard = jax.random.randint(key_long, (), 0, shard_count)
    shard_index = jnp.arange(shard_count, dtype=jnp.int32)[:, None]
    cut_rate = jnp.where(shard_index == long_shard, 0, cut_rate)
    cut_draw = jax.random.randint(key_cut, (shard_count, TOK_DEV), 0, TOK_DEV)
    cut_marks = (cut_draw < cut_rate).astype(jnp.int32)
    cut_marks = cut_marks.at[:, 0].set(0)
    local_ids = jnp.cumsum(cut_marks, axis=1).astype(jnp.int32)
    last_shift = jnp.where(shard_index == shard_count - 1, TOK_DEV - 1 - local_ids[:, -1:], 0).astype(jnp.int32)
    global_ids = local_ids + shard_index * TOK_DEV + last_shift
    return global_ids.reshape(TOKENS).astype(jnp.int32)


def block_scale(own_key, extent, split, low, high):
    gain, own = 1.0, jax.random.fold_in(own_key, 6)
    for axis_at, shards_of in split:
        heights = jnp.exp(jax.random.uniform(jax.random.fold_in(own, axis_at), (shards_of,), jnp.float32, low / len(split), high / len(split)))
        gain = gain * jnp.repeat(heights, extent[axis_at] // shards_of).reshape([-1 if axis == axis_at else 1 for axis in range(len(extent))])
    return gain


def bell_draw(rng, extent, deviation, limit, shards=(), kind=jnp.bfloat16):
    entries = jax.random.normal(rng, extent, jnp.float32) * deviation
    if len(shards) > 0:
        entries = block_scale(rng, extent, shards, -0.22, 0.18) * entries
    return jnp.clip(entries, min=-limit, max=limit).astype(kind)


def setup_inputs(seed: int = 0) -> dict:
    streams_of = jax.random.split(jax.random.key(seed), 28)
    layer_input = bell_draw(streams_of[0], (TOKENS, MODEL_WIDTH), 1.0, 6.0, ((0, 8),))
    out_grad = bell_draw(streams_of[1], (TOKENS, MODEL_WIDTH), 1.0, 6.0, ((0, 8),))
    segment_ids = draw_segment_ids(jax.random.fold_in(streams_of[27], 71), 0)
    query_weight = bell_draw(streams_of[3], (MODEL_WIDTH, QUERY_HEADS * HEAD_SIZE), MODEL_WIDTH ** -0.5, 0.125, ((0, 8), (1, 4)), jnp.float32)
    key_weight = bell_draw(streams_of[4], (MODEL_WIDTH, KEY_VALUE_HEADS * HEAD_SIZE), MODEL_WIDTH ** -0.5, 0.125, ((0, 8), (1, 4)), jnp.float32)
    value_matrix = bell_draw(streams_of[5], (MODEL_WIDTH, KEY_VALUE_HEADS * HEAD_SIZE), MODEL_WIDTH ** -0.5, 0.125, ((0, 8), (1, 4)), jnp.float32)
    output_weight = bell_draw(streams_of[6], (MODEL_WIDTH, QUERY_HEADS * HEAD_SIZE), (QUERY_HEADS * HEAD_SIZE // 16) ** -0.5, 0.5, ((0, 8), (1, 4)), jnp.float32)
    gate_up_weight = bell_draw(streams_of[7], (2, MODEL_WIDTH, FF), MODEL_WIDTH ** -0.5, 0.125, ((1, 8), (2, 4)), jnp.float32)
    down_weight = bell_draw(streams_of[8], (MODEL_WIDTH, FF), (FF // 4) ** -0.5, 0.15625, ((0, 8), (1, 4)), jnp.float32)
    norm_gains = jnp.clip(1.0 + 0.1 * jax.random.normal(streams_of[9], (2, MODEL_WIDTH), jnp.float32), 0.5, 1.5)
    headnorm_gains = jnp.clip(1.0 + 0.1 * jax.random.normal(streams_of[10], (2, HEAD_SIZE), jnp.float32), 0.5, 1.5)
    query_weight_mean = bell_draw(streams_of[11], (MODEL_WIDTH, QUERY_HEADS * HEAD_SIZE), (0.2 * (MODEL_WIDTH * TOKENS // (QUERY_HEADS * HEAD_SIZE)) ** 0.5), 112.0, ((0, 8), (1, 4)), jnp.float32)
    key_weight_first_moment = bell_draw(streams_of[12], (MODEL_WIDTH, KEY_VALUE_HEADS * HEAD_SIZE), (0.26 * (MODEL_WIDTH * TOKENS // (QUERY_HEADS * HEAD_SIZE)) ** 0.5), 128.0, ((0, 8), (1, 4)), jnp.float32)
    value_weight_first_moment = bell_draw(streams_of[13], (MODEL_WIDTH, KEY_VALUE_HEADS * HEAD_SIZE), (0.44 * (MODEL_WIDTH * TOKENS // (QUERY_HEADS * HEAD_SIZE)) ** 0.5), 256.0, ((0, 8), (1, 4)), jnp.float32)
    output_weight_mean = bell_draw(streams_of[14], (MODEL_WIDTH, QUERY_HEADS * HEAD_SIZE), (0.044 * TOKENS ** 0.5), 24.0, ((0, 8), (1, 4)), jnp.float32)
    gate_up_weight_mean = bell_draw(streams_of[15], (2, MODEL_WIDTH, FF), (0.132 * (TOKENS * MODEL_WIDTH // FF) ** 0.5), 40.0, ((1, 8), (2, 4)), jnp.float32)
    down_weight_mean = bell_draw(streams_of[16], (MODEL_WIDTH, FF), (0.066 * TOKENS ** 0.5), 32.0, ((0, 8), (1, 4)), jnp.float32)
    norm_gains_mean = bell_draw(streams_of[17], (2, MODEL_WIDTH), (0.22 * TOKENS ** 0.5), 128.0, ((1, 8),), jnp.float32)
    headnorm_gains_mean = bell_draw(streams_of[18], (2, HEAD_SIZE), (0.2 * (MODEL_WIDTH * TOKENS // HEAD_SIZE) ** 0.5), 448.0, ((1, 8),), jnp.float32)
    query_weight_square = jnp.clip(jnp.exp(math.log(4014.08) - 2.3025851 * jax.random.uniform(streams_of[19], (MODEL_WIDTH, QUERY_HEADS * HEAD_SIZE), jnp.float32) ** block_scale(streams_of[19], (MODEL_WIDTH, QUERY_HEADS * HEAD_SIZE), ((0, 8), (1, 4)), -0.2, 0.2)), 401.408, 4014.08)
    key_weight_second_moment = jnp.clip(jnp.exp(math.log(7045.12) - 2.3025851 * jax.random.uniform(streams_of[20], (MODEL_WIDTH, KEY_VALUE_HEADS * HEAD_SIZE), jnp.float32) ** block_scale(streams_of[20], (MODEL_WIDTH, KEY_VALUE_HEADS * HEAD_SIZE), ((0, 8), (1, 4)), -0.2, 0.2)), 704.512, 7045.12)
    value_weight_second_moment = jnp.clip(jnp.exp(math.log(19660.8) - 2.3025852 * jax.random.uniform(streams_of[21], (MODEL_WIDTH, KEY_VALUE_HEADS * HEAD_SIZE), jnp.float32) ** block_scale(streams_of[21], (MODEL_WIDTH, KEY_VALUE_HEADS * HEAD_SIZE), ((0, 8), (1, 4)), -0.2, 0.2)), 1966.08, 19660.8)
    output_weight_square = jnp.clip(jnp.exp(math.log(196.608) - 2.3025851 * jax.random.uniform(streams_of[22], (MODEL_WIDTH, QUERY_HEADS * HEAD_SIZE), jnp.float32) ** block_scale(streams_of[22], (MODEL_WIDTH, QUERY_HEADS * HEAD_SIZE), ((0, 8), (1, 4)), -0.2, 0.2)), 19.6608, 196.608)
    gate_up_weight_square = jnp.clip(jnp.exp(math.log(589.68) - 2.3025851 * jax.random.uniform(streams_of[23], (2, MODEL_WIDTH, FF), jnp.float32) ** block_scale(streams_of[23], (2, MODEL_WIDTH, FF), ((1, 8), (2, 4)), -0.2, 0.2)), 58.968, 589.68)
    down_weight_square = jnp.clip(jnp.exp(math.log(442.368) - 2.3025851 * jax.random.uniform(streams_of[24], (MODEL_WIDTH, FF), jnp.float32) ** block_scale(streams_of[24], (MODEL_WIDTH, FF), ((0, 8), (1, 4)), -0.2, 0.2)), 44.2368, 442.368)
    norm_gains_square = jnp.clip(jnp.exp(math.log(4915.2) - 2.3025852 * jax.random.uniform(streams_of[25], (2, MODEL_WIDTH), jnp.float32) ** block_scale(streams_of[25], (2, MODEL_WIDTH), ((1, 8),), -0.2, 0.2)), 491.52, 4915.2)
    headnorm_gains_square = jnp.clip(jnp.exp(math.log(64225.28) - 2.3025851 * jax.random.uniform(streams_of[26], (2, HEAD_SIZE), jnp.float32) ** block_scale(streams_of[26], (2, HEAD_SIZE), ((1, 8),), -0.2, 0.2)), 6422.528, 64225.28)
    return {"layer_input": layer_input, "out_grad": out_grad, "segment_ids": segment_ids, "query_weight": query_weight, "key_weight": key_weight, "value_matrix": value_matrix, "output_weight": output_weight, "gate_up_weight": gate_up_weight, "down_weight": down_weight, "norm_gains": norm_gains, "headnorm_gains": headnorm_gains, "query_weight_mean": query_weight_mean, "key_weight_first_moment": key_weight_first_moment, "value_weight_first_moment": value_weight_first_moment, "output_weight_mean": output_weight_mean, "gate_up_weight_mean": gate_up_weight_mean, "down_weight_mean": down_weight_mean, "norm_gains_mean": norm_gains_mean, "headnorm_gains_mean": headnorm_gains_mean, "query_weight_square": query_weight_square, "key_weight_second_moment": key_weight_second_moment, "value_weight_second_moment": value_weight_second_moment, "output_weight_square": output_weight_square, "gate_up_weight_square": gate_up_weight_square, "down_weight_square": down_weight_square, "norm_gains_square": norm_gains_square, "headnorm_gains_square": headnorm_gains_square}


EPSILON = 1e-06
ROPE_BASE = 1000000.0
MASKED = -1e+30
BETA_ONE = 0.9
BETA_TWO = 0.95
ADAM_EPSILON = 1e-08
MATRIX_RATE = 0.02
GAIN_RATE = 0.1
WEIGHT_DECAY = 0.1
HIGHEST_PRECISION = lax.Precision.HIGHEST

@jax.custom_vjp
def low(v):
    return lax.optimization_barrier(v.astype(jnp.bfloat16)).astype(jnp.float32)

@jax.custom_vjp
def low_back(v):
    return v

def low_keep(v):
    return (low(v), None)

def low_pass(kept, grad):
    return (grad,)

def back_keep(v):
    return (v, None)

def back_low(kept, grad):
    return (low(grad),)
low.defvjp(low_keep, low_pass)
low_back.defvjp(back_keep, back_low)

def root_mean_scale(values):
    return values * lax.rsqrt(lax.optimization_barrier(jnp.mean(values * values, axis=-1, keepdims=True)) + EPSILON)

def positions_of(segments):
    earlier = lax.optimization_barrier(jnp.sum((segments[None, :] < segments[:, None]).astype(jnp.int32), axis=1))
    return jnp.arange(segments.shape[0], dtype=jnp.int32) - earlier.astype(jnp.int32)

def rotary_embedding(values, token_positions):
    head_width = values.shape[-1]
    half_width = head_width // 2
    frequencies = ROPE_BASE ** (-2.0 * jnp.arange(half_width).astype(values.dtype) / head_width)
    angles = token_positions.astype(values.dtype)[:, None] * frequencies[None, :]
    cosine = jnp.cos(angles)[:, None, :]
    sine_part = jnp.sin(angles)[:, None, :]
    first_half = values[..., :half_width]
    second_half = values[..., half_width:]
    return jnp.concatenate([first_half * cosine - second_half * sine_part, second_half * cosine + first_half * sine_part], axis=-1)

def matmul(left, right):
    return jnp.dot(left, right, precision=HIGHEST_PRECISION, preferred_element_type=jnp.float32)

def shard_block(params, input_rows, segments):
    query_w, key_w, value_w, output_w, gate_up_w, down_w, norm_g, grouped_head = params
    packed_token_count = input_rows.shape[0]
    token_positions = positions_of(segments)
    normed_one = low(root_mean_scale(input_rows) * norm_g[0])
    query_proj = low_back(matmul(normed_one, query_w))
    key_projected = low_back(matmul(normed_one, key_w))
    value_projected = matmul(normed_one, value_w)
    query_heads = rotary_embedding(root_mean_scale(query_proj.reshape(packed_token_count, QUERY_HEADS, HEAD_SIZE)) * grouped_head[0], token_positions)
    per_head_keys = rotary_embedding(root_mean_scale(key_projected.reshape(packed_token_count, KEY_VALUE_HEADS, HEAD_SIZE)) * grouped_head[1], token_positions)
    query_heads = low_back(low(query_heads))
    per_head_keys = low_back(low(per_head_keys))
    per_head_values = low_back(low(value_projected.reshape(packed_token_count, KEY_VALUE_HEADS, HEAD_SIZE)))
    query_group_width = QUERY_HEADS // KEY_VALUE_HEADS
    key_wide = jnp.repeat(per_head_keys, query_group_width, axis=1)
    value_wide = jnp.repeat(per_head_values, query_group_width, axis=1)
    score_scale = 1.0 / math.sqrt(HEAD_SIZE)
    raw_scores = jnp.einsum('qhd,khd->hqk', query_heads, key_wide, precision=HIGHEST_PRECISION) * score_scale
    token_index = jnp.arange(packed_token_count)
    allowed = (segments[:, None] == segments[None, :]) & (token_index[None, :] <= token_index[:, None])
    scores = low_back(jnp.where(allowed[None], raw_scores, MASKED))
    row_max = lax.optimization_barrier(jnp.max(scores, axis=-1, keepdims=True))
    exponent = jnp.exp(scores - row_max)
    probs = exponent / lax.optimization_barrier(jnp.sum(exponent, axis=-1, keepdims=True))
    mixed = jnp.einsum('hqk,khd->qhd', low(probs), value_wide, precision=HIGHEST_PRECISION)
    mixed = low_back(low(mixed.reshape(packed_token_count, QUERY_HEADS * HEAD_SIZE)))
    attention_out = low_back(matmul(mixed, output_w.T))
    middle = input_rows + attention_out
    normed_two = low(root_mean_scale(middle) * norm_g[1])
    gate_proj = low_back(matmul(normed_two, gate_up_w[0]))
    up_proj = low_back(matmul(normed_two, gate_up_w[1]))
    hidden = low(jax.nn.silu(gate_proj) * up_proj)
    return middle + low_back(matmul(hidden, down_w.T))

def forward(input_rows, params, segments):
    rounded_params = tuple((low(weight) for weight in params))

    def one_shard(shard_item):
        return shard_block(rounded_params, shard_item[0], shard_item[1])
    outputs = lax.map(jax.checkpoint(one_shard), (input_rows.reshape(-1, TOK_DEV, MODEL_WIDTH), segments.reshape(-1, TOK_DEV)))
    return outputs.reshape(TOKENS, MODEL_WIDTH)

def adam_step(weight, gradient, mean_state, square_state, learn_rate, decay_rate):
    mean_next = BETA_ONE * mean_state + (1.0 - BETA_ONE) * gradient
    square_next = BETA_TWO * square_state + (1.0 - BETA_TWO) * gradient * gradient
    mean_hat = mean_next / (1.0 - BETA_ONE ** ADAM_STEP)
    square_hat = square_next / (1.0 - BETA_TWO ** ADAM_STEP)
    weight_next = weight - learn_rate * (mean_hat / (jnp.sqrt(square_hat) + ADAM_EPSILON) + decay_rate * weight)
    return (weight_next - weight, mean_next, square_next)

def reference(layer_input, out_grad, segment_ids, query_weight, key_weight, value_matrix, output_weight, gate_up_weight, down_weight, norm_gains, headnorm_gains, query_weight_mean, key_weight_first_moment, value_weight_first_moment, output_weight_mean, gate_up_weight_mean, down_weight_mean, norm_gains_mean, headnorm_gains_mean, query_weight_square, key_weight_second_moment, value_weight_second_moment, output_weight_square, gate_up_weight_square, down_weight_square, norm_gains_square, headnorm_gains_square):
    params = (query_weight, key_weight, value_matrix, output_weight, gate_up_weight, down_weight, norm_gains, headnorm_gains)
    means = (query_weight_mean, key_weight_first_moment, value_weight_first_moment, output_weight_mean, gate_up_weight_mean, down_weight_mean, norm_gains_mean, headnorm_gains_mean)
    squares = (query_weight_square, key_weight_second_moment, value_weight_second_moment, output_weight_square, gate_up_weight_square, down_weight_square, norm_gains_square, headnorm_gains_square)
    input_rows = layer_input.astype(jnp.float32)

    def whole(rows_in, *weights):
        return forward(rows_in, weights, segment_ids)
    output_rows, pull_back = jax.vjp(whole, input_rows, *params)
    gradients = pull_back(out_grad.astype(jnp.float32))
    input_grad = gradients[0]
    weight_grads = gradients[1:]
    updates = []
    for param_index in range(8):
        learn_rate = MATRIX_RATE if param_index < 6 else GAIN_RATE
        decay_rate = WEIGHT_DECAY if param_index < 6 else 0.0
        updates.append(adam_step(params[param_index], weight_grads[param_index], means[param_index], squares[param_index], learn_rate, decay_rate))
    return (output_rows, input_grad, weight_grads[0], weight_grads[1], weight_grads[2], weight_grads[3], weight_grads[4], weight_grads[5], weight_grads[6], weight_grads[7], updates[0][0], updates[1][0], updates[2][0], updates[3][0], updates[4][0], updates[5][0], updates[6][0], updates[7][0], updates[0][1], updates[1][1], updates[2][1], updates[3][1], updates[4][1], updates[5][1], updates[6][1], updates[7][1], updates[0][2], updates[1][2], updates[2][2], updates[3][2], updates[4][2], updates[5][2], updates[6][2], updates[7][2])
```

```python
import math

import jax
import jax.numpy as jnp
from jax import lax
from jax.sharding import PartitionSpec as P

HEAD_SIZE = 128
ADAM_STEP = 3


EPSILON = 1e-06
ROPE_BASE = 1000000.0
MASKED = -1e30
BETA_ONE = 0.9
BETA_TWO = 0.95
ADAM_EPSILON = 1e-08
MATRIX_RATE = 0.02
GAIN_RATE = 0.1
WEIGHT_DECAY = 0.1


def root_mean_scale(values):
    return values * lax.rsqrt(jnp.mean(values * values, axis=-1, keepdims=True) + EPSILON)


def positions_of(segments):
    earlier = jnp.sum((segments[None, :] < segments[:, None]).astype(jnp.int32), axis=1)
    return jnp.arange(segments.shape[0], dtype=jnp.int32) - earlier


def rotary_embedding(values, token_positions):
    head_width = values.shape[-1]
    half_width = head_width // 2
    frequencies = ROPE_BASE ** (-2.0 * jnp.arange(half_width).astype(values.dtype) / head_width)
    angles = token_positions.astype(values.dtype)[:, None] * frequencies[None, :]
    cosine = jnp.cos(angles)[:, None, :]
    sine_part = jnp.sin(angles)[:, None, :]
    first_half = values[..., :half_width]
    second_half = values[..., half_width:]
    return jnp.concatenate(
        [
            first_half * cosine - second_half * sine_part,
            second_half * cosine + first_half * sine_part,
        ],
        axis=-1,
    )


def contract_rows(left, right):
    return lax.dot_general(
        left, right, (((0,), (0,)), ((), ())), preferred_element_type=jnp.float32
    )


def contract_cols(left, right):
    return lax.dot_general(
        left, right, (((1,), (1,)), ((), ())), preferred_element_type=jnp.float32
    )


def gained_norm(values, gain):
    return root_mean_scale(values) * gain


def swiglu(gate_proj, up_proj):
    return jax.nn.silu(gate_proj) * up_proj


def adam_step(weight, gradient, mean_state, square_state, learn_rate, decay_rate):
    mean_next = BETA_ONE * mean_state + (1.0 - BETA_ONE) * gradient
    square_next = BETA_TWO * square_state + (1.0 - BETA_TWO) * gradient * gradient
    mean_hat = mean_next / (1.0 - BETA_ONE**ADAM_STEP)
    square_hat = square_next / (1.0 - BETA_TWO**ADAM_STEP)
    weight_next = weight - learn_rate * (
        mean_hat / (jnp.sqrt(square_hat) + ADAM_EPSILON) + decay_rate * weight
    )
    return (weight_next - weight, mean_next, square_next)


def per_device(
    layer_input,
    out_grad,
    segment_ids,
    query_weight,
    key_weight,
    value_matrix,
    output_weight,
    gate_up_weight,
    down_weight,
    norm_gains,
    headnorm_gains,
    query_weight_mean,
    key_weight_first_moment,
    value_weight_first_moment,
    output_weight_mean,
    gate_up_weight_mean,
    down_weight_mean,
    norm_gains_mean,
    headnorm_gains_mean,
    query_weight_square,
    key_weight_second_moment,
    value_weight_second_moment,
    output_weight_square,
    gate_up_weight_square,
    down_weight_square,
    norm_gains_square,
    headnorm_gains_square,
):
    params = (
        query_weight,
        key_weight,
        value_matrix,
        output_weight,
        gate_up_weight,
        down_weight,
        norm_gains,
        headnorm_gains,
    )
    means = (
        query_weight_mean,
        key_weight_first_moment,
        value_weight_first_moment,
        output_weight_mean,
        gate_up_weight_mean,
        down_weight_mean,
        norm_gains_mean,
        headnorm_gains_mean,
    )
    squares = (
        query_weight_square,
        key_weight_second_moment,
        value_weight_second_moment,
        output_weight_square,
        gate_up_weight_square,
        down_weight_square,
        norm_gains_square,
        headnorm_gains_square,
    )
    gain_rows = norm_gains.shape[1]
    gains_low = lax.all_gather(
        jnp.concatenate([norm_gains, headnorm_gains], axis=1).astype(jnp.bfloat16),
        "fsdp",
        axis=0,
    )
    norm_full = jnp.swapaxes(gains_low[:, :, :gain_rows], 0, 1).reshape(2, -1)
    head_full = jnp.swapaxes(gains_low[:, :, gain_rows:], 0, 1).reshape(2, -1)
    query_cols = query_weight.shape[1]
    key_cols = key_weight.shape[1]
    attn_low = jnp.concatenate(
        [query_weight, key_weight, value_matrix, output_weight], axis=1
    ).astype(jnp.bfloat16)
    attn_full = lax.all_gather(attn_low, "fsdp", axis=0, tiled=True)
    query_full = attn_full[:, :query_cols]
    key_full = attn_full[:, query_cols : query_cols + key_cols]
    value_full = attn_full[:, query_cols + key_cols : query_cols + 2 * key_cols]
    output_full = attn_full[:, query_cols + 2 * key_cols :]
    gate_up_full = lax.all_gather(gate_up_weight.astype(jnp.bfloat16), "fsdp", axis=1, tiled=True)
    down_full = lax.all_gather(down_weight.astype(jnp.bfloat16), "fsdp", axis=0, tiled=True)
    norm_gain = norm_full.astype(jnp.float32)
    head_gain = head_full.astype(jnp.float32)
    packed_token_count = layer_input.shape[0]
    local_query = query_full.shape[1] // HEAD_SIZE
    local_groups = key_full.shape[1] // HEAD_SIZE
    query_group_width = local_query // local_groups
    score_scale = 1.0 / math.sqrt(HEAD_SIZE)
    token_positions = positions_of(segment_ids)
    token_index = jnp.arange(packed_token_count, dtype=jnp.int32)
    input_rows = layer_input.astype(jnp.float32)

    def head_map(projected, gain, heads):
        return rotary_embedding(
            root_mean_scale(projected.reshape(packed_token_count, heads, HEAD_SIZE)) * gain,
            token_positions,
        )

    normed_one = gained_norm(input_rows, norm_gain[0]).astype(jnp.bfloat16)
    query_proj = jnp.dot(normed_one, query_full, preferred_element_type=jnp.float32)
    key_projected = jnp.dot(normed_one, key_full, preferred_element_type=jnp.float32)
    value_projected = jnp.dot(normed_one, value_full, preferred_element_type=jnp.float32)
    query_heads = (
        head_map(query_proj, head_gain[0], local_query)
        .astype(jnp.bfloat16)
        .reshape(packed_token_count, local_groups, query_group_width, HEAD_SIZE)
    )
    per_head_keys = head_map(key_projected, head_gain[1], local_groups).astype(jnp.bfloat16)
    per_head_values = value_projected.astype(jnp.bfloat16).reshape(
        packed_token_count, local_groups, HEAD_SIZE
    )
    block_rows = min(512, packed_token_count)
    block_count = packed_token_count // block_rows

    def block_scores(row_start, row_stop):
        raw_scores = (
            jnp.einsum(
                "qhgd,khd->hgqk",
                query_heads[row_start:row_stop],
                per_head_keys[:row_stop],
                preferred_element_type=jnp.float32,
            )
            * score_scale
        )
        allowed = (segment_ids[row_start:row_stop, None] == segment_ids[None, :row_stop]) & (
            token_index[None, :row_stop] <= token_index[row_start:row_stop, None]
        )
        return jnp.where(allowed, raw_scores, MASKED)

    mixed_blocks = []
    log_sums = []
    for block_index in range(block_count):
        row_start = block_index * block_rows
        row_stop = row_start + block_rows
        scores = block_scores(row_start, row_stop)
        row_max = jnp.max(scores, axis=-1, keepdims=True)
        exponent = jnp.exp(scores - row_max)
        row_sum = jnp.sum(exponent, axis=-1, keepdims=True)
        weights_block = (exponent / row_sum).astype(jnp.bfloat16)
        log_sums.append(row_max + jnp.log(row_sum))
        mixed_blocks.append(
            jnp.einsum(
                "hgqk,khd->qhgd",
                weights_block,
                per_head_values[:row_stop],
                preferred_element_type=jnp.float32,
            )
        )
    mixed = (
        jnp.concatenate(mixed_blocks, axis=0)
        .reshape(packed_token_count, local_query * HEAD_SIZE)
        .astype(jnp.bfloat16)
    )
    attention_part = contract_cols(mixed, output_full)
    attention_out = lax.psum(attention_part.astype(jnp.bfloat16), "tensor").astype(jnp.float32)
    middle = input_rows + attention_out
    normed_two = gained_norm(middle, norm_gain[1]).astype(jnp.bfloat16)
    gate_proj = jnp.dot(normed_two, gate_up_full[0], preferred_element_type=jnp.float32)
    up_proj = jnp.dot(normed_two, gate_up_full[1], preferred_element_type=jnp.float32)
    hidden = swiglu(gate_proj, up_proj).astype(jnp.bfloat16)
    down_part = contract_cols(hidden, down_full)
    feedforward_out = lax.psum(down_part.astype(jnp.bfloat16), "tensor").astype(jnp.float32)
    layer_output = middle + feedforward_out
    query_back, key_back, value_back, output_back, gate_up_back, down_back = (
        query_full,
        key_full,
        value_full,
        output_full,
        gate_up_full,
        down_full,
    )
    grad_rows = out_grad.astype(jnp.float32)
    down_grad = contract_rows(out_grad, hidden)
    hidden_grad = jnp.dot(out_grad, down_back, preferred_element_type=jnp.float32)
    swiglu_out, swiglu_back = jax.vjp(swiglu, gate_proj, up_proj)
    gate_grad, up_grad = swiglu_back(hidden_grad)
    gate_grad_low = gate_grad.astype(jnp.bfloat16)
    up_grad_low = up_grad.astype(jnp.bfloat16)
    gate_up_grad = jnp.stack(
        [contract_rows(normed_two, gate_grad_low), contract_rows(normed_two, up_grad_low)]
    )
    normed_two_part = contract_cols(gate_grad_low, gate_up_back[0]) + contract_cols(
        up_grad_low, gate_up_back[1]
    )
    normed_two_grad = lax.psum(normed_two_part.astype(jnp.bfloat16), "tensor").astype(jnp.float32)
    norm_two_out, norm_two_back = jax.vjp(gained_norm, middle, norm_gain[1])
    middle_norm_grad, gain_two_grad = norm_two_back(normed_two_grad)
    middle_grad = grad_rows + middle_norm_grad
    middle_grad_low = middle_grad.astype(jnp.bfloat16)
    output_grad_w = contract_rows(middle_grad_low, mixed)
    mixed_grad = jnp.dot(middle_grad_low, output_back, preferred_element_type=jnp.float32).astype(
        jnp.bfloat16
    )
    mixed_grad = mixed_grad.reshape(packed_token_count, local_groups, query_group_width, HEAD_SIZE)
    query_grad_blocks = []
    key_grad_acc = jnp.zeros((packed_token_count, local_groups, HEAD_SIZE), jnp.float32)
    value_grad_acc = jnp.zeros((packed_token_count, local_groups, HEAD_SIZE), jnp.float32)
    for block_index in range(block_count):
        row_start = block_index * block_rows
        row_stop = row_start + block_rows
        scores = block_scores(row_start, row_stop)
        probs = jnp.exp(scores - log_sums[block_index])
        grad_block = mixed_grad[row_start:row_stop]
        prob_grad = jnp.einsum(
            "qhgd,khd->hgqk",
            grad_block,
            per_head_values[:row_stop],
            preferred_element_type=jnp.float32,
        )
        row_inner = jnp.sum(probs * prob_grad, axis=-1, keepdims=True)
        score_grad = (probs * (prob_grad - row_inner)).astype(jnp.bfloat16)
        query_grad_blocks.append(
            jnp.einsum(
                "hgqk,khd->qhgd",
                score_grad,
                per_head_keys[:row_stop],
                preferred_element_type=jnp.float32,
            )
            * score_scale
        )
        key_grad_acc = key_grad_acc.at[:row_stop].add(
            jnp.einsum(
                "hgqk,qhgd->khd",
                score_grad,
                query_heads[row_start:row_stop],
                preferred_element_type=jnp.float32,
            )
            * score_scale
        )
        value_grad_acc = value_grad_acc.at[:row_stop].add(
            jnp.einsum(
                "hgqk,qhgd->khd",
                probs.astype(jnp.bfloat16),
                grad_block,
                preferred_element_type=jnp.float32,
            )
        )
    query_grad_heads = (
        jnp.concatenate(query_grad_blocks, axis=0)
        .reshape(packed_token_count, local_query, HEAD_SIZE)
        .astype(jnp.bfloat16)
        .astype(jnp.float32)
    )
    key_grad_heads = key_grad_acc.astype(jnp.bfloat16).astype(jnp.float32)
    value_grad_low = value_grad_acc.astype(jnp.bfloat16).reshape(
        packed_token_count, local_groups * HEAD_SIZE
    )
    query_map_out, query_map_back = jax.vjp(
        lambda projected, gain: head_map(projected, gain, local_query), query_proj, head_gain[0]
    )
    query_proj_grad, head_query_grad = query_map_back(query_grad_heads)
    key_map_out, key_map_back = jax.vjp(
        lambda projected, gain: head_map(projected, gain, local_groups), key_projected, head_gain[1]
    )
    key_proj_grad, head_key_grad = key_map_back(key_grad_heads)
    query_proj_low = query_proj_grad.astype(jnp.bfloat16)
    key_proj_low = key_proj_grad.astype(jnp.bfloat16)
    query_grad_w = contract_rows(normed_one, query_proj_low)
    key_grad_w = contract_rows(normed_one, key_proj_low)
    value_grad_w = contract_rows(normed_one, value_grad_low)
    normed_one_part = (
        contract_cols(query_proj_low, query_back)
        + contract_cols(key_proj_low, key_back)
        + contract_cols(value_grad_low, value_back)
    )
    normed_one_grad = lax.psum(normed_one_part.astype(jnp.bfloat16), "tensor").astype(jnp.float32)
    head_query_total, head_key_total = lax.psum((head_query_grad, head_key_grad), "tensor")
    norm_one_out, norm_one_back = jax.vjp(gained_norm, input_rows, norm_gain[0])
    input_norm_grad, gain_one_grad = norm_one_back(normed_one_grad)
    input_grad = middle_grad + input_norm_grad
    norm_grads = jnp.stack([gain_one_grad, gain_two_grad])
    head_grads = jnp.stack([head_query_total, head_key_total])
    attn_grads = lax.psum_scatter(
        jnp.concatenate(
            [
                query_grad_w.astype(jnp.bfloat16),
                key_grad_w.astype(jnp.bfloat16),
                value_grad_w.astype(jnp.bfloat16),
                output_grad_w.astype(jnp.bfloat16),
            ],
            axis=1,
        ),
        "fsdp",
        scatter_dimension=0,
        tiled=True,
    ).astype(jnp.float32)
    shards = norm_grads.shape[1] // gain_rows
    gains_grad = lax.psum_scatter(
        jnp.concatenate(
            [norm_grads.reshape(2, shards, gain_rows), head_grads.reshape(2, shards, -1)], axis=2
        ),
        "fsdp",
        scatter_dimension=1,
        tiled=False,
    )
    shard_grads = (
        attn_grads[:, :query_cols],
        attn_grads[:, query_cols : query_cols + key_cols],
        attn_grads[:, query_cols + key_cols : query_cols + 2 * key_cols],
        attn_grads[:, query_cols + 2 * key_cols :],
        lax.psum_scatter(
            gate_up_grad.astype(jnp.bfloat16), "fsdp", scatter_dimension=1, tiled=True
        ).astype(jnp.float32),
        lax.psum_scatter(
            down_grad.astype(jnp.bfloat16), "fsdp", scatter_dimension=0, tiled=True
        ).astype(jnp.float32),
        gains_grad[:, :gain_rows],
        gains_grad[:, gain_rows:],
    )
    next_steps = []
    next_means = []
    next_squares = []
    for param_index in range(8):
        learn_rate = MATRIX_RATE if param_index < 6 else GAIN_RATE
        decay_rate = WEIGHT_DECAY if param_index < 6 else 0.0
        weight_step, mean_next, square_next = adam_step(
            params[param_index],
            shard_grads[param_index],
            means[param_index],
            squares[param_index],
            learn_rate,
            decay_rate,
        )
        next_steps.append(weight_step)
        next_means.append(mean_next)
        next_squares.append(square_next)
    results = (
        [layer_output, input_grad] + list(shard_grads) + next_steps + next_means + next_squares
    )
    return tuple(results)


def solution(mesh):
    return jax.shard_map(
        per_device,
        mesh=mesh,
        in_specs=(
            P("fsdp", None),
            P("fsdp", None),
            P("fsdp"),
            P("fsdp", "tensor"),
            P("fsdp", "tensor"),
            P("fsdp", "tensor"),
            P("fsdp", "tensor"),
            P(None, "fsdp", "tensor"),
            P("fsdp", "tensor"),
            P(None, "fsdp"),
            P(None, "fsdp"),
            P("fsdp", "tensor"),
            P("fsdp", "tensor"),
            P("fsdp", "tensor"),
            P("fsdp", "tensor"),
            P(None, "fsdp", "tensor"),
            P("fsdp", "tensor"),
            P(None, "fsdp"),
            P(None, "fsdp"),
            P("fsdp", "tensor"),
            P("fsdp", "tensor"),
            P("fsdp", "tensor"),
            P("fsdp", "tensor"),
            P(None, "fsdp", "tensor"),
            P("fsdp", "tensor"),
            P(None, "fsdp"),
            P(None, "fsdp"),
        ),
        out_specs=(
            P("fsdp", None),
            P("fsdp", None),
            P("fsdp", "tensor"),
            P("fsdp", "tensor"),
            P("fsdp", "tensor"),
            P("fsdp", "tensor"),
            P(None, "fsdp", "tensor"),
            P("fsdp", "tensor"),
            P(None, "fsdp"),
            P(None, "fsdp"),
            P("fsdp", "tensor"),
            P("fsdp", "tensor"),
            P("fsdp", "tensor"),
            P("fsdp", "tensor"),
            P(None, "fsdp", "tensor"),
            P("fsdp", "tensor"),
            P(None, "fsdp"),
            P(None, "fsdp"),
            P("fsdp", "tensor"),
            P("fsdp", "tensor"),
            P("fsdp", "tensor"),
            P("fsdp", "tensor"),
            P(None, "fsdp", "tensor"),
            P("fsdp", "tensor"),
            P(None, "fsdp"),
            P(None, "fsdp"),
            P("fsdp", "tensor"),
            P("fsdp", "tensor"),
            P("fsdp", "tensor"),
            P("fsdp", "tensor"),
            P(None, "fsdp", "tensor"),
            P("fsdp", "tensor"),
            P(None, "fsdp"),
            P(None, "fsdp"),
        ),
        check_vma=False,
    )
```

```python
import functools
import math

import jax
import jax.numpy as jnp
from jax import lax
from jax.experimental import pallas as pl
from jax.experimental.pallas import tpu as pltpu
from jax.sharding import PartitionSpec as P

HEAD_SIZE = 128
MODEL_WIDTH = 2048
ADAM_STEP = 3


EPSILON = 1e-06
ROPE_BASE = 1000000.0
MASKED = -1e30
BETA_ONE = 0.9
BETA_TWO = 0.95
ADAM_EPSILON = 1e-08
MATRIX_RATE = 0.02
GAIN_RATE = 0.1
WEIGHT_DECAY = 0.1


def root_mean_scale(values):
    return values * lax.rsqrt(jnp.mean(values * values, axis=-1, keepdims=True) + EPSILON)


def positions_of(segments):
    earlier = jnp.sum((segments[None, :] < segments[:, None]).astype(jnp.int32), axis=1)
    return jnp.arange(segments.shape[0], dtype=jnp.int32) - earlier


def rotary_embedding(values, token_positions):
    head_width = values.shape[-1]
    half_width = head_width // 2
    frequencies = ROPE_BASE ** (-2.0 * jnp.arange(half_width).astype(values.dtype) / head_width)
    angles = token_positions.astype(values.dtype)[:, None] * frequencies[None, :]
    cosine = jnp.cos(angles)[:, None, :]
    sine_part = jnp.sin(angles)[:, None, :]
    first_half = values[..., :half_width]
    second_half = values[..., half_width:]
    return jnp.concatenate(
        [
            first_half * cosine - second_half * sine_part,
            second_half * cosine + first_half * sine_part,
        ],
        axis=-1,
    )


def contract_rows(left, right):
    return lax.dot_general(
        left, right, (((0,), (0,)), ((), ())), preferred_element_type=jnp.float32
    )


def contract_cols(left, right):
    return lax.dot_general(
        left, right, (((1,), (1,)), ((), ())), preferred_element_type=jnp.float32
    )


def gained_norm(values, gain):
    return root_mean_scale(values) * gain


def swiglu(gate_proj, up_proj):
    return jax.nn.silu(gate_proj) * up_proj


def adam_step(weight, gradient, mean_state, square_state, learn_rate, decay_rate):
    mean_next = BETA_ONE * mean_state + (1.0 - BETA_ONE) * gradient
    square_next = BETA_TWO * square_state + (1.0 - BETA_TWO) * gradient * gradient
    mean_hat = mean_next / (1.0 - BETA_ONE**ADAM_STEP)
    square_hat = square_next / (1.0 - BETA_TWO**ADAM_STEP)
    weight_next = weight - learn_rate * (
        mean_hat / (jnp.sqrt(square_hat) + ADAM_EPSILON) + decay_rate * weight
    )
    return (weight_next - weight, mean_next, square_next)


def plain_device(
    layer_input,
    out_grad,
    segment_ids,
    query_weight,
    key_weight,
    value_matrix,
    output_weight,
    gate_up_weight,
    down_weight,
    norm_gains,
    headnorm_gains,
    query_weight_mean,
    key_weight_first_moment,
    value_weight_first_moment,
    output_weight_mean,
    gate_up_weight_mean,
    down_weight_mean,
    norm_gains_mean,
    headnorm_gains_mean,
    query_weight_square,
    key_weight_second_moment,
    value_weight_second_moment,
    output_weight_square,
    gate_up_weight_square,
    down_weight_square,
    norm_gains_square,
    headnorm_gains_square,
):
    params = (
        query_weight,
        key_weight,
        value_matrix,
        output_weight,
        gate_up_weight,
        down_weight,
        norm_gains,
        headnorm_gains,
    )
    means = (
        query_weight_mean,
        key_weight_first_moment,
        value_weight_first_moment,
        output_weight_mean,
        gate_up_weight_mean,
        down_weight_mean,
        norm_gains_mean,
        headnorm_gains_mean,
    )
    squares = (
        query_weight_square,
        key_weight_second_moment,
        value_weight_second_moment,
        output_weight_square,
        gate_up_weight_square,
        down_weight_square,
        norm_gains_square,
        headnorm_gains_square,
    )
    gain_rows = norm_gains.shape[1]
    gains_low = lax.all_gather(
        jnp.concatenate([norm_gains, headnorm_gains], axis=1).astype(jnp.bfloat16),
        "fsdp",
        axis=0,
    )
    norm_full = jnp.swapaxes(gains_low[:, :, :gain_rows], 0, 1).reshape(2, -1)
    head_full = jnp.swapaxes(gains_low[:, :, gain_rows:], 0, 1).reshape(2, -1)
    query_cols = query_weight.shape[1]
    key_cols = key_weight.shape[1]
    attn_low = jnp.concatenate(
        [query_weight, key_weight, value_matrix, output_weight], axis=1
    ).astype(jnp.bfloat16)
    attn_full = lax.all_gather(attn_low, "fsdp", axis=0, tiled=True)
    query_full = attn_full[:, :query_cols]
    key_full = attn_full[:, query_cols : query_cols + key_cols]
    value_full = attn_full[:, query_cols + key_cols : query_cols + 2 * key_cols]
    output_full = attn_full[:, query_cols + 2 * key_cols :]
    gate_up_full = lax.all_gather(gate_up_weight.astype(jnp.bfloat16), "fsdp", axis=1, tiled=True)
    down_full = lax.all_gather(down_weight.astype(jnp.bfloat16), "fsdp", axis=0, tiled=True)
    norm_gain = norm_full.astype(jnp.float32)
    head_gain = head_full.astype(jnp.float32)
    packed_token_count = layer_input.shape[0]
    local_query = query_full.shape[1] // HEAD_SIZE
    local_groups = key_full.shape[1] // HEAD_SIZE
    query_group_width = local_query // local_groups
    score_scale = 1.0 / math.sqrt(HEAD_SIZE)
    token_positions = positions_of(segment_ids)
    token_index = jnp.arange(packed_token_count, dtype=jnp.int32)
    input_rows = layer_input.astype(jnp.float32)

    def head_map(projected, gain, heads):
        return rotary_embedding(
            root_mean_scale(projected.reshape(packed_token_count, heads, HEAD_SIZE)) * gain,
            token_positions,
        )

    normed_one = gained_norm(input_rows, norm_gain[0]).astype(jnp.bfloat16)
    query_proj = jnp.dot(normed_one, query_full, preferred_element_type=jnp.float32)
    key_projected = jnp.dot(normed_one, key_full, preferred_element_type=jnp.float32)
    value_projected = jnp.dot(normed_one, value_full, preferred_element_type=jnp.float32)
    query_heads = (
        head_map(query_proj, head_gain[0], local_query)
        .astype(jnp.bfloat16)
        .reshape(packed_token_count, local_groups, query_group_width, HEAD_SIZE)
    )
    per_head_keys = head_map(key_projected, head_gain[1], local_groups).astype(jnp.bfloat16)
    per_head_values = value_projected.astype(jnp.bfloat16).reshape(
        packed_token_count, local_groups, HEAD_SIZE
    )
    block_rows = min(512, packed_token_count)
    block_count = packed_token_count // block_rows

    def block_scores(row_start, row_stop):
        raw_scores = (
            jnp.einsum(
                "qhgd,khd->hgqk",
                query_heads[row_start:row_stop],
                per_head_keys[:row_stop],
                preferred_element_type=jnp.float32,
            )
            * score_scale
        )
        allowed = (segment_ids[row_start:row_stop, None] == segment_ids[None, :row_stop]) & (
            token_index[None, :row_stop] <= token_index[row_start:row_stop, None]
        )
        return jnp.where(allowed, raw_scores, MASKED)

    mixed_blocks = []
    log_sums = []
    for block_index in range(block_count):
        row_start = block_index * block_rows
        row_stop = row_start + block_rows
        scores = block_scores(row_start, row_stop)
        row_max = jnp.max(scores, axis=-1, keepdims=True)
        exponent = jnp.exp(scores - row_max)
        row_sum = jnp.sum(exponent, axis=-1, keepdims=True)
        weights_block = (exponent / row_sum).astype(jnp.bfloat16)
        log_sums.append(row_max + jnp.log(row_sum))
        mixed_blocks.append(
            jnp.einsum(
                "hgqk,khd->qhgd",
                weights_block,
                per_head_values[:row_stop],
                preferred_element_type=jnp.float32,
            )
        )
    mixed = (
        jnp.concatenate(mixed_blocks, axis=0)
        .reshape(packed_token_count, local_query * HEAD_SIZE)
        .astype(jnp.bfloat16)
    )
    attention_part = contract_cols(mixed, output_full)
    attention_out = lax.psum(attention_part.astype(jnp.bfloat16), "tensor").astype(jnp.float32)
    middle = input_rows + attention_out
    normed_two = gained_norm(middle, norm_gain[1]).astype(jnp.bfloat16)
    gate_proj = jnp.dot(normed_two, gate_up_full[0], preferred_element_type=jnp.float32)
    up_proj = jnp.dot(normed_two, gate_up_full[1], preferred_element_type=jnp.float32)
    hidden = swiglu(gate_proj, up_proj).astype(jnp.bfloat16)
    down_part = contract_cols(hidden, down_full)
    feedforward_out = lax.psum(down_part.astype(jnp.bfloat16), "tensor").astype(jnp.float32)
    layer_output = middle + feedforward_out
    query_back, key_back, value_back, output_back, gate_up_back, down_back = (
        query_full,
        key_full,
        value_full,
        output_full,
        gate_up_full,
        down_full,
    )
    grad_rows = out_grad.astype(jnp.float32)
    down_grad = contract_rows(out_grad, hidden)
    hidden_grad = jnp.dot(out_grad, down_back, preferred_element_type=jnp.float32)
    swiglu_out, swiglu_back = jax.vjp(swiglu, gate_proj, up_proj)
    gate_grad, up_grad = swiglu_back(hidden_grad)
    gate_grad_low = gate_grad.astype(jnp.bfloat16)
    up_grad_low = up_grad.astype(jnp.bfloat16)
    gate_up_grad = jnp.stack(
        [contract_rows(normed_two, gate_grad_low), contract_rows(normed_two, up_grad_low)]
    )
    normed_two_part = contract_cols(gate_grad_low, gate_up_back[0]) + contract_cols(
        up_grad_low, gate_up_back[1]
    )
    normed_two_grad = lax.psum(normed_two_part.astype(jnp.bfloat16), "tensor").astype(jnp.float32)
    norm_two_out, norm_two_back = jax.vjp(gained_norm, middle, norm_gain[1])
    middle_norm_grad, gain_two_grad = norm_two_back(normed_two_grad)
    middle_grad = grad_rows + middle_norm_grad
    middle_grad_low = middle_grad.astype(jnp.bfloat16)
    output_grad_w = contract_rows(middle_grad_low, mixed)
    mixed_grad = jnp.dot(middle_grad_low, output_back, preferred_element_type=jnp.float32).astype(
        jnp.bfloat16
    )
    mixed_grad = mixed_grad.reshape(packed_token_count, local_groups, query_group_width, HEAD_SIZE)
    query_grad_blocks = []
    key_grad_acc = jnp.zeros((packed_token_count, local_groups, HEAD_SIZE), jnp.float32)
    value_grad_acc = jnp.zeros((packed_token_count, local_groups, HEAD_SIZE), jnp.float32)
    for block_index in range(block_count):
        row_start = block_index * block_rows
        row_stop = row_start + block_rows
        scores = block_scores(row_start, row_stop)
        probs = jnp.exp(scores - log_sums[block_index])
        grad_block = mixed_grad[row_start:row_stop]
        prob_grad = jnp.einsum(
            "qhgd,khd->hgqk",
            grad_block,
            per_head_values[:row_stop],
            preferred_element_type=jnp.float32,
        )
        row_inner = jnp.sum(probs * prob_grad, axis=-1, keepdims=True)
        score_grad = (probs * (prob_grad - row_inner)).astype(jnp.bfloat16)
        query_grad_blocks.append(
            jnp.einsum(
                "hgqk,khd->qhgd",
                score_grad,
                per_head_keys[:row_stop],
                preferred_element_type=jnp.float32,
            )
            * score_scale
        )
        key_grad_acc = key_grad_acc.at[:row_stop].add(
            jnp.einsum(
                "hgqk,qhgd->khd",
                score_grad,
                query_heads[row_start:row_stop],
                preferred_element_type=jnp.float32,
            )
            * score_scale
        )
        value_grad_acc = value_grad_acc.at[:row_stop].add(
            jnp.einsum(
                "hgqk,qhgd->khd",
                probs.astype(jnp.bfloat16),
                grad_block,
                preferred_element_type=jnp.float32,
            )
        )
    query_grad_heads = (
        jnp.concatenate(query_grad_blocks, axis=0)
        .reshape(packed_token_count, local_query, HEAD_SIZE)
        .astype(jnp.bfloat16)
        .astype(jnp.float32)
    )
    key_grad_heads = key_grad_acc.astype(jnp.bfloat16).astype(jnp.float32)
    value_grad_low = value_grad_acc.astype(jnp.bfloat16).reshape(
        packed_token_count, local_groups * HEAD_SIZE
    )
    query_map_out, query_map_back = jax.vjp(
        lambda projected, gain: head_map(projected, gain, local_query), query_proj, head_gain[0]
    )
    query_proj_grad, head_query_grad = query_map_back(query_grad_heads)
    key_map_out, key_map_back = jax.vjp(
        lambda projected, gain: head_map(projected, gain, local_groups), key_projected, head_gain[1]
    )
    key_proj_grad, head_key_grad = key_map_back(key_grad_heads)
    query_proj_low = query_proj_grad.astype(jnp.bfloat16)
    key_proj_low = key_proj_grad.astype(jnp.bfloat16)
    query_grad_w = contract_rows(normed_one, query_proj_low)
    key_grad_w = contract_rows(normed_one, key_proj_low)
    value_grad_w = contract_rows(normed_one, value_grad_low)
    normed_one_part = (
        contract_cols(query_proj_low, query_back)
        + contract_cols(key_proj_low, key_back)
        + contract_cols(value_grad_low, value_back)
    )
    normed_one_grad = lax.psum(normed_one_part.astype(jnp.bfloat16), "tensor").astype(jnp.float32)
    head_query_total, head_key_total = lax.psum((head_query_grad, head_key_grad), "tensor")
    norm_one_out, norm_one_back = jax.vjp(gained_norm, input_rows, norm_gain[0])
    input_norm_grad, gain_one_grad = norm_one_back(normed_one_grad)
    input_grad = middle_grad + input_norm_grad
    norm_grads = jnp.stack([gain_one_grad, gain_two_grad])
    head_grads = jnp.stack([head_query_total, head_key_total])
    attn_grads = lax.psum_scatter(
        jnp.concatenate(
            [
                query_grad_w.astype(jnp.bfloat16),
                key_grad_w.astype(jnp.bfloat16),
                value_grad_w.astype(jnp.bfloat16),
                output_grad_w.astype(jnp.bfloat16),
            ],
            axis=1,
        ),
        "fsdp",
        scatter_dimension=0,
        tiled=True,
    ).astype(jnp.float32)
    shards = norm_grads.shape[1] // gain_rows
    gains_grad = lax.psum_scatter(
        jnp.concatenate(
            [norm_grads.reshape(2, shards, gain_rows), head_grads.reshape(2, shards, -1)], axis=2
        ),
        "fsdp",
        scatter_dimension=1,
        tiled=False,
    )
    shard_grads = (
        attn_grads[:, :query_cols],
        attn_grads[:, query_cols : query_cols + key_cols],
        attn_grads[:, query_cols + key_cols : query_cols + 2 * key_cols],
        attn_grads[:, query_cols + 2 * key_cols :],
        lax.psum_scatter(
            gate_up_grad.astype(jnp.bfloat16), "fsdp", scatter_dimension=1, tiled=True
        ).astype(jnp.float32),
        lax.psum_scatter(
            down_grad.astype(jnp.bfloat16), "fsdp", scatter_dimension=0, tiled=True
        ).astype(jnp.float32),
        gains_grad[:, :gain_rows],
        gains_grad[:, gain_rows:],
    )
    next_steps = []
    next_means = []
    next_squares = []
    for param_index in range(8):
        learn_rate = MATRIX_RATE if param_index < 6 else GAIN_RATE
        decay_rate = WEIGHT_DECAY if param_index < 6 else 0.0
        weight_step, mean_next, square_next = adam_step(
            params[param_index],
            shard_grads[param_index],
            means[param_index],
            squares[param_index],
            learn_rate,
            decay_rate,
        )
        next_steps.append(weight_step)
        next_means.append(mean_next)
        next_squares.append(square_next)
    results = (
        [layer_output, input_grad] + list(shard_grads) + next_steps + next_means + next_squares
    )
    return tuple(results)


CORE_PAIRS = [(0, 1), (1, 0), (2, 3), (3, 2)]
CHIP_PAIRS = [(0, 2), (2, 0), (1, 3), (3, 1)]
FF_CHUNKS = 3
ROW_TILE = 256
FULL_TILE = 256


def ring_place(place, shards):
    place = place % shards
    column = place // (shards // 2)
    return 2 * (place + column * (shards - 1 - 2 * place)) + column


def place_of(index, shards):
    row, column = index // 2, index % 2
    return row + column * (shards - 1 - 2 * row)


def ring_pairs(shards, step):
    return [
        (ring_place(place, shards), ring_place(place + step + shards, shards))
        for place in range(shards)
    ]


def spread(pieces, shards):
    return [pieces[0]] + [
        lax.ppermute(pieces[shards - step], "fsdp", ring_pairs(shards, step))
        for step in range(1, shards)
    ]


def row_scale(values):
    return lax.rsqrt(jnp.mean(values * values, axis=-1, keepdims=True) + EPSILON)


def row_call(body, scalars, arrays, gains, outs, sums=0, cost=8):
    tokens, width = arrays[0].shape
    tiles = tokens // ROW_TILE
    row = pl.BlockSpec((ROW_TILE, width), lambda tile, *_: (tile, 0))
    whole = pl.BlockSpec((1, width), lambda tile, *_: (0, 0))
    return pl.pallas_call(
        body,
        grid_spec=pltpu.PrefetchScalarGridSpec(
            num_scalar_prefetch=1,
            grid=(tiles,),
            in_specs=[row] * len(arrays)
            + [whole] * len(gains),
            out_specs=[row] * len(outs) + [whole] * sums,
        ),
        out_shape=[jax.ShapeDtypeStruct((tokens, width), kind) for kind in outs]
        + [jax.ShapeDtypeStruct((1, width), jnp.float32)] * sums,
        cost_estimate=pl.CostEstimate(
            flops=cost * tokens * width, bytes_accessed=3 * cost * tokens * width // 2, transcendentals=0
        ),
        name=body.__name__,
    )(scalars, *arrays, *gains)


def turned_in(scalars, x_ref, g_ref, gain_ref, xr_ref, gr_ref, n_ref):
    shards = scalars.shape[0] - 1
    width = x_ref.shape[1] // shards
    scale = row_scale(x_ref[...].astype(jnp.float32))
    for at in range(shards):
        source = pl.ds(pl.multiple_of(scalars[at] * width, 128), width)
        target = slice(at * width, (at + 1) * width)
        values = x_ref[:, source]
        xr_ref[:, target] = values
        gr_ref[:, target] = g_ref[:, source]
        n_ref[:, target] = (values.astype(jnp.float32) * scale * gain_ref[:, target]).astype(
            n_ref.dtype
        )


def layer_out(scalars, mid_ref, came_ref, out_ref):
    shards = scalars.shape[0] - 1
    width = mid_ref.shape[1] // shards
    value = mid_ref[...] + came_ref[...].astype(jnp.float32)
    for at in range(shards):
        out_ref[:, pl.ds(pl.multiple_of(scalars[at] * width, 128), width)] = value[
            :, at * width : (at + 1) * width
        ]


def norm_grad(values, grad, gain, sum_ref):
    scale = row_scale(values)
    unit = values * scale
    inner = grad * gain

    @pl.when(pl.program_id(0) == 0)
    def _():
        sum_ref[...] = jnp.zeros_like(sum_ref)

    sum_ref[...] += jnp.sum(grad * unit, axis=0, keepdims=True)
    return scale * (inner - unit * jnp.mean(inner * unit, axis=-1, keepdims=True))


def second_back(scalars, mid_ref, g_ref, came_ref, gain_ref, dx_ref, low_ref, sum_ref):
    grad = came_ref[...].astype(jnp.float32)
    value = g_ref[...].astype(jnp.float32) + norm_grad(mid_ref[...], grad, gain_ref[...], sum_ref)
    dx_ref[...] = value
    low_ref[...] = value.astype(low_ref.dtype)


def first_back(scalars, dx_ref, x_ref, came_ref, gain_ref, out_ref, sum_ref):
    shards = scalars.shape[0] - 1
    width = x_ref.shape[1] // shards
    grad = came_ref[...].astype(jnp.float32)
    value = dx_ref[...] + norm_grad(
        x_ref[...].astype(jnp.float32), grad, gain_ref[...], sum_ref
    )
    for at in range(shards):
        out_ref[:, pl.ds(pl.multiple_of(scalars[at] * width, 128), width)] = value[
            :, at * width : (at + 1) * width
        ]


def full_call(body, scalars, lefts, matrix, window, outs, halves, name):
    tokens = lefts[0].shape[0]
    tiles = tokens // FULL_TILE
    half = tiles // 2
    columns, at = window

    def turned(step, scalars):
        return (lax.rem(step + scalars[scalars.shape[0] - 1] * half, tiles), 0)

    def kernel(scalars, *refs):
        left_refs, whole = refs[: len(lefts)], refs[len(lefts)]
        out_refs = refs[len(lefts) + 1 : len(lefts) + 1 + len(outs)]
        half_refs = refs[len(lefts) + 1 + len(outs) :]
        step = pl.program_id(0)
        values = body(left_refs, whole, out_refs)
        for place, value in enumerate(values):
            kept, sent = half_refs[2 * place : 2 * place + 2]

            @pl.when(step < half)
            def _():
                kept[...] = value.astype(kept.dtype)

            @pl.when(step >= half)
            def _():
                sent[...] = value.astype(sent.dtype)

    def row_spec(width):
        return pl.BlockSpec((FULL_TILE, width), turned)

    half_out = []
    for width, _ in halves:
        half_out.append(
            pl.BlockSpec((FULL_TILE, width), lambda step, _: (jnp.minimum(step, half - 1), 0))
        )
        half_out.append(
            pl.BlockSpec((FULL_TILE, width), lambda step, _: (jnp.maximum(step - half, 0), 0))
        )
    work = 2 * tokens * matrix.shape[0] * columns
    return pl.pallas_call(
        kernel,
        grid_spec=pltpu.PrefetchScalarGridSpec(
            num_scalar_prefetch=1,
            grid=(tiles,),
            in_specs=[row_spec(left.shape[1]) for left in lefts]
            + [pl.BlockSpec((matrix.shape[0], columns), lambda step, _: (0, at))],
            out_specs=[row_spec(width) for width, _ in outs] + half_out,
        ),
        out_shape=[jax.ShapeDtypeStruct((tokens, width), kind) for width, kind in outs]
        + [
            jax.ShapeDtypeStruct((tokens // 2, width), kind)
            for width, kind in halves
            for _ in range(2)
        ],
        cost_estimate=pl.CostEstimate(flops=work, bytes_accessed=work // 250, transcendentals=0),
        name=name,
    )(scalars, *lefts, matrix)


def rows_times(left, right):
    return jnp.dot(left, right, preferred_element_type=jnp.float32)


def project_body(cuts, lefts, whole, outs):
    start = 0
    for out, stop in zip(outs, cuts):
        out[...] = rows_times(lefts[0][...], whole[:, start:stop]).astype(out.dtype)
        start = stop
    return []


def back_body(lefts, whole, outs):
    start, value = 0, None
    for left in lefts:
        stop = start + left.shape[1]
        term = contract_cols(left[...], whole[:, start:stop])
        value = term if value is None else value + term
        start = stop
    return [value]


def adam_body(places, grad_ref, *refs):
    count = len({place[0] for place in places})
    states, outs = refs[: 3 * count], refs[3 * count :]
    start = 0
    for array, plane in places:
        at = (Ellipsis,) if plane is None else (plane,)
        weight, mean, square = (states[3 * array + kind][at] for kind in range(3))
        stop = start + weight.shape[-1]
        grad = grad_ref[:, start:stop]
        step, mean_next, square_next = adam_step(
            weight, grad, mean, square, MATRIX_RATE, WEIGHT_DECAY
        )
        for kind, result in enumerate((grad, step, mean_next, square_next)):
            outs[4 * array + kind][at] = result
        start = stop


def adam_update(grads, places, states, parts=None):
    rows, columns = grads.shape[-2:]
    tile = min(64, rows)
    if parts is None:
        grads, parts = grads[None], 1

    def window(array):
        lead = array.shape[:-2]
        shape = lead + (tile, array.shape[-1] // parts)
        return pl.BlockSpec(shape, lambda part, at: (0,) * len(lead) + (at, part))

    flat = [array for group in states for array in group]
    out_like = [group[0] for group in states for _ in range(4)]
    return pl.pallas_call(
        functools.partial(adam_body, places),
        grid=(parts, rows // tile),
        in_specs=[pl.BlockSpec((None, tile, columns), lambda part, at: (part, at, 0))]
        + [window(array) for array in flat],
        out_specs=[window(array) for array in out_like],
        out_shape=[jax.ShapeDtypeStruct(array.shape, jnp.float32) for array in out_like],
        cost_estimate=pl.CostEstimate(
            flops=20 * parts * rows * columns,
            bytes_accessed=32 * parts * rows * columns,
            transcendentals=0,
        ),
        name="adam_update",
    )(grads, *flat)


class Hops:
    def __init__(self, shards):
        self.shards = shards
        place = place_of(lax.axis_index("fsdp"), shards)
        self.neighbours = [
            {"fsdp": ring_place(place + shards + step, shards)} for step in (1, -1)
        ]
        tensor = lax.axis_index("tensor")
        self.core = lax.rem(tensor, 2)
        chip = tensor // 2
        self.partner = {"tensor": 2 * chip + 1 - self.core}
        self.across = {"tensor": 2 * (1 - chip) + self.core}

    def meet(self, others):
        barrier = pltpu.get_barrier_semaphore()
        for other in others:
            pl.semaphore_signal(
                barrier, inc=1, device_id=other, device_id_type=pl.DeviceIdType.MESH
            )
        pl.semaphore_wait(barrier, len(others))


def remote(source, target, sent, arrived, device):
    return pltpu.make_async_remote_copy(
        src_ref=source,
        dst_ref=target,
        send_sem=sent,
        recv_sem=arrived,
        device_id=device,
        device_id_type=pl.DeviceIdType.MESH,
    )


class RingGather:
    def __init__(self, hops, own, slots, sems, forward):
        legs = hops.shards // 2
        self.reach = (legs, legs - 1) if forward else (legs - 1, legs)
        self.hops, self.own, self.slots, self.sems = hops, own, slots, sems

    def copy(self, way, step):
        shards = self.hops.shards
        source, target = (step - 1, step) if way == 0 else (shards - step + 1, shards - step)
        return remote(
            self.own if step == 1 else self.slots.at[source],
            self.slots.at[target],
            self.sems[0].at[way, step - 1],
            self.sems[1].at[way, step - 1],
            self.hops.neighbours[way],
        )

    def hop(self, step):
        for way in range(2):
            if 1 < step <= self.reach[way] + 1:
                self.copy(way, step - 1).wait_recv()
            if step <= self.reach[way]:
                self.copy(way, step).start()

    def close(self):
        for way in range(2):
            for step in range(1, self.reach[way] + 1):
                self.copy(way, step).wait_send()


def by_rows(count, body):
    @pl.loop(0, count // ROW_STEP)
    def _(step):
        body(pl.ds(pl.multiple_of(step * ROW_STEP, ROW_STEP), ROW_STEP))


class RingScatter:
    SLOTS = 3

    def __init__(self, hops, partial, sent, came, sems, credits, jobs, plan):
        self.hops, self.partial, self.sent, self.came = hops, partial, sent, came
        self.sems, self.credits, self.jobs = sems, credits, jobs
        self.total = [sum(job[way] for job in jobs) for way in range(2)]
        self.number = [{}, {}]
        for job, step in plan:
            for way in range(2):
                hop = step - (max(jobs[job]) - jobs[job][way])
                if hop >= 1:
                    self.number[way][job, hop] = len(self.number[way])

    def copy(self, way, number):
        slot = number % self.SLOTS
        return remote(
            self.sent.at[way, slot],
            self.came.at[way, slot],
            self.sems[0].at[way, slot],
            self.sems[1].at[way, slot],
            self.hops.neighbours[way],
        )

    def add(self, way, job, hop, base, out):
        number = self.number[way][job, hop]
        self.copy(way, number).wait_recv()
        slot = number % self.SLOTS

        def body(rows):
            out[rows, :] = (
                base[rows, :].astype(jnp.float32) + self.came[way, slot, rows].astype(jnp.float32)
            ).astype(out.dtype)

        by_rows(out.shape[0], body)
        if number + self.SLOTS < self.total[way]:
            pl.semaphore_signal(
                self.credits.at[way],
                inc=1,
                device_id=self.hops.neighbours[1 - way],
                device_id_type=pl.DeviceIdType.MESH,
            )

    def hop(self, job, step):
        longest = max(self.jobs[job])
        for way in range(2):
            reach = self.jobs[job][way]
            hop = step - (longest - reach)
            if hop < 1 or hop > reach:
                continue
            distance = reach - hop + 1
            number = self.number[way][job, hop]
            slot = number % self.SLOTS
            if number >= self.SLOTS:
                self.copy(way, number - self.SLOTS).wait_send()
            self.partial(
                job,
                self.hops.shards - distance if way == 0 else distance,
                self.sent.at[way, slot],
            )
            if hop > 1:
                own = self.sent.at[way, slot]
                self.add(way, job, hop - 1, own, own)
            if number >= self.SLOTS:
                pl.semaphore_wait(self.credits.at[way], 1)
            self.copy(way, number).start()

    def last(self, job, own):
        self.partial(job, 0, own)
        for way in range(2):
            self.add(way, job, self.jobs[job][way], own, own)

    def close(self):
        for way in range(2):
            for number in range(max(0, self.total[way] - self.SLOTS), self.total[way]):
                self.copy(way, number).wait_send()


class CoreSum:
    def __init__(self, hops, sent, kept, first, chip, second, out, sems):
        self.hops, self.sent, self.kept, self.first = hops, sent, kept, first
        self.chip, self.second, self.out, self.sems = chip, second, out, sems
        self.half = chip.shape[0]

    def copy(self, stage):
        rows = self.out.at[pl.ds(pl.multiple_of(self.hops.core * self.half, 128), self.half)]
        source, target, device = (
            (self.sent, self.first, self.hops.partner),
            (self.chip, self.second, self.hops.across),
            (self.chip, rows, self.hops.partner),
        )[stage]
        return remote(source, target, self.sems.at[0, stage], self.sems.at[1, stage], device)

    def local(self):
        rows = self.out.at[pl.ds(pl.multiple_of(self.hops.core * self.half, 128), self.half)]
        return pltpu.make_async_copy(self.chip, rows, self.sems.at[0, 3])

    def add(self, left, right):
        def body(rows):
            self.chip[rows, :] = (
                left[rows, :].astype(jnp.float32) + right[rows, :].astype(jnp.float32)
            ).astype(jnp.bfloat16)

        by_rows(self.half, body)

    def start(self):
        self.copy(0).start()

    def to_chip(self):
        self.copy(0).wait_recv()
        self.add(self.kept, self.first)
        self.copy(1).start()

    def to_all(self):
        self.copy(1).wait()
        self.add(self.chip, self.second)
        self.copy(2).start()
        self.local().start()

    def done(self):
        self.copy(0).wait_send()
        self.copy(2).wait()
        self.local().wait()


RING_LIMIT = 66500000


def gather_body(shards, own_ref, small_ref, out_ref, few_ref, *sems):
    hops = Hops(shards)
    hops.meet(hops.neighbours)
    few = RingGather(hops, small_ref, few_ref, sems[2:4], True)
    big = RingGather(hops, own_ref, out_ref, sems[0:2], True)
    rings = (few, big)
    copies = [
        pltpu.make_async_copy(own_ref, out_ref.at[0], sems[4].at[0]),
        pltpu.make_async_copy(small_ref, few_ref.at[0], sems[4].at[1]),
    ]
    for step in range(1, shards // 2 + 2):
        for ring in rings:
            ring.hop(step)
        if step == 1:
            for copy in copies:
                copy.start()
    for ring in rings:
        ring.close()
    for copy in copies:
        copy.wait()


def gather_call(own, small, shards):
    legs = shards // 2
    return pl.pallas_call(
        functools.partial(gather_body, shards),
        in_specs=[pl.BlockSpec(memory_space=pl.ANY)] * 2,
        out_specs=[pl.BlockSpec(memory_space=pl.ANY)] * 2,
        out_shape=[
            jax.ShapeDtypeStruct((shards, *array.shape), array.dtype) for array in (own, small)
        ],
        scratch_shapes=[pltpu.SemaphoreType.DMA((2, legs))] * 4
        + [pltpu.SemaphoreType.DMA((2,))],
        compiler_params=pltpu.CompilerParams(collective_id=0, has_side_effects=True),
        name="gather_ring",
    )(own, small)


FF_TILE = 256
ROW_STEP = 32


def ff_kernel(shards, parts, *refs):
    (sent_ref, kept_ref, x_ref, grad_ref, gain_ref, own_ref) = refs[:6]
    (mid_ref, norm_out, normsum_ref, downsum_ref, grads_ref, whole_ref) = refs[6:12]
    (acts, whole, pairs, norm_acc, r_sent, r_came, total) = refs[12:19]
    (out_half, kept_half, chip, first) = refs[19:23]
    seconds = refs[23:25]
    (x_tile, mid_tile) = refs[25:27]
    (ag_sent, ag_came, rs_sent, rs_came, credits, sums, local) = refs[27:]
    hops = Hops(shards)
    hops.meet([*hops.neighbours, hops.partner, hops.across])
    core = hops.core
    tokens, wide = x_ref.shape
    half = tokens // 2
    columns = pairs.shape[2]
    width = wide // shards
    legs = shards // 2
    gathers = [
        RingGather(
            hops,
            own_ref.at[part],
            whole_ref.at[part],
            (ag_sent.at[part], ag_came.at[part]),
            part % 2 == 0,
        )
        for part in range(parts)
    ]

    def partial(job, at, out):
        @pl.loop(0, 3)
        def _(pair):
            left = acts[pair // 2, :, at * width : (at + 1) * width]
            right = pairs[3 * job + pair]
            out[:, pl.ds(pl.multiple_of(pair * columns, 128), columns)] = contract_rows(
                left, right
            ).astype(out.dtype)

    scatter = RingScatter(
        hops,
        partial,
        r_sent,
        r_came,
        (rs_sent, rs_came),
        credits,
        [(legs, legs - 1) if part % 2 == 0 else (legs - 1, legs) for part in range(parts)],
        [(part, step) for part in range(parts) for step in range(1, legs + 1)],
    )
    attention = CoreSum(
        hops, sent_ref, kept_half, first, chip, seconds[0], acts.at[0], sums.at[0]
    )
    attention.start()
    take_kept = pltpu.make_async_copy(kept_ref, kept_half, local.at[0])
    take_grad = pltpu.make_async_copy(grad_ref, acts.at[1], local.at[1])
    take_kept.start()
    take_grad.start()
    gathers[0].hop(1)
    take_kept.wait()
    attention.to_chip()
    gathers[0].hop(2)
    gathers[0].hop(3)
    gathers[0].hop(4)
    gathers[1].hop(1)
    attention.to_all()
    attention.done()

    @pl.loop(0, tokens // FF_TILE)
    def _(tile):
        rows = pl.ds(pl.multiple_of(tile * FF_TILE, FF_TILE), FF_TILE)
        take = pltpu.make_async_copy(x_ref.at[rows], x_tile, local.at[2])
        take.start()
        take.wait()
        middle = x_tile[...].astype(jnp.float32) + acts[0, rows, :].astype(jnp.float32)
        mid_tile[...] = middle
        put = pltpu.make_async_copy(mid_tile, mid_ref.at[rows], local.at[2])
        put.start()
        acts[0, rows, :] = (middle * row_scale(middle) * gain_ref[...]).astype(jnp.bfloat16)
        put.wait()

    gathers[0].hop(5)
    take_grad.wait()

    def load(part):
        copies = [
            pltpu.make_async_copy(
                own_ref.at[part] if at == 0 else whole_ref.at[part, at],
                whole.at[pl.ds(at * width, width)],
                local.at[3 + at],
            )
            for at in range(shards)
        ]
        for copy in copies:
            copy.start()
        for copy in copies:
            copy.wait()

    def tiles(part, start, stop):
        @pl.loop(start, stop)
        def _(tile):
            rows = pl.ds(pl.multiple_of(tile * FF_TILE, FF_TILE), FF_TILE)
            norm = acts[0, rows, :]
            grad = acts[1, rows, :]
            gate_proj = rows_times(norm, whole[:, :columns])
            up_proj = rows_times(norm, whole[:, columns : 2 * columns])
            hidden_grad = rows_times(grad, whole[:, 2 * columns :])
            gate = 1.0 / (1.0 + jnp.exp(-gate_proj))
            swish = gate_proj * gate
            gate_grad = (
                hidden_grad * up_proj * (gate * (1.0 + gate_proj * (1.0 - gate)))
            ).astype(jnp.bfloat16)
            up_grad = (hidden_grad * swish).astype(jnp.bfloat16)
            pairs[3 * part, rows, :] = gate_grad
            pairs[3 * part + 1, rows, :] = up_grad
            pairs[3 * part + 2, rows, :] = (swish * up_proj).astype(jnp.bfloat16)
            value = contract_cols(gate_grad, whole[:, :columns]) + contract_cols(
                up_grad, whole[:, columns : 2 * columns]
            )
            if part > 0:
                value += norm_acc[rows, :]
            norm_acc[rows, :] = value

    count = tokens // FF_TILE
    load(0)
    tiles(0, 0, 2)
    gathers[1].hop(2)
    tiles(0, 2, count)
    gathers[1].hop(3)
    gathers[1].hop(4)
    gathers[2].hop(1)
    gathers[1].hop(5)
    load(1)
    tiles(1, 0, 2)
    gathers[2].hop(2)
    tiles(1, 2, count)
    gathers[2].hop(3)
    scatter.hop(0, 1)
    gathers[2].hop(4)
    scatter.hop(0, 2)
    gathers[2].hop(5)
    load(2)
    tiles(2, 0, 2)
    scatter.hop(0, 3)
    tiles(2, 2, count)
    scatter.hop(0, 4)
    scatter.hop(1, 1)

    def finish(part):
        scatter.last(part, total)
        put = pltpu.make_async_copy(total, grads_ref.at[part], local.at[2])
        put.start()
        put.wait()

    mine = pl.ds(pl.multiple_of(core * half, 128), half)
    other = pl.ds(pl.multiple_of((1 - core) * half, 128), half)
    out_half[...] = norm_acc[other, :].astype(jnp.bfloat16)
    norm_sum = CoreSum(
        hops, out_half, norm_acc.at[mine], first, chip, seconds[1], normsum_ref, sums.at[1]
    )
    norm_sum.start()
    finish(0)
    scatter.hop(1, 2)
    norm_sum.to_chip()

    downs = [
        pltpu.make_async_copy(
            (own_ref.at[part] if at == 0 else whole_ref.at[part, at]).at[
                :, pl.ds(2 * columns, columns)
            ],
            whole.at[pl.ds(at * width, width), pl.ds(part * columns, columns)],
            local.at[3 + at],
        )
        for part in range(parts)
        for at in range(shards)
    ]
    for part in range(parts):
        for copy in downs[part * shards : (part + 1) * shards]:
            copy.start()
        for copy in downs[part * shards : (part + 1) * shards]:
            copy.wait()
    scatter.hop(1, 3)
    scatter.hop(1, 4)
    scatter.hop(2, 1)
    norm_sum.to_all()
    finish(1)
    scatter.hop(2, 2)
    norm_sum.done()

    def down_tile(tile, offset):
        rows = pl.ds(pl.multiple_of(offset + tile * FF_TILE, FF_TILE), FF_TILE)
        value = contract_cols(pairs[2, rows, :], whole[:, :columns])
        for part in range(1, parts):
            value += contract_cols(
                pairs[3 * part + 2, rows, :], whole[:, part * columns : (part + 1) * columns]
            )
        return value

    @pl.loop(0, half // FF_TILE)
    def _(tile):
        rows = pl.ds(pl.multiple_of(tile * FF_TILE, FF_TILE), FF_TILE)
        out_half[rows, :] = down_tile(tile, (1 - core) * half).astype(jnp.bfloat16)

    down_sum = CoreSum(
        hops, out_half, kept_half, first, chip, seconds[0], downsum_ref, sums.at[2]
    )
    down_sum.start()

    @pl.loop(0, half // FF_TILE)
    def _(tile):
        rows = pl.ds(pl.multiple_of(tile * FF_TILE, FF_TILE), FF_TILE)
        kept_half[rows, :] = down_tile(tile, core * half).astype(jnp.bfloat16)

    down_sum.to_chip()
    scatter.hop(2, 3)
    scatter.hop(2, 4)
    down_sum.to_all()
    put_norm = pltpu.make_async_copy(acts.at[0], norm_out, local.at[0])
    put_norm.start()
    finish(2)
    down_sum.done()
    put_norm.wait()
    for gather in gathers:
        gather.close()
    scatter.close()


def ff_call(sent, kept, rows, grad, gain, own):
    parts, width, columns3 = own.shape
    tokens, wide = rows.shape
    shards = wide // width
    columns = columns3 // 3
    half = tokens // 2
    legs = shards // 2
    low = jnp.bfloat16
    anywhere = pl.BlockSpec(memory_space=pl.ANY)
    slots = RingScatter.SLOTS
    return pl.pallas_call(
        functools.partial(ff_kernel, shards, parts),
        in_specs=[anywhere] * 4 + [pl.BlockSpec(memory_space=pltpu.VMEM)] + [anywhere],
        out_specs=[anywhere] * 6,
        out_shape=[
            jax.ShapeDtypeStruct((tokens, wide), jnp.float32),
            jax.ShapeDtypeStruct((tokens, wide), low),
            jax.ShapeDtypeStruct((tokens, wide), low),
            jax.ShapeDtypeStruct((tokens, wide), low),
            jax.ShapeDtypeStruct((parts, width, columns3), jnp.float32),
            jax.ShapeDtypeStruct((parts, shards, width, columns3), low),
        ],
        scratch_shapes=[
            pltpu.VMEM((2, tokens, wide), low),
            pltpu.VMEM((wide, columns3), low),
            pltpu.VMEM((3 * parts, tokens, columns), low),
            pltpu.VMEM((tokens, wide), jnp.float32),
            pltpu.VMEM((2, slots, width, columns3), low),
            pltpu.VMEM((2, slots, width, columns3), low),
            pltpu.VMEM((width, columns3), jnp.float32),
        ]
        + [pltpu.VMEM((half, wide), low)] * 6
        + [
            pltpu.VMEM((FF_TILE, wide), low),
            pltpu.VMEM((FF_TILE, wide), jnp.float32),
            pltpu.SemaphoreType.DMA((parts, 2, legs)),
            pltpu.SemaphoreType.DMA((parts, 2, legs)),
            pltpu.SemaphoreType.DMA((2, slots)),
            pltpu.SemaphoreType.DMA((2, slots)),
            pltpu.SemaphoreType.REGULAR((2,)),
            pltpu.SemaphoreType.DMA((3, 2, 4)),
            pltpu.SemaphoreType.DMA((3 + shards,)),
        ],
        compiler_params=pltpu.CompilerParams(
            collective_id=1, has_side_effects=True, vmem_limit_bytes=RING_LIMIT
        ),
        name="ff_ring",
    )(sent, kept, rows, grad, gain, own)


def tail_kernel(shards, jobs, *refs):
    (sent_ref, kept_ref, norm_ref, grad_ref) = refs[:4]
    rights = refs[4:8]
    (sum_ref, grads_ref, acts, r_sent, r_came, total) = refs[8:14]
    (kept_half, chip, first, second) = refs[14:18]
    (rs_sent, rs_came, credits, sums, local) = refs[18:]
    hops = Hops(shards)
    hops.meet([*hops.neighbours, hops.partner, hops.across])
    wide = norm_ref.shape[1]
    width = wide // shards
    legs = shards // 2

    def partial(job, at, out):
        start = 0
        for left, right in jobs[job]:
            stop = start + rights[right].shape[1]
            out[:, start:stop] = contract_rows(
                acts[left, :, at * width : (at + 1) * width], rights[right][...]
            ).astype(out.dtype)
            start = stop

    scatter = RingScatter(
        hops,
        partial,
        r_sent,
        r_came,
        (rs_sent, rs_came),
        credits,
        [(legs, legs - 1) if job % 2 == 0 else (legs - 1, legs) for job in range(len(jobs))],
        [(job, step) for step in range(1, legs + 1) for job in range(len(jobs))],
    )
    take = [
        pltpu.make_async_copy(ref, target, local.at[at])
        for at, (ref, target) in enumerate(
            [(kept_ref, kept_half), (norm_ref, acts.at[0]), (grad_ref, acts.at[1])]
        )
    ]
    norm_sum = CoreSum(
        hops, sent_ref, kept_half, first, chip, second, sum_ref, sums.at[0]
    )
    norm_sum.start()
    for copy in take:
        copy.start()
    for copy in take:
        copy.wait()
    scatter.hop(0, 1)
    scatter.hop(1, 1)
    norm_sum.to_chip()
    scatter.hop(0, 2)
    scatter.hop(1, 2)
    scatter.hop(0, 3)
    scatter.hop(1, 3)
    scatter.hop(0, 4)
    scatter.hop(1, 4)
    norm_sum.to_all()
    for job in range(2):
        scatter.last(job, total)
        put = pltpu.make_async_copy(total, grads_ref.at[job], local.at[0])
        put.start()
        put.wait()
    norm_sum.done()
    scatter.close()


def tail_call(sent, kept, norm, grad, rights, jobs, shards):
    tokens, wide = norm.shape
    half, width, legs = tokens // 2, wide // shards, shards // 2
    columns = sum(rights[right].shape[1] for _, right in jobs[0])
    low = jnp.bfloat16
    anywhere = pl.BlockSpec(memory_space=pl.ANY)
    slots = RingScatter.SLOTS
    return pl.pallas_call(
        functools.partial(tail_kernel, shards, jobs),
        in_specs=[anywhere] * 4 + [pl.BlockSpec(memory_space=pltpu.VMEM)] * len(rights),
        out_specs=[anywhere] * 2,
        out_shape=[
            jax.ShapeDtypeStruct((tokens, wide), low),
            jax.ShapeDtypeStruct((len(jobs), width, columns), jnp.float32),
        ],
        scratch_shapes=[
            pltpu.VMEM((2, tokens, wide), low),
            pltpu.VMEM((2, slots, width, columns), low),
            pltpu.VMEM((2, slots, width, columns), low),
            pltpu.VMEM((width, columns), jnp.float32),
        ]
        + [pltpu.VMEM((half, wide), low)] * 4
        + [
            pltpu.SemaphoreType.DMA((2, slots)),
            pltpu.SemaphoreType.DMA((2, slots)),
            pltpu.SemaphoreType.REGULAR((2,)),
            pltpu.SemaphoreType.DMA((1, 2, 4)),
            pltpu.SemaphoreType.DMA((3,)),
        ],
        compiler_params=pltpu.CompilerParams(
            collective_id=2, has_side_effects=True, vmem_limit_bytes=48 * 1024 * 1024
        ),
        name="tail_ring",
    )(sent, kept, norm, grad, *rights)


def ring_device(
    shards,
    layer_input,
    out_grad,
    segment_ids,
    query_weight,
    key_weight,
    value_matrix,
    output_weight,
    gate_up_weight,
    down_weight,
    norm_gains,
    headnorm_gains,
    query_weight_mean,
    key_weight_first_moment,
    value_weight_first_moment,
    output_weight_mean,
    gate_up_weight_mean,
    down_weight_mean,
    norm_gains_mean,
    headnorm_gains_mean,
    query_weight_square,
    key_weight_second_moment,
    value_weight_second_moment,
    output_weight_square,
    gate_up_weight_square,
    down_weight_square,
    norm_gains_square,
    headnorm_gains_square,
):
    place = place_of(lax.axis_index("fsdp"), shards)
    core = lax.axis_index("tensor") % 2
    turn = jnp.stack([ring_place(place - at + shards, shards) for at in range(shards)])
    turn = turn.astype(jnp.int32)
    scalars = jnp.concatenate([turn, core[None].astype(jnp.int32)])
    back = (place - place_of(jnp.arange(shards), shards)) % shards

    gain_cols, head_cols = norm_gains.shape[1], headnorm_gains.shape[1]
    low = jnp.bfloat16
    packed_token_count, width = layer_input.shape
    query_cols, key_cols = query_weight.shape[1], key_weight.shape[1]
    local_query = query_cols // HEAD_SIZE
    local_groups = key_cols // HEAD_SIZE
    query_group_width = local_query // local_groups
    score_scale = 1.0 / math.sqrt(HEAD_SIZE)
    chunk_cols = down_weight.shape[1] // FF_CHUNKS
    states = [
        (query_weight, query_weight_mean, query_weight_square),
        (key_weight, key_weight_first_moment, key_weight_second_moment),
        (value_matrix, value_weight_first_moment, value_weight_second_moment),
        (output_weight, output_weight_mean, output_weight_square),
        (gate_up_weight, gate_up_weight_mean, gate_up_weight_square),
        (down_weight, down_weight_mean, down_weight_square),
        (norm_gains, norm_gains_mean, norm_gains_square),
        (headnorm_gains, headnorm_gains_mean, headnorm_gains_square),
    ]

    attention_block = jnp.concatenate(
        [
            query_weight.astype(low),
            key_weight.astype(low),
            value_matrix.astype(low),
            output_weight.astype(low),
        ],
        axis=1,
    )
    own_gains = jnp.concatenate([norm_gains, headnorm_gains], axis=1).astype(low)
    own_gains = jnp.pad(own_gains, ((0, 14), (0, -own_gains.shape[1] % 128)))
    attention_full, gains = gather_call(attention_block, own_gains, shards)
    attention_full = attention_full.reshape(width, -1)
    gains = jnp.swapaxes(gains[:, :2].astype(jnp.float32), 0, 1)
    norm_gain = gains[:, :, :gain_cols].reshape(2, 1, -1)
    head_gain = gains[:, :, gain_cols : gain_cols + head_cols][:, back].reshape(2, -1)
    inward_window = (query_cols + 2 * key_cols, 0)
    outward_window = (query_cols, (query_cols + 2 * key_cols) // query_cols)
    ff_block = jnp.stack(
        [
            jnp.concatenate(
                [
                    gate_up_weight[0, :, cols].astype(low),
                    gate_up_weight[1, :, cols].astype(low),
                    down_weight[:, cols].astype(low),
                ],
                axis=1,
            )
            for cols in (
                slice(chunk * chunk_cols, (chunk + 1) * chunk_cols) for chunk in range(FF_CHUNKS)
            )
        ]
    )
    token_positions = positions_of(segment_ids)
    token_index = jnp.arange(packed_token_count, dtype=jnp.int32)

    def head_map(projected, gain, heads):
        return rotary_embedding(
            root_mean_scale(projected.reshape(packed_token_count, heads, HEAD_SIZE)) * gain,
            token_positions,
        )

    input_rows, grad_low, normed_one = row_call(
        turned_in, scalars, [layer_input, out_grad], [norm_gain[0]], [low, low, low]
    )
    query_proj, key_projected, value_projected = full_call(
        functools.partial(
            project_body, (query_cols, query_cols + key_cols, query_cols + 2 * key_cols)
        ),
        scalars,
        [normed_one],
        attention_full,
        inward_window,
        [(query_cols, jnp.float32), (key_cols, jnp.float32), (key_cols, low)],
        [],
        "project",
    )
    query_heads = (
        head_map(query_proj, head_gain[0], local_query)
        .astype(low)
        .reshape(packed_token_count, local_groups, query_group_width, HEAD_SIZE)
    )
    per_head_keys = head_map(key_projected, head_gain[1], local_groups).astype(low)
    per_head_values = value_projected.reshape(packed_token_count, local_groups, HEAD_SIZE)
    block_rows = min(512, packed_token_count)
    block_count = packed_token_count // block_rows

    def block_scores(row_start, row_stop):
        raw_scores = (
            jnp.einsum(
                "qhgd,khd->hgqk",
                query_heads[row_start:row_stop],
                per_head_keys[:row_stop],
                preferred_element_type=jnp.float32,
            )
            * score_scale
        )
        allowed = (segment_ids[row_start:row_stop, None] == segment_ids[None, :row_stop]) & (
            token_index[None, :row_stop] <= token_index[row_start:row_stop, None]
        )
        return jnp.where(allowed, raw_scores, MASKED)

    mixed_blocks = []
    log_sums = []
    for block_index in range(block_count):
        row_start = block_index * block_rows
        row_stop = row_start + block_rows
        scores = block_scores(row_start, row_stop)
        row_max = jnp.max(scores, axis=-1, keepdims=True)
        exponent = jnp.exp(scores - row_max)
        row_sum = jnp.sum(exponent, axis=-1, keepdims=True)
        weights_block = (exponent / row_sum).astype(low)
        log_sums.append(row_max + jnp.log(row_sum))
        mixed_blocks.append(
            jnp.einsum(
                "hgqk,khd->qhgd",
                weights_block,
                per_head_values[:row_stop],
                preferred_element_type=jnp.float32,
            )
        )
    mixed = (
        jnp.concatenate(mixed_blocks, axis=0)
        .reshape(packed_token_count, local_query * HEAD_SIZE)
        .astype(low)
    )
    kept, sent = full_call(
        back_body, scalars, [mixed], attention_full, outward_window, [], [(width, low)], "attention_out"
    )
    middle, normed_two, norm_sum, down_sum, ff_sums, _ = ff_call(
        sent, kept, input_rows, grad_low, norm_gain[1], ff_block
    )
    middle_grad, middle_grad_low, gain_two_grad = row_call(
        second_back,
        scalars,
        [middle, grad_low, norm_sum],
        [norm_gain[1]],
        [jnp.float32, low],
        sums=1,
    )
    (mixed_grad,) = full_call(
        functools.partial(project_body, (query_cols,)),
        scalars,
        [middle_grad_low],
        attention_full,
        outward_window,
        [(query_cols, low)],
        [],
        "mixed_back",
    )
    mixed_grad = mixed_grad.reshape(packed_token_count, local_groups, query_group_width, HEAD_SIZE)
    query_grad_blocks = []
    key_grad_acc = jnp.zeros((packed_token_count, local_groups, HEAD_SIZE), jnp.float32)
    value_grad_acc = jnp.zeros((packed_token_count, local_groups, HEAD_SIZE), jnp.float32)
    for block_index in range(block_count):
        row_start = block_index * block_rows
        row_stop = row_start + block_rows
        scores = block_scores(row_start, row_stop)
        probs = jnp.exp(scores - log_sums[block_index])
        grad_block = mixed_grad[row_start:row_stop]
        prob_grad = jnp.einsum(
            "qhgd,khd->hgqk",
            grad_block,
            per_head_values[:row_stop],
            preferred_element_type=jnp.float32,
        )
        row_inner = jnp.sum(probs * prob_grad, axis=-1, keepdims=True)
        score_grad = (probs * (prob_grad - row_inner)).astype(low)
        query_grad_blocks.append(
            jnp.einsum(
                "hgqk,khd->qhgd",
                score_grad,
                per_head_keys[:row_stop],
                preferred_element_type=jnp.float32,
            )
            * score_scale
        )
        key_grad_acc = key_grad_acc.at[:row_stop].add(
            jnp.einsum(
                "hgqk,qhgd->khd",
                score_grad,
                query_heads[row_start:row_stop],
                preferred_element_type=jnp.float32,
            )
            * score_scale
        )
        value_grad_acc = value_grad_acc.at[:row_stop].add(
            jnp.einsum(
                "hgqk,qhgd->khd",
                probs.astype(low),
                grad_block,
                preferred_element_type=jnp.float32,
            )
        )
    query_grad_heads = (
        jnp.concatenate(query_grad_blocks, axis=0)
        .reshape(packed_token_count, local_query, HEAD_SIZE)
        .astype(low)
        .astype(jnp.float32)
    )
    key_grad_heads = key_grad_acc.astype(low).astype(jnp.float32)
    value_grad_low = value_grad_acc.astype(low).reshape(
        packed_token_count, local_groups * HEAD_SIZE
    )
    query_map_out, query_map_back = jax.vjp(
        lambda projected, gain: head_map(projected, gain, local_query), query_proj, head_gain[0]
    )
    query_proj_grad, head_query_grad = query_map_back(query_grad_heads)
    key_map_out, key_map_back = jax.vjp(
        lambda projected, gain: head_map(projected, gain, local_groups), key_projected, head_gain[1]
    )
    key_proj_grad, head_key_grad = key_map_back(key_grad_heads)
    query_proj_low = query_proj_grad.astype(low)
    key_proj_low = key_proj_grad.astype(low)
    kept, sent = full_call(
        back_body,
        scalars,
        [query_proj_low, key_proj_low, value_grad_low],
        attention_full,
        inward_window,
        [],
        [(width, low)],
        "projection_back",
    )
    norm_one_sum, attention_sums = tail_call(
        sent,
        kept,
        normed_one,
        middle_grad_low,
        [query_proj_low, key_proj_low, value_grad_low, mixed],
        (((0, 0), (0, 1)), ((0, 2), (1, 3))),
        shards,
    )
    (layer_output,) = row_call(layer_out, scalars, [middle, down_sum], [], [jnp.float32])
    head_grads = jnp.stack([head_query_grad, head_key_grad])
    head_grads = head_grads + lax.ppermute(head_grads, "tensor", CORE_PAIRS)
    head_grads = head_grads + lax.ppermute(head_grads, "tensor", CHIP_PAIRS)
    head_pieces = head_grads.reshape(2, shards, head_cols)[:, turn]
    early_pieces = [
        jnp.concatenate(
            [
                gain_two_grad[:, at * gain_cols : (at + 1) * gain_cols],
                head_pieces[0:1, at],
                head_pieces[1:2, at],
            ],
            axis=1,
        )
        for at in range(shards)
    ]
    early_sum = functools.reduce(jnp.add, spread(early_pieces, shards))
    input_grad, gain_one_grad = row_call(
        first_back,
        scalars,
        [middle_grad, input_rows, norm_one_sum],
        [norm_gain[0]],
        [jnp.float32],
        sums=1,
    )
    late_pieces = spread(
        [gain_one_grad[:, at * gain_cols : (at + 1) * gain_cols] for at in range(shards)], shards
    )
    ff_updates = adam_update(
        ff_sums, [(0, 0), (0, 1), (1, None)], states[4:6], parts=FF_CHUNKS
    )
    inner_updates = adam_update(attention_sums[0], [(0, None), (1, None)], states[0:2])
    outer_updates = adam_update(attention_sums[1], [(0, None), (1, None)], states[2:4])
    late_sum = functools.reduce(jnp.add, late_pieces)
    gain_shards = [
        jnp.concatenate([late_sum, early_sum[:, :gain_cols]], axis=0),
        early_sum[:, gain_cols:].reshape(2, head_cols),
    ]
    updates = [inner_updates[:4], inner_updates[4:], outer_updates[:4], outer_updates[4:]]
    updates += [ff_updates[:4], ff_updates[4:]]
    for (weight, mean, square), grad in zip(states[6:], gain_shards):
        updates.append([grad, *adam_step(weight, grad, mean, square, GAIN_RATE, 0.0)])
    return tuple([layer_output, input_grad] + [update[kind] for kind in range(4) for update in updates])


def solution(mesh):
    shards, parts = mesh.shape["fsdp"], mesh.shape["tensor"]
    ringed = parts == 4 and shards == 8
    return jax.shard_map(
        functools.partial(ring_device, shards) if ringed else plain_device,
        mesh=mesh,
        in_specs=(
            P("fsdp", None),
            P("fsdp", None),
            P("fsdp"),
            P("fsdp", "tensor"),
            P("fsdp", "tensor"),
            P("fsdp", "tensor"),
            P("fsdp", "tensor"),
            P(None, "fsdp", "tensor"),
            P("fsdp", "tensor"),
            P(None, "fsdp"),
            P(None, "fsdp"),
            P("fsdp", "tensor"),
            P("fsdp", "tensor"),
            P("fsdp", "tensor"),
            P("fsdp", "tensor"),
            P(None, "fsdp", "tensor"),
            P("fsdp", "tensor"),
            P(None, "fsdp"),
            P(None, "fsdp"),
            P("fsdp", "tensor"),
            P("fsdp", "tensor"),
            P("fsdp", "tensor"),
            P("fsdp", "tensor"),
            P(None, "fsdp", "tensor"),
            P("fsdp", "tensor"),
            P(None, "fsdp"),
            P(None, "fsdp"),
        ),
        out_specs=(
            P("fsdp", None),
            P("fsdp", None),
            P("fsdp", "tensor"),
            P("fsdp", "tensor"),
            P("fsdp", "tensor"),
            P("fsdp", "tensor"),
            P(None, "fsdp", "tensor"),
            P("fsdp", "tensor"),
            P(None, "fsdp"),
            P(None, "fsdp"),
            P("fsdp", "tensor"),
            P("fsdp", "tensor"),
            P("fsdp", "tensor"),
            P("fsdp", "tensor"),
            P(None, "fsdp", "tensor"),
            P("fsdp", "tensor"),
            P(None, "fsdp"),
            P(None, "fsdp"),
            P("fsdp", "tensor"),
            P("fsdp", "tensor"),
            P("fsdp", "tensor"),
            P("fsdp", "tensor"),
            P(None, "fsdp", "tensor"),
            P("fsdp", "tensor"),
            P(None, "fsdp"),
            P(None, "fsdp"),
            P("fsdp", "tensor"),
            P("fsdp", "tensor"),
            P("fsdp", "tensor"),
            P("fsdp", "tensor"),
            P(None, "fsdp", "tensor"),
            P("fsdp", "tensor"),
            P(None, "fsdp"),
            P(None, "fsdp"),
        ),
        check_vma=False,
    )
```

```python
import functools
import math

import jax
import jax.numpy as jnp
from jax import lax
from jax.experimental import pallas as pl
from jax.experimental.pallas import tpu as pltpu
from jax.sharding import PartitionSpec as P

HEAD_SIZE = 128
MODEL_WIDTH = 2048
ADAM_STEP = 3


EPSILON = 1e-06
ROPE_BASE = 1000000.0
MASKED = -1e30
BETA_ONE = 0.9
BETA_TWO = 0.95
ADAM_EPSILON = 1e-08
MATRIX_RATE = 0.02
GAIN_RATE = 0.1
WEIGHT_DECAY = 0.1


def root_mean_scale(values):
    return values * lax.rsqrt(jnp.mean(values * values, axis=-1, keepdims=True) + EPSILON)


def positions_of(segments):
    earlier = jnp.sum((segments[None, :] < segments[:, None]).astype(jnp.int32), axis=1)
    return jnp.arange(segments.shape[0], dtype=jnp.int32) - earlier


def rotary_embedding(values, token_positions):
    head_width = values.shape[-1]
    half_width = head_width // 2
    frequencies = ROPE_BASE ** (-2.0 * jnp.arange(half_width).astype(values.dtype) / head_width)
    angles = token_positions.astype(values.dtype)[:, None] * frequencies[None, :]
    cosine = jnp.cos(angles)[:, None, :]
    sine_part = jnp.sin(angles)[:, None, :]
    first_half = values[..., :half_width]
    second_half = values[..., half_width:]
    return jnp.concatenate(
        [
            first_half * cosine - second_half * sine_part,
            second_half * cosine + first_half * sine_part,
        ],
        axis=-1,
    )


def contract_rows(left, right):
    return lax.dot_general(
        left, right, (((0,), (0,)), ((), ())), preferred_element_type=jnp.float32
    )


def contract_cols(left, right):
    return lax.dot_general(
        left, right, (((1,), (1,)), ((), ())), preferred_element_type=jnp.float32
    )


def gained_norm(values, gain):
    return root_mean_scale(values) * gain


def swiglu(gate_proj, up_proj):
    return jax.nn.silu(gate_proj) * up_proj


def adam_step(weight, gradient, mean_state, square_state, learn_rate, decay_rate):
    mean_next = BETA_ONE * mean_state + (1.0 - BETA_ONE) * gradient
    square_next = BETA_TWO * square_state + (1.0 - BETA_TWO) * gradient * gradient
    mean_hat = mean_next / (1.0 - BETA_ONE**ADAM_STEP)
    square_hat = square_next / (1.0 - BETA_TWO**ADAM_STEP)
    weight_next = weight - learn_rate * (
        mean_hat / (jnp.sqrt(square_hat) + ADAM_EPSILON) + decay_rate * weight
    )
    return (weight_next - weight, mean_next, square_next)


def plain_device(
    layer_input,
    out_grad,
    segment_ids,
    query_weight,
    key_weight,
    value_matrix,
    output_weight,
    gate_up_weight,
    down_weight,
    norm_gains,
    headnorm_gains,
    query_weight_mean,
    key_weight_first_moment,
    value_weight_first_moment,
    output_weight_mean,
    gate_up_weight_mean,
    down_weight_mean,
    norm_gains_mean,
    headnorm_gains_mean,
    query_weight_square,
    key_weight_second_moment,
    value_weight_second_moment,
    output_weight_square,
    gate_up_weight_square,
    down_weight_square,
    norm_gains_square,
    headnorm_gains_square,
):
    params = (
        query_weight,
        key_weight,
        value_matrix,
        output_weight,
        gate_up_weight,
        down_weight,
        norm_gains,
        headnorm_gains,
    )
    means = (
        query_weight_mean,
        key_weight_first_moment,
        value_weight_first_moment,
        output_weight_mean,
        gate_up_weight_mean,
        down_weight_mean,
        norm_gains_mean,
        headnorm_gains_mean,
    )
    squares = (
        query_weight_square,
        key_weight_second_moment,
        value_weight_second_moment,
        output_weight_square,
        gate_up_weight_square,
        down_weight_square,
        norm_gains_square,
        headnorm_gains_square,
    )
    gain_rows = norm_gains.shape[1]
    gains_low = lax.all_gather(
        jnp.concatenate([norm_gains, headnorm_gains], axis=1).astype(jnp.bfloat16),
        "fsdp",
        axis=0,
    )
    norm_full = jnp.swapaxes(gains_low[:, :, :gain_rows], 0, 1).reshape(2, -1)
    head_full = jnp.swapaxes(gains_low[:, :, gain_rows:], 0, 1).reshape(2, -1)
    query_cols = query_weight.shape[1]
    key_cols = key_weight.shape[1]
    attn_low = jnp.concatenate(
        [query_weight, key_weight, value_matrix, output_weight], axis=1
    ).astype(jnp.bfloat16)
    attn_full = lax.all_gather(attn_low, "fsdp", axis=0, tiled=True)
    query_full = attn_full[:, :query_cols]
    key_full = attn_full[:, query_cols : query_cols + key_cols]
    value_full = attn_full[:, query_cols + key_cols : query_cols + 2 * key_cols]
    output_full = attn_full[:, query_cols + 2 * key_cols :]
    gate_up_full = lax.all_gather(gate_up_weight.astype(jnp.bfloat16), "fsdp", axis=1, tiled=True)
    down_full = lax.all_gather(down_weight.astype(jnp.bfloat16), "fsdp", axis=0, tiled=True)
    norm_gain = norm_full.astype(jnp.float32)
    head_gain = head_full.astype(jnp.float32)
    packed_token_count = layer_input.shape[0]
    local_query = query_full.shape[1] // HEAD_SIZE
    local_groups = key_full.shape[1] // HEAD_SIZE
    query_group_width = local_query // local_groups
    score_scale = 1.0 / math.sqrt(HEAD_SIZE)
    token_positions = positions_of(segment_ids)
    token_index = jnp.arange(packed_token_count, dtype=jnp.int32)
    input_rows = layer_input.astype(jnp.float32)

    def head_map(projected, gain, heads):
        return rotary_embedding(
            root_mean_scale(projected.reshape(packed_token_count, heads, HEAD_SIZE)) * gain,
            token_positions,
        )

    normed_one = gained_norm(input_rows, norm_gain[0]).astype(jnp.bfloat16)
    query_proj = jnp.dot(normed_one, query_full, preferred_element_type=jnp.float32)
    key_projected = jnp.dot(normed_one, key_full, preferred_element_type=jnp.float32)
    value_projected = jnp.dot(normed_one, value_full, preferred_element_type=jnp.float32)
    query_heads = (
        head_map(query_proj, head_gain[0], local_query)
        .astype(jnp.bfloat16)
        .reshape(packed_token_count, local_groups, query_group_width, HEAD_SIZE)
    )
    per_head_keys = head_map(key_projected, head_gain[1], local_groups).astype(jnp.bfloat16)
    per_head_values = value_projected.astype(jnp.bfloat16).reshape(
        packed_token_count, local_groups, HEAD_SIZE
    )
    block_rows = min(512, packed_token_count)
    block_count = packed_token_count // block_rows

    def block_scores(row_start, row_stop):
        raw_scores = (
            jnp.einsum(
                "qhgd,khd->hgqk",
                query_heads[row_start:row_stop],
                per_head_keys[:row_stop],
                preferred_element_type=jnp.float32,
            )
            * score_scale
        )
        allowed = (segment_ids[row_start:row_stop, None] == segment_ids[None, :row_stop]) & (
            token_index[None, :row_stop] <= token_index[row_start:row_stop, None]
        )
        return jnp.where(allowed, raw_scores, MASKED)

    mixed_blocks = []
    log_sums = []
    for block_index in range(block_count):
        row_start = block_index * block_rows
        row_stop = row_start + block_rows
        scores = block_scores(row_start, row_stop)
        row_max = jnp.max(scores, axis=-1, keepdims=True)
        exponent = jnp.exp(scores - row_max)
        row_sum = jnp.sum(exponent, axis=-1, keepdims=True)
        weights_block = (exponent / row_sum).astype(jnp.bfloat16)
        log_sums.append(row_max + jnp.log(row_sum))
        mixed_blocks.append(
            jnp.einsum(
                "hgqk,khd->qhgd",
                weights_block,
                per_head_values[:row_stop],
                preferred_element_type=jnp.float32,
            )
        )
    mixed = (
        jnp.concatenate(mixed_blocks, axis=0)
        .reshape(packed_token_count, local_query * HEAD_SIZE)
        .astype(jnp.bfloat16)
    )
    attention_part = contract_cols(mixed, output_full)
    attention_out = lax.psum(attention_part.astype(jnp.bfloat16), "tensor").astype(jnp.float32)
    middle = input_rows + attention_out
    normed_two = gained_norm(middle, norm_gain[1]).astype(jnp.bfloat16)
    gate_proj = jnp.dot(normed_two, gate_up_full[0], preferred_element_type=jnp.float32)
    up_proj = jnp.dot(normed_two, gate_up_full[1], preferred_element_type=jnp.float32)
    hidden = swiglu(gate_proj, up_proj).astype(jnp.bfloat16)
    down_part = contract_cols(hidden, down_full)
    feedforward_out = lax.psum(down_part.astype(jnp.bfloat16), "tensor").astype(jnp.float32)
    layer_output = middle + feedforward_out
    query_back, key_back, value_back, output_back, gate_up_back, down_back = (
        query_full,
        key_full,
        value_full,
        output_full,
        gate_up_full,
        down_full,
    )
    grad_rows = out_grad.astype(jnp.float32)
    down_grad = contract_rows(out_grad, hidden)
    hidden_grad = jnp.dot(out_grad, down_back, preferred_element_type=jnp.float32)
    swiglu_out, swiglu_back = jax.vjp(swiglu, gate_proj, up_proj)
    gate_grad, up_grad = swiglu_back(hidden_grad)
    gate_grad_low = gate_grad.astype(jnp.bfloat16)
    up_grad_low = up_grad.astype(jnp.bfloat16)
    gate_up_grad = jnp.stack(
        [contract_rows(normed_two, gate_grad_low), contract_rows(normed_two, up_grad_low)]
    )
    normed_two_part = contract_cols(gate_grad_low, gate_up_back[0]) + contract_cols(
        up_grad_low, gate_up_back[1]
    )
    normed_two_grad = lax.psum(normed_two_part.astype(jnp.bfloat16), "tensor").astype(jnp.float32)
    norm_two_out, norm_two_back = jax.vjp(gained_norm, middle, norm_gain[1])
    middle_norm_grad, gain_two_grad = norm_two_back(normed_two_grad)
    middle_grad = grad_rows + middle_norm_grad
    middle_grad_low = middle_grad.astype(jnp.bfloat16)
    output_grad_w = contract_rows(middle_grad_low, mixed)
    mixed_grad = jnp.dot(middle_grad_low, output_back, preferred_element_type=jnp.float32).astype(
        jnp.bfloat16
    )
    mixed_grad = mixed_grad.reshape(packed_token_count, local_groups, query_group_width, HEAD_SIZE)
    query_grad_blocks = []
    key_grad_acc = jnp.zeros((packed_token_count, local_groups, HEAD_SIZE), jnp.float32)
    value_grad_acc = jnp.zeros((packed_token_count, local_groups, HEAD_SIZE), jnp.float32)
    for block_index in range(block_count):
        row_start = block_index * block_rows
        row_stop = row_start + block_rows
        scores = block_scores(row_start, row_stop)
        probs = jnp.exp(scores - log_sums[block_index])
        grad_block = mixed_grad[row_start:row_stop]
        prob_grad = jnp.einsum(
            "qhgd,khd->hgqk",
            grad_block,
            per_head_values[:row_stop],
            preferred_element_type=jnp.float32,
        )
        row_inner = jnp.sum(probs * prob_grad, axis=-1, keepdims=True)
        score_grad = (probs * (prob_grad - row_inner)).astype(jnp.bfloat16)
        query_grad_blocks.append(
            jnp.einsum(
                "hgqk,khd->qhgd",
                score_grad,
                per_head_keys[:row_stop],
                preferred_element_type=jnp.float32,
            )
            * score_scale
        )
        key_grad_acc = key_grad_acc.at[:row_stop].add(
            jnp.einsum(
                "hgqk,qhgd->khd",
                score_grad,
                query_heads[row_start:row_stop],
                preferred_element_type=jnp.float32,
            )
            * score_scale
        )
        value_grad_acc = value_grad_acc.at[:row_stop].add(
            jnp.einsum(
                "hgqk,qhgd->khd",
                probs.astype(jnp.bfloat16),
                grad_block,
                preferred_element_type=jnp.float32,
            )
        )
    query_grad_heads = (
        jnp.concatenate(query_grad_blocks, axis=0)
        .reshape(packed_token_count, local_query, HEAD_SIZE)
        .astype(jnp.bfloat16)
        .astype(jnp.float32)
    )
    key_grad_heads = key_grad_acc.astype(jnp.bfloat16).astype(jnp.float32)
    value_grad_low = value_grad_acc.astype(jnp.bfloat16).reshape(
        packed_token_count, local_groups * HEAD_SIZE
    )
    query_map_out, query_map_back = jax.vjp(
        lambda projected, gain: head_map(projected, gain, local_query), query_proj, head_gain[0]
    )
    query_proj_grad, head_query_grad = query_map_back(query_grad_heads)
    key_map_out, key_map_back = jax.vjp(
        lambda projected, gain: head_map(projected, gain, local_groups), key_projected, head_gain[1]
    )
    key_proj_grad, head_key_grad = key_map_back(key_grad_heads)
    query_proj_low = query_proj_grad.astype(jnp.bfloat16)
    key_proj_low = key_proj_grad.astype(jnp.bfloat16)
    query_grad_w = contract_rows(normed_one, query_proj_low)
    key_grad_w = contract_rows(normed_one, key_proj_low)
    value_grad_w = contract_rows(normed_one, value_grad_low)
    normed_one_part = (
        contract_cols(query_proj_low, query_back)
        + contract_cols(key_proj_low, key_back)
        + contract_cols(value_grad_low, value_back)
    )
    normed_one_grad = lax.psum(normed_one_part.astype(jnp.bfloat16), "tensor").astype(jnp.float32)
    head_query_total, head_key_total = lax.psum((head_query_grad, head_key_grad), "tensor")
    norm_one_out, norm_one_back = jax.vjp(gained_norm, input_rows, norm_gain[0])
    input_norm_grad, gain_one_grad = norm_one_back(normed_one_grad)
    input_grad = middle_grad + input_norm_grad
    norm_grads = jnp.stack([gain_one_grad, gain_two_grad])
    head_grads = jnp.stack([head_query_total, head_key_total])
    attn_grads = lax.psum_scatter(
        jnp.concatenate(
            [
                query_grad_w.astype(jnp.bfloat16),
                key_grad_w.astype(jnp.bfloat16),
                value_grad_w.astype(jnp.bfloat16),
                output_grad_w.astype(jnp.bfloat16),
            ],
            axis=1,
        ),
        "fsdp",
        scatter_dimension=0,
        tiled=True,
    ).astype(jnp.float32)
    shards = norm_grads.shape[1] // gain_rows
    gains_grad = lax.psum_scatter(
        jnp.concatenate(
            [norm_grads.reshape(2, shards, gain_rows), head_grads.reshape(2, shards, -1)], axis=2
        ),
        "fsdp",
        scatter_dimension=1,
        tiled=False,
    )
    shard_grads = (
        attn_grads[:, :query_cols],
        attn_grads[:, query_cols : query_cols + key_cols],
        attn_grads[:, query_cols + key_cols : query_cols + 2 * key_cols],
        attn_grads[:, query_cols + 2 * key_cols :],
        lax.psum_scatter(
            gate_up_grad.astype(jnp.bfloat16), "fsdp", scatter_dimension=1, tiled=True
        ).astype(jnp.float32),
        lax.psum_scatter(
            down_grad.astype(jnp.bfloat16), "fsdp", scatter_dimension=0, tiled=True
        ).astype(jnp.float32),
        gains_grad[:, :gain_rows],
        gains_grad[:, gain_rows:],
    )
    next_steps = []
    next_means = []
    next_squares = []
    for param_index in range(8):
        learn_rate = MATRIX_RATE if param_index < 6 else GAIN_RATE
        decay_rate = WEIGHT_DECAY if param_index < 6 else 0.0
        weight_step, mean_next, square_next = adam_step(
            params[param_index],
            shard_grads[param_index],
            means[param_index],
            squares[param_index],
            learn_rate,
            decay_rate,
        )
        next_steps.append(weight_step)
        next_means.append(mean_next)
        next_squares.append(square_next)
    results = (
        [layer_output, input_grad] + list(shard_grads) + next_steps + next_means + next_squares
    )
    return tuple(results)


FF_CHUNKS = 3
ROW_TILE = 128
ROW_GROUP = 16


def ring_place(place, shards):
    place = place % shards
    column = place // (shards // 2)
    return 2 * (place + column * (shards - 1 - 2 * place)) + column


def place_of(index, shards):
    row, column = index // 2, index % 2
    return row + column * (shards - 1 - 2 * row)


def row_scale(values):
    return lax.rsqrt(jnp.mean(values * values, axis=-1, keepdims=True) + EPSILON)


def row_call(body, scalars, arrays, gains, outs, sums=0, cost=8):
    tokens, width = arrays[0].shape
    tiles = tokens // ROW_TILE
    row = pl.BlockSpec((ROW_TILE, width), lambda tile, *_: (tile, 0))
    whole = pl.BlockSpec((1, width), lambda tile, *_: (0, 0))
    return pl.pallas_call(
        body,
        grid_spec=pltpu.PrefetchScalarGridSpec(
            num_scalar_prefetch=1,
            grid=(tiles,),
            in_specs=[row] * len(arrays)
            + [whole] * len(gains),
            out_specs=[row] * len(outs)
            + [pl.BlockSpec((8, width), lambda tile, *_: (0, 0))] * sums,
        ),
        out_shape=[jax.ShapeDtypeStruct((tokens, width), kind) for kind in outs]
        + [jax.ShapeDtypeStruct((8, width), jnp.float32)] * sums,
        cost_estimate=pl.CostEstimate(
            flops=cost * tokens * width, bytes_accessed=3 * cost * tokens * width // 2, transcendentals=0
        ),
        name=body.__name__,
    )(scalars, *arrays, *gains)


def row_groups(ref, body):
    @pl.loop(0, ref.shape[0] // ROW_GROUP)
    def _(step):
        body(pl.ds(pl.multiple_of(step * ROW_GROUP, ROW_GROUP), ROW_GROUP))


def count_of(scalars):
    return (len(scalars) if isinstance(scalars, list) else scalars.shape[0]) - 1


def turned_in(scalars, x_ref, g_ref, gain_ref, xr_ref, gr_ref, n_ref):
    shards = count_of(scalars)
    width = x_ref.shape[1] // shards
    sources = [pl.ds(pl.multiple_of(scalars[at] * width, 128), width) for at in range(shards)]

    def body(rows):
        scale = row_scale(x_ref[rows, :].astype(jnp.float32))
        for at in range(shards):
            target = slice(at * width, (at + 1) * width)
            values = x_ref[rows, sources[at]]
            xr_ref[rows, target] = values
            gr_ref[rows, target] = g_ref[rows, sources[at]]
            n_ref[rows, target] = (
                values.astype(jnp.float32) * scale * gain_ref[:, target]
            ).astype(n_ref.dtype)

    row_groups(x_ref, body)


def put_back(scalars, out_ref, rows, value):
    shards = count_of(scalars)
    width = value.shape[1] // shards
    for at in range(shards):
        out_ref[rows, pl.ds(pl.multiple_of(scalars[at] * width, 128), width)] = value[
            :, at * width : (at + 1) * width
        ]


def layer_out(scalars, mid_ref, came_ref, out_ref):
    def body(rows):
        put_back(
            scalars, out_ref, rows, mid_ref[rows, :] + came_ref[rows, :].astype(jnp.float32)
        )

    row_groups(mid_ref, body)


def norm_grad(values, grad, gain, sum_ref):
    scale = row_scale(values)
    unit = values * scale
    share = grad * unit
    sum_ref[...] += jnp.sum(share.reshape(-1, 8, share.shape[1]), axis=0)
    inner = grad * gain
    return scale * (inner - unit * jnp.mean(inner * unit, axis=-1, keepdims=True))


def clear_first(sum_ref):
    @pl.when(pl.program_id(0) == 0)
    def _():
        sum_ref[...] = jnp.zeros_like(sum_ref)


def second_back(scalars, mid_ref, g_ref, came_ref, gain_ref, dx_ref, low_ref, sum_ref):
    clear_first(sum_ref)

    def body(rows):
        grad = came_ref[rows, :].astype(jnp.float32)
        value = g_ref[rows, :].astype(jnp.float32) + norm_grad(
            mid_ref[rows, :], grad, gain_ref[...], sum_ref
        )
        dx_ref[rows, :] = value
        low_ref[rows, :] = value.astype(low_ref.dtype)

    row_groups(mid_ref, body)


def first_back(scalars, dx_ref, x_ref, came_ref, gain_ref, out_ref, sum_ref):
    clear_first(sum_ref)

    def body(rows):
        value = dx_ref[rows, :] + norm_grad(
            x_ref[rows, :].astype(jnp.float32),
            came_ref[rows, :].astype(jnp.float32),
            gain_ref[...],
            sum_ref,
        )
        put_back(scalars, out_ref, rows, value)

    row_groups(x_ref, body)


def full_call(body, scalars, lefts, matrix, window, outs, halves, name, extras=()):
    tokens = lefts[0].shape[0]
    tiles = tokens // FULL_TILE
    half = tiles // 2
    columns, at = window

    def turned(step, scalars):
        return (lax.rem(step + scalars[scalars.shape[0] - 1] * half, tiles), 0)

    def kernel(scalars, *refs):
        left_refs, whole = refs[: len(lefts)], refs[len(lefts)]
        extra_refs = refs[len(lefts) + 1 : len(lefts) + 1 + len(extras)]
        rest = refs[len(lefts) + 1 + len(extras) :]
        out_refs, half_refs = rest[: len(outs)], rest[len(outs) :]
        step = pl.program_id(0)
        values = body(left_refs, whole, extra_refs, out_refs)
        for place, value in enumerate(values):
            kept, sent = half_refs[2 * place : 2 * place + 2]

            @pl.when(step < half)
            def _():
                kept[...] = value.astype(kept.dtype)

            @pl.when(step >= half)
            def _():
                sent[...] = value.astype(sent.dtype)

    def row_spec(width):
        return pl.BlockSpec((FULL_TILE, width), turned)

    half_out = []
    for width, _ in halves:
        half_out.append(
            pl.BlockSpec((FULL_TILE, width), lambda step, _: (jnp.minimum(step, half - 1), 0))
        )
        half_out.append(
            pl.BlockSpec((FULL_TILE, width), lambda step, _: (jnp.maximum(step - half, 0), 0))
        )
    work = 2 * tokens * matrix.shape[0] * columns
    return pl.pallas_call(
        kernel,
        grid_spec=pltpu.PrefetchScalarGridSpec(
            num_scalar_prefetch=1,
            grid=(tiles,),
            in_specs=[row_spec(left.shape[1]) for left in lefts]
            + [pl.BlockSpec((matrix.shape[0], columns), lambda step, _: (0, at))]
            + [pl.BlockSpec(extra.shape, lambda step, _: (0, 0)) for extra in extras],
            out_specs=[row_spec(width) for width, _ in outs] + half_out,
        ),
        out_shape=[jax.ShapeDtypeStruct((tokens, width), kind) for width, kind in outs]
        + [
            jax.ShapeDtypeStruct((tokens // 2, width), kind)
            for width, kind in halves
            for _ in range(2)
        ],
        cost_estimate=pl.CostEstimate(flops=work, bytes_accessed=work // 250, transcendentals=0),
        name=name,
    )(scalars, *lefts, matrix, *extras)


def rows_times(left, right):
    return jnp.dot(left, right, preferred_element_type=jnp.float32)


def project_body(cuts, lefts, whole, extras, outs):
    start = 0
    for out, stop in zip(outs, cuts):
        out[...] = rows_times(lefts[0][...], whole[:, start:stop]).astype(out.dtype)
        start = stop
    return []


def back_body(lefts, whole, extras, outs):
    start, value = 0, None
    for left in lefts:
        stop = start + left.shape[1]
        term = contract_cols(left[...], whole[:, start:stop])
        value = term if value is None else value + term
        start = stop
    return [value]


def adam_body(places, count, *refs):
    arrays = len({place[0] for place in places})
    grad_refs, refs = refs[:count], refs[count:]
    states, outs = refs[: 3 * arrays], refs[3 * arrays :]
    start = 0
    for array, plane in places:
        at = (Ellipsis,) if plane is None else (plane,)
        weight, mean, square = (states[3 * array + kind][at] for kind in range(3))
        stop = start + weight.shape[-1]
        grad = grad_refs[0][:, start:stop]
        for part in range(1, count):
            other = grad_refs[part][:, start:stop].astype(jnp.float32)
            grad = jnp.where(pl.program_id(0) == part, other, grad)
        step, mean_next, square_next = adam_step(
            weight, grad, mean, square, MATRIX_RATE, WEIGHT_DECAY
        )
        for kind, result in enumerate((grad, step, mean_next, square_next)):
            outs[4 * array + kind][at] = result
        start = stop


def adam_update(grads, places, states):
    parts = len(grads)
    rows, columns = grads[0].shape
    tile = min(64, rows)

    def window(array):
        lead = array.shape[:-2]
        shape = lead + (tile, array.shape[-1] // parts)
        return pl.BlockSpec(shape, lambda part, at: (0,) * len(lead) + (at, part))

    def grad_index(own, part, at):
        return (jnp.where(part == own, at, 0), 0)

    flat = [array for group in states for array in group]
    out_like = [group[0] for group in states for _ in range(4)]
    return pl.pallas_call(
        functools.partial(adam_body, places, parts),
        grid=(parts, rows // tile),
        in_specs=[
            pl.BlockSpec((tile, columns), functools.partial(grad_index, own))
            for own in range(parts)
        ]
        + [window(array) for array in flat],
        out_specs=[window(array) for array in out_like],
        out_shape=[jax.ShapeDtypeStruct(array.shape, jnp.float32) for array in out_like],
        cost_estimate=pl.CostEstimate(
            flops=20 * parts * rows * columns,
            bytes_accessed=32 * parts * rows * columns,
            transcendentals=0,
        ),
        name="adam_update",
    )(*grads, *flat)


class Hops:
    def __init__(self, shards):
        self.shards = shards
        place = place_of(lax.axis_index("fsdp"), shards)
        self.neighbours = [
            {"fsdp": ring_place(place + shards + step, shards)} for step in (1, -1)
        ]
        tensor = lax.axis_index("tensor")
        self.core = lax.rem(tensor, 2)
        chip = tensor // 2
        self.partner = {"tensor": 2 * chip + 1 - self.core}
        self.across = {"tensor": 2 * (1 - chip) + self.core}

    def meet(self, others):
        barrier = pltpu.get_barrier_semaphore()
        for other in others:
            pl.semaphore_signal(
                barrier, inc=1, device_id=other, device_id_type=pl.DeviceIdType.MESH
            )
        pl.semaphore_wait(barrier, len(others))


def remote(source, target, sent, arrived, device):
    return pltpu.make_async_remote_copy(
        src_ref=source,
        dst_ref=target,
        send_sem=sent,
        recv_sem=arrived,
        device_id=device,
        device_id_type=pl.DeviceIdType.MESH,
    )


HALVES = 2


def half_rows(ref, half):
    rows = ref.shape[0] // HALVES
    return ref.at[pl.ds(half * rows, rows)]


class RingGather:
    def __init__(self, hops, own, slots, sems, forward):
        legs = hops.shards // 2
        reach = (legs, legs - 1) if forward else (legs - 1, legs)
        self.reach = [reach if half % 2 == 0 else reach[::-1] for half in range(HALVES)]
        self.hops, self.own, self.slots, self.sems = hops, own, slots, sems

    def copy(self, way, step, half):
        shards = self.hops.shards
        source, target = (step - 1, step) if way == 0 else (shards - step + 1, shards - step)
        return remote(
            half_rows(self.own if step == 1 else self.slots.at[source], half),
            half_rows(self.slots.at[target], half),
            self.sems[0].at[way, step - 1, half],
            self.sems[1].at[way, step - 1, half],
            self.hops.neighbours[way],
        )

    def hop(self, step):
        for half in range(HALVES):
            for way in range(2):
                if 1 < step <= self.reach[half][way] + 1:
                    self.copy(way, step - 1, half).wait_recv()
                if step <= self.reach[half][way]:
                    self.copy(way, step, half).start()

    def close(self):
        for half in range(HALVES):
            for way in range(2):
                for step in range(1, self.reach[half][way] + 1):
                    self.copy(way, step, half).wait_send()


def by_rows(count, body):
    @pl.loop(0, count // ROW_STEP)
    def _(step):
        body(pl.ds(pl.multiple_of(step * ROW_STEP, ROW_STEP), ROW_STEP))


class RingScatter:
    SLOTS = 3

    def __init__(self, hops, partial, sent, came, sems, credits, jobs, plan):
        self.hops, self.partial, self.sent, self.came = hops, partial, sent, came
        self.sems, self.credits, self.jobs = sems, credits, jobs
        self.total = [sum(job[way] for job in jobs) for way in range(2)]
        self.number = [{}, {}]
        for job, step in plan:
            for way in range(2):
                if step <= jobs[job][way]:
                    self.number[way][job, step] = len(self.number[way])

    def copy(self, way, number, half):
        slot = number % self.SLOTS
        return remote(
            half_rows(self.sent.at[way, slot], half),
            half_rows(self.came.at[way, slot], half),
            self.sems[0].at[way, slot, half],
            self.sems[1].at[way, slot, half],
            self.hops.neighbours[way],
        )

    def add(self, way, job, hop, half, out):
        number = self.number[way][job, hop]
        self.copy(way, number, half).wait_recv()
        slot = number % self.SLOTS
        count = out.shape[0] // HALVES

        @pl.loop(0, count // ROW_STEP)
        def _(step):
            rows = pl.ds(pl.multiple_of(half * count + step * ROW_STEP, ROW_STEP), ROW_STEP)
            out[rows, :] = (
                out[rows, :].astype(jnp.float32) + self.came[way, slot, rows].astype(jnp.float32)
            ).astype(out.dtype)

        if number + self.SLOTS < self.total[way]:
            pl.semaphore_signal(
                self.credits.at[way, half],
                inc=1,
                device_id=self.hops.neighbours[1 - way],
                device_id_type=pl.DeviceIdType.MESH,
            )

    def prepare(self, job, hop):
        for way in range(2):
            distance = self.jobs[job][way] - hop + 1
            if distance < 1:
                continue
            number = self.number[way][job, hop]
            if number >= self.SLOTS:
                for half in range(HALVES):
                    self.copy(way, number - self.SLOTS, half).wait_send()
            self.partial(
                job,
                self.hops.shards - distance if way == 0 else distance,
                self.sent.at[way, number % self.SLOTS],
            )

    def hop(self, job, hop):
        for half in range(HALVES):
            for way in range(2):
                if hop > self.jobs[job][way]:
                    continue
                number = self.number[way][job, hop]
                if hop > 1:
                    self.add(way, job, hop - 1, half, self.sent.at[way, number % self.SLOTS])
                if number >= self.SLOTS:
                    pl.semaphore_wait(self.credits.at[way, half], 1)
                self.copy(way, number, half).start()

    def last(self, job, own):
        for half in range(HALVES):
            for way in range(2):
                self.add(way, job, self.jobs[job][way], half, own)

    def close(self):
        for way in range(2):
            for number in range(max(0, self.total[way] - self.SLOTS), self.total[way]):
                for half in range(HALVES):
                    self.copy(way, number, half).wait_send()


class CoreSum:
    def __init__(self, hops, sent, kept, first, chip, second, out, sems):
        self.hops, self.sent, self.kept, self.first = hops, sent, kept, first
        self.chip, self.second, self.out, self.sems = chip, second, out, sems
        self.half = chip.shape[0]

    def copy(self, stage):
        rows = self.out.at[pl.ds(pl.multiple_of(self.hops.core * self.half, 128), self.half)]
        source, target, device = (
            (self.sent, self.first, self.hops.partner),
            (self.chip, self.second, self.hops.across),
            (self.chip, rows, self.hops.partner),
        )[stage]
        return remote(source, target, self.sems.at[0, stage], self.sems.at[1, stage], device)

    def local(self):
        rows = self.out.at[pl.ds(pl.multiple_of(self.hops.core * self.half, 128), self.half)]
        return pltpu.make_async_copy(self.chip, rows, self.sems.at[0, 3])

    def add(self, left, right):
        def body(rows):
            self.chip[rows, :] = (
                left[rows, :].astype(jnp.float32) + right[rows, :].astype(jnp.float32)
            ).astype(jnp.bfloat16)

        by_rows(self.half, body)

    def start(self):
        self.copy(0).start()

    def to_chip(self):
        self.copy(0).wait_recv()
        self.add(self.kept, self.first)
        self.copy(1).start()

    def to_all(self):
        self.copy(1).wait()
        self.add(self.chip, self.second)
        self.copy(2).start()
        self.local().start()

    def done(self):
        self.copy(0).wait_send()
        self.copy(2).wait()
        self.local().wait()


RING_LIMIT = 66500000


FULL_TILE = 256


def gather_body(shards, gain_cols, query_cols, key_cols, *refs):
    (own_ref, small_ref, x_ref, g_ref, ff_ref, cosine_ref, sine_ref, first_ref) = refs[:8]
    (out_ref, few_ref, early_ref, xr_ref, gr_ref, n_ref) = refs[8:14]
    (query_raw, key_raw, query_ref, key_ref, value_ref, mixed_ref) = refs[14:20]
    (kept_ref, sent_ref) = refs[20:22]
    (few, gain, head_gain, whole) = refs[22:26]
    (big_sent, big_came, ff_sent, ff_came, few_sent, few_came, local) = refs[26:]
    hops = Hops(shards)
    place = place_of(lax.axis_index("fsdp"), shards)
    ahead = [{"fsdp": ring_place(place + at, shards)} for at in range(1, shards)]
    hops.meet(ahead)
    smalls = [
        remote(small_ref, few.at[at], few_sent.at[at - 1], few_came.at[at - 1], ahead[at - 1])
        for at in range(1, shards)
    ]
    for copy in smalls:
        copy.start()
    big = RingGather(hops, own_ref, out_ref, (big_sent, big_came), True)
    early = RingGather(hops, ff_ref.at[0], early_ref, (ff_sent, ff_came), True)
    big.hop(1)
    copies = [
        pltpu.make_async_copy(own_ref, out_ref.at[0], local.at[0]),
        pltpu.make_async_copy(small_ref, few.at[0], local.at[1]),
    ]
    for copy in copies:
        copy.start()
    for copy in copies:
        copy.wait()
    for copy in smalls:
        copy.wait_recv()
    put = pltpu.make_async_copy(few, few_ref, local.at[1])
    put.start()
    turn = [ring_place(place - at + shards, shards) for at in range(shards)]
    heads = jnp.zeros((few.shape[1], HEAD_SIZE), jnp.float32)
    for at in range(shards):
        gain[:, at * gain_cols : (at + 1) * gain_cols] = few[at, 0:1, :gain_cols].astype(
            jnp.float32
        )
        heads += pltpu.roll(
            few[at, :, gain_cols : gain_cols + HEAD_SIZE].astype(jnp.float32),
            turn[at] * (HEAD_SIZE // shards),
            1,
        )
    head_gain[...] = heads
    scalars = turn + [hops.core]
    tokens, width = x_ref.shape
    tiles = tokens // ROW_TILE
    legs = shards // 2

    def turned_part(part):
        def index(tile):
            return (tile + part * (tiles // legs), 0)

        pltpu.emit_pipeline(
            lambda *refs: turned_in(scalars, *refs[:2], gain, *refs[2:]),
            grid=(tiles // legs,),
            in_specs=[pl.BlockSpec((ROW_TILE, width), index)] * 2,
            out_specs=[pl.BlockSpec((ROW_TILE, width), index)] * 3,
        )(x_ref, g_ref, xr_ref, gr_ref, n_ref)

    for part in range(legs):
        turned_part(part)
        if part + 2 <= legs:
            big.hop(part + 2)
    early.hop(1)
    big.hop(legs + 1)
    loads = [
        pltpu.make_async_copy(
            out_ref.at[at],
            whole.at[pl.ds(at * out_ref.shape[1], out_ref.shape[1])],
            local.at[2 + at],
        )
        for at in range(shards)
    ]
    for copy in loads:
        copy.start()
    for copy in loads:
        copy.wait()
    inward = query_cols + 2 * key_cols

    def project_part(part):
        def index(tile):
            return (tile + part * (tokens // FULL_TILE // 2), 0)

        def spec(array):
            return pl.BlockSpec((FULL_TILE, array.shape[1]), index)

        outs = [query_raw, key_raw, query_ref, key_ref, value_ref]
        lefts = [n_ref, cosine_ref, sine_ref]
        pltpu.emit_pipeline(
            lambda *refs: turn_body(
                query_cols, key_cols, refs[:3], whole.at[:, pl.ds(0, inward)], [head_gain], refs[3:]
            )
            and None,
            grid=(tokens // FULL_TILE // 2,),
            in_specs=[spec(left) for left in lefts],
            out_specs=[spec(out) for out in outs],
        )(*lefts, *outs)

    groups = key_cols // HEAD_SIZE

    def attention_part(group):
        def spec(array):
            return pl.BlockSpec((tokens, array.shape[1] // groups), lambda _: (0, group))

        arrays = [query_ref, key_ref, value_ref, mixed_ref]
        pltpu.emit_pipeline(
            lambda query, key, value, out: attention_body(query, key, value, first_ref, out),
            grid=(1,),
            in_specs=[spec(array) for array in arrays[:3]],
            out_specs=[spec(mixed_ref)],
        )(*arrays)

    half = tokens // 2

    def out_part(core, out):
        rows = mixed_ref.at[pl.ds(pl.multiple_of(core * half, half), half)]

        def body(left, value):
            value[...] = contract_cols(left[...], whole[:, inward:]).astype(value.dtype)

        pltpu.emit_pipeline(
            body,
            grid=(half // FULL_TILE,),
            in_specs=[pl.BlockSpec((FULL_TILE, query_cols), lambda tile: (tile, 0))],
            out_specs=[pl.BlockSpec((FULL_TILE, width), lambda tile: (tile, 0))],
        )(rows, out)

    project_part(0)
    early.hop(2)
    project_part(1)
    attention_part(0)
    early.hop(3)
    for group in range(1, groups):
        attention_part(group)
    early.hop(4)
    out_part(1 - hops.core, sent_ref)
    out_part(hops.core, kept_ref)
    early.hop(5)
    big.close()
    early.close()
    for copy in smalls:
        copy.wait_send()
    put.wait()


def gather_call(own, small, rows, grads, ff_block, cosine, sine, first, gain_cols, cuts):
    tokens, width = rows.shape
    shards = width // own.shape[0]
    legs = shards // 2
    query_cols, key_cols = cuts
    low = jnp.bfloat16
    anywhere = pl.BlockSpec(memory_space=pl.ANY)

    def like(columns, kind=low, count=tokens):
        return jax.ShapeDtypeStruct((count, columns), kind)

    return pl.pallas_call(
        functools.partial(gather_body, shards, gain_cols, query_cols, key_cols),
        in_specs=[anywhere] * 7 + [pl.BlockSpec(memory_space=pltpu.VMEM)],
        out_specs=[anywhere] * 14,
        out_shape=[
            jax.ShapeDtypeStruct((shards, *shape), low)
            for shape in (own.shape, small.shape, ff_block.shape[1:])
        ]
        + [like(width)] * 3
        + [like(query_cols, jnp.float32), like(key_cols, jnp.float32)]
        + [like(query_cols), like(key_cols), like(key_cols), like(query_cols)]
        + [like(width, low, tokens // 2)] * 2,
        scratch_shapes=[
            pltpu.VMEM((shards, *small.shape), small.dtype),
            pltpu.VMEM((1, width), jnp.float32),
            pltpu.VMEM((small.shape[0], HEAD_SIZE), jnp.float32),
            pltpu.VMEM((width, own.shape[1]), low),
        ]
        + [pltpu.SemaphoreType.DMA((2, legs, HALVES))] * 4
        + [
            pltpu.SemaphoreType.DMA((shards - 1,)),
            pltpu.SemaphoreType.DMA((shards - 1,)),
            pltpu.SemaphoreType.DMA((2 + shards,)),
        ],
        compiler_params=pltpu.CompilerParams(
            collective_id=0, has_side_effects=True, vmem_limit_bytes=56 * 1024 * 1024
        ),
        name="gather_ring",
    )(own, small, rows, grads, ff_block, cosine, sine, first)


FF_TILE = 256
ROW_STEP = 32


def ff_kernel(shards, parts, *refs):
    (sent_ref, kept_ref, x_ref, grad_ref, gain_ref, own_ref, early_ref) = refs[:7]
    (mid_ref, normsum_ref, downsum_ref, grads_ref, late_ref, whole_ref) = refs[7:13]
    (acts, whole, pairs, norm_acc, r_sent, r_came, total, late) = refs[13:21]
    (out_half, kept_half, chip, first) = refs[21:25]
    seconds = refs[25:27]
    (x_tile, mid_tile) = refs[27:29]
    (ag_sent, ag_came, rs_sent, rs_came, credits, sums, local) = refs[29:]
    place = place_of(lax.axis_index("fsdp"), shards)
    hops = Hops(shards)
    hops.meet([*hops.neighbours, hops.partner, hops.across])
    core = hops.core
    tokens, wide = x_ref.shape
    half = tokens // 2
    columns = pairs.shape[2]
    width = wide // shards
    legs = shards // 2
    gathers = [
        RingGather(
            hops,
            own_ref.at[part],
            whole_ref.at[part - 1],
            (ag_sent.at[part - 1], ag_came.at[part - 1]),
            part % 2 == 0,
        )
        for part in range(1, parts)
    ]

    def chunk_block(part, at):
        if at == 0:
            return own_ref.at[part]
        return early_ref.at[at] if part == 0 else whole_ref.at[part - 1, at]

    def partial(job, at, out):
        @pl.loop(0, 3)
        def _(pair):
            left = acts[pair // 2, :, at * width : (at + 1) * width]
            right = pairs[3 * job + pair]
            out[:, pl.ds(pl.multiple_of(pair * columns, 128), columns)] = contract_rows(
                left, right
            ).astype(out.dtype)

    scatter = RingScatter(
        hops,
        partial,
        r_sent,
        r_came,
        (rs_sent, rs_came),
        credits,
        [(legs, legs - 1) if part % 2 == 0 else (legs - 1, legs) for part in range(parts - 1)],
        [(part, step) for part in range(parts - 1) for step in range(1, legs + 1)],
    )
    attention = CoreSum(
        hops, sent_ref, kept_half, first, chip, seconds[0], acts.at[0], sums.at[0]
    )
    attention.start()
    take_kept = pltpu.make_async_copy(kept_ref, kept_half, local.at[0])
    take_grad = pltpu.make_async_copy(grad_ref, acts.at[1], local.at[1])
    take_kept.start()
    take_grad.start()
    gathers[0].hop(1)
    take_kept.wait()
    attention.to_chip()
    gathers[0].hop(2)
    gathers[0].hop(3)
    attention.to_all()
    gathers[0].hop(4)
    gathers[1].hop(1)
    attention.done()

    @pl.loop(0, tokens // FF_TILE)
    def _(tile):
        rows = pl.ds(pl.multiple_of(tile * FF_TILE, FF_TILE), FF_TILE)
        take = pltpu.make_async_copy(x_ref.at[rows], x_tile, local.at[2])
        take.start()
        take.wait()
        middle = x_tile[...].astype(jnp.float32) + acts[0, rows, :].astype(jnp.float32)
        mid_tile[...] = middle
        put = pltpu.make_async_copy(mid_tile, mid_ref.at[rows], local.at[2])
        put.start()
        acts[0, rows, :] = (middle * row_scale(middle) * gain_ref[...]).astype(jnp.bfloat16)
        put.wait()

    take_grad.wait()

    def load(part):
        copies = [
            pltpu.make_async_copy(
                chunk_block(part, at), whole.at[pl.ds(at * width, width)], local.at[3 + at]
            )
            for at in range(shards)
        ]
        for copy in copies:
            copy.start()
        for copy in copies:
            copy.wait()

    def tiles(part, start, stop):
        @pl.loop(start, stop)
        def _(tile):
            rows = pl.ds(pl.multiple_of(tile * FF_TILE, FF_TILE), FF_TILE)
            norm = acts[0, rows, :]
            grad = acts[1, rows, :]
            gate_proj = rows_times(norm, whole[:, :columns])
            up_proj = rows_times(norm, whole[:, columns : 2 * columns])
            hidden_grad = rows_times(grad, whole[:, 2 * columns :])
            gate = 1.0 / (1.0 + jnp.exp(-gate_proj))
            swish = gate_proj * gate
            gate_grad = (
                hidden_grad * up_proj * (gate * (1.0 + gate_proj * (1.0 - gate)))
            ).astype(jnp.bfloat16)
            up_grad = (hidden_grad * swish).astype(jnp.bfloat16)
            pairs[3 * part, rows, :] = gate_grad
            pairs[3 * part + 1, rows, :] = up_grad
            pairs[3 * part + 2, rows, :] = (swish * up_proj).astype(jnp.bfloat16)
            value = contract_cols(gate_grad, whole[:, :columns]) + contract_cols(
                up_grad, whole[:, columns : 2 * columns]
            )
            if part > 0:
                value += norm_acc[rows, :]
            norm_acc[rows, :] = value

    count = tokens // FF_TILE
    mine = pl.ds(pl.multiple_of(core * half, 128), half)
    other = pl.ds(pl.multiple_of((1 - core) * half, 128), half)
    norm_sum = CoreSum(
        hops, out_half, norm_acc.at[mine], first, chip, seconds[1], normsum_ref, sums.at[1]
    )
    puts = [
        pltpu.make_async_copy(total, grads_ref.at[part], local.at[2]) for part in range(parts - 1)
    ]

    def own_block(part):
        if part > 0:
            puts[part - 1].wait()
        partial(part, 0, total)

    def finish(part):
        scatter.last(part, total)
        puts[part].start()

    lates = [
        pltpu.make_async_copy(
            late.at[at % 2],
            late_ref.at[ring_place(place - at + shards, shards)],
            local.at[3 + shards + at % 2],
        )
        for at in range(shards)
    ]

    def leave(at):
        if at > 1:
            lates[at - 2].wait()
        partial(parts - 1, at, late.at[at % 2])
        lates[at].start()

    load(0)
    tiles(0, 0, 2)
    gathers[0].hop(5)
    tiles(0, 2, count)
    gathers[1].hop(2)
    load(1)
    tiles(1, 0, 2)
    gathers[1].hop(3)
    tiles(1, 2, count)
    scatter.prepare(0, 1)
    gathers[1].hop(4)
    scatter.hop(0, 1)
    scatter.prepare(0, 2)
    gathers[1].hop(5)
    load(2)
    tiles(2, 0, 2)
    scatter.hop(0, 2)
    scatter.prepare(0, 3)
    tiles(2, 2, count)

    def cast_half(rows):
        out_half[rows, :] = norm_acc[
            pl.ds(pl.multiple_of((1 - core) * half + rows.start, ROW_STEP), ROW_STEP), :
        ].astype(jnp.bfloat16)

    by_rows(half, cast_half)
    norm_sum.start()
    scatter.hop(0, 3)
    scatter.prepare(0, 4)
    norm_sum.to_chip()
    scatter.prepare(1, 1)
    leave(0)
    scatter.hop(0, 4)
    scatter.hop(1, 1)
    own_block(0)
    scatter.prepare(1, 2)
    leave(1)
    finish(0)
    scatter.hop(1, 2)
    scatter.prepare(1, 3)
    leave(2)
    leave(3)
    for part in range(parts):
        copies = [
            pltpu.make_async_copy(
                chunk_block(part, at).at[:, pl.ds(2 * columns, columns)],
                whole.at[pl.ds(at * width, width), pl.ds(part * columns, columns)],
                local.at[3 + at],
            )
            for at in range(shards)
        ]
        for copy in copies:
            copy.start()
        for copy in copies:
            copy.wait()
    scatter.hop(1, 3)
    scatter.prepare(1, 4)
    leave(4)
    norm_sum.to_all()
    norm_sum.done()

    def down_tile(tile, offset):
        rows = pl.ds(pl.multiple_of(offset + tile * FF_TILE, FF_TILE), FF_TILE)
        value = contract_cols(pairs[2, rows, :], whole[:, :columns])
        for part in range(1, parts):
            value += contract_cols(
                pairs[3 * part + 2, rows, :], whole[:, part * columns : (part + 1) * columns]
            )
        return value

    @pl.loop(0, half // FF_TILE)
    def _(tile):
        rows = pl.ds(pl.multiple_of(tile * FF_TILE, FF_TILE), FF_TILE)
        out_half[rows, :] = down_tile(tile, (1 - core) * half).astype(jnp.bfloat16)

    down_sum = CoreSum(
        hops, out_half, kept_half, first, chip, seconds[0], downsum_ref, sums.at[2]
    )
    down_sum.start()

    @pl.loop(0, half // FF_TILE)
    def _(tile):
        rows = pl.ds(pl.multiple_of(tile * FF_TILE, FF_TILE), FF_TILE)
        kept_half[rows, :] = down_tile(tile, core * half).astype(jnp.bfloat16)

    down_sum.to_chip()
    scatter.hop(1, 4)
    own_block(1)
    for at in range(5, shards):
        leave(at)
    finish(1)
    down_sum.to_all()
    down_sum.done()
    puts[parts - 2].wait()
    for copy in lates[-2:]:
        copy.wait()
    for gather in gathers:
        gather.close()
    scatter.close()


def ff_call(sent, kept, rows, grad, gain, own, early):
    parts, width, columns3 = own.shape
    tokens, wide = rows.shape
    shards = wide // width
    columns = columns3 // 3
    half = tokens // 2
    legs = shards // 2
    low = jnp.bfloat16
    anywhere = pl.BlockSpec(memory_space=pl.ANY)
    slots = RingScatter.SLOTS
    return pl.pallas_call(
        functools.partial(ff_kernel, shards, parts),
        in_specs=[anywhere] * 4 + [pl.BlockSpec(memory_space=pltpu.VMEM)] + [anywhere] * 2,
        out_specs=[anywhere] * 6,
        out_shape=[
            jax.ShapeDtypeStruct((tokens, wide), jnp.float32),
            jax.ShapeDtypeStruct((tokens, wide), low),
            jax.ShapeDtypeStruct((tokens, wide), low),
            jax.ShapeDtypeStruct((parts - 1, width, columns3), jnp.float32),
            jax.ShapeDtypeStruct((shards, width, columns3), low),
            jax.ShapeDtypeStruct((parts - 1, shards, width, columns3), low),
        ],
        scratch_shapes=[
            pltpu.VMEM((2, tokens, wide), low),
            pltpu.VMEM((wide, columns3), low),
            pltpu.VMEM((3 * parts, tokens, columns), low),
            pltpu.VMEM((tokens, wide), jnp.float32),
            pltpu.VMEM((2, slots, width, columns3), low),
            pltpu.VMEM((2, slots, width, columns3), low),
            pltpu.VMEM((width, columns3), jnp.float32),
            pltpu.VMEM((2, width, columns3), low),
        ]
        + [pltpu.VMEM((half, wide), low)] * 6
        + [
            pltpu.VMEM((FF_TILE, wide), low),
            pltpu.VMEM((FF_TILE, wide), jnp.float32),
            pltpu.SemaphoreType.DMA((parts - 1, 2, legs, HALVES)),
            pltpu.SemaphoreType.DMA((parts - 1, 2, legs, HALVES)),
            pltpu.SemaphoreType.DMA((2, slots, HALVES)),
            pltpu.SemaphoreType.DMA((2, slots, HALVES)),
            pltpu.SemaphoreType.REGULAR((2, HALVES)),
            pltpu.SemaphoreType.DMA((3, 2, 4)),
            pltpu.SemaphoreType.DMA((5 + shards,)),
        ],
        compiler_params=pltpu.CompilerParams(
            collective_id=1, has_side_effects=True, vmem_limit_bytes=RING_LIMIT
        ),
        name="ff_ring",
    )(sent, kept, rows, grad, gain, own, early)


def tail_kernel(shards, jobs, *refs):
    (sent_ref, kept_ref, norm_ref, grad_ref) = refs[:4]
    rights = refs[4:8]
    (sum_ref, grads_ref, acts, r_sent, r_came, total) = refs[8:14]
    (kept_half, chip, first, second) = refs[14:18]
    (rs_sent, rs_came, credits, sums, local) = refs[18:]
    hops = Hops(shards)
    hops.meet([*hops.neighbours, hops.partner, hops.across])
    wide = norm_ref.shape[1]
    width = wide // shards
    legs = shards // 2

    def partial(job, at, out):
        start = 0
        for left, right in jobs[job]:
            stop = start + rights[right].shape[1]
            out[:, start:stop] = contract_rows(
                acts[left, :, at * width : (at + 1) * width], rights[right][...]
            ).astype(out.dtype)
            start = stop

    scatter = RingScatter(
        hops,
        partial,
        r_sent,
        r_came,
        (rs_sent, rs_came),
        credits,
        [(legs, legs - 1) if job % 2 == 0 else (legs - 1, legs) for job in range(len(jobs))],
        [(job, step) for step in range(1, legs + 1) for job in range(len(jobs))],
    )
    take = [
        pltpu.make_async_copy(ref, target, local.at[at])
        for at, (ref, target) in enumerate(
            [(kept_ref, kept_half), (norm_ref, acts.at[0]), (grad_ref, acts.at[1])]
        )
    ]
    norm_sum = CoreSum(
        hops, sent_ref, kept_half, first, chip, second, sum_ref, sums.at[0]
    )
    puts = [pltpu.make_async_copy(total, grads_ref.at[job], local.at[0]) for job in range(2)]
    norm_sum.start()
    for copy in take:
        copy.start()
    for copy in take:
        copy.wait()
    scatter.prepare(0, 1)
    scatter.hop(0, 1)
    scatter.prepare(1, 1)
    scatter.hop(1, 1)
    norm_sum.to_chip()
    for step in range(2, legs + 1):
        for job in range(2):
            scatter.prepare(job, step)
            scatter.hop(job, step)
    for job in range(2):
        if job > 0:
            puts[job - 1].wait()
        partial(job, 0, total)
        scatter.last(job, total)
        puts[job].start()
    norm_sum.to_all()
    puts[1].wait()
    norm_sum.done()
    scatter.close()


def tail_call(sent, kept, norm, grad, rights, jobs, shards):
    tokens, wide = norm.shape
    half, width, legs = tokens // 2, wide // shards, shards // 2
    columns = sum(rights[right].shape[1] for _, right in jobs[0])
    low = jnp.bfloat16
    anywhere = pl.BlockSpec(memory_space=pl.ANY)
    slots = RingScatter.SLOTS
    return pl.pallas_call(
        functools.partial(tail_kernel, shards, jobs),
        in_specs=[anywhere] * 4 + [pl.BlockSpec(memory_space=pltpu.VMEM)] * len(rights),
        out_specs=[anywhere] * 2,
        out_shape=[
            jax.ShapeDtypeStruct((tokens, wide), low),
            jax.ShapeDtypeStruct((len(jobs), width, columns), jnp.float32),
        ],
        scratch_shapes=[
            pltpu.VMEM((2, tokens, wide), low),
            pltpu.VMEM((2, slots, width, columns), low),
            pltpu.VMEM((2, slots, width, columns), low),
            pltpu.VMEM((width, columns), jnp.float32),
        ]
        + [pltpu.VMEM((half, wide), low)] * 4
        + [
            pltpu.SemaphoreType.DMA((2, slots, HALVES)),
            pltpu.SemaphoreType.DMA((2, slots, HALVES)),
            pltpu.SemaphoreType.REGULAR((2, HALVES)),
            pltpu.SemaphoreType.DMA((1, 2, 4)),
            pltpu.SemaphoreType.DMA((3,)),
        ],
        compiler_params=pltpu.CompilerParams(
            collective_id=2, has_side_effects=True, vmem_limit_bytes=48 * 1024 * 1024
        ),
        name="tail_ring",
    )(sent, kept, norm, grad, *rights)


ATTENTION_ROWS = 256


def head_turn(raw, cosine, sine, gain):
    scaled = raw * row_scale(raw) * gain
    return scaled * cosine + pltpu.roll(scaled, HEAD_SIZE // 2, 1) * sine


def head_back(grad, raw, cosine, sine, gain):
    turned = grad * cosine - pltpu.roll(grad, HEAD_SIZE // 2, 1) * sine
    scale = row_scale(raw)
    unit = raw * scale
    inner = turned * gain
    raw_grad = scale * (inner - unit * jnp.mean(inner * unit, axis=-1, keepdims=True))
    return raw_grad, jnp.sum(turned * unit, axis=0, keepdims=True)


def turn_body(query_cols, key_cols, lefts, whole, extras, outs):
    normed, cosine_ref, sine_ref = lefts
    query_raw, key_raw, query_out, key_out, value_out = outs
    cosine, sine = cosine_ref[...], sine_ref[...]
    raw = rows_times(normed[...], whole[:, : query_cols + key_cols])
    query_raw[...] = raw[:, :query_cols]
    key_raw[...] = raw[:, query_cols:]
    value_out[...] = rows_times(normed[...], whole[:, query_cols + key_cols :]).astype(
        value_out.dtype
    )
    for out, base, gain in ((query_out, 0, 0), (key_out, query_cols, 1)):
        for start in range(0, out.shape[1], HEAD_SIZE):
            out[:, start : start + HEAD_SIZE] = head_turn(
                raw[:, base + start : base + start + HEAD_SIZE],
                cosine,
                sine,
                extras[0][gain : gain + 1, :],
            ).astype(out.dtype)
    return []


def attention_probs(query, keys, first_ref, row_start):
    rows, stop = query.shape[0], keys.shape[0]
    scores = contract_cols(query, keys) * (1.0 / math.sqrt(HEAD_SIZE))
    column = lax.broadcasted_iota(jnp.int32, (rows, stop), 1)
    row = lax.broadcasted_iota(jnp.int32, (rows, stop), 0) + row_start
    first = first_ref[row_start : row_start + rows, :]
    scores = jnp.where((column <= row) & (column >= first), scores, MASKED)
    exponent = jnp.exp(scores - jnp.max(scores, axis=-1, keepdims=True))
    return exponent * (1.0 / jnp.sum(exponent, axis=-1, keepdims=True))


def attention_body(query_ref, key_ref, value_ref, first_ref, out_ref):
    low = out_ref.dtype
    for start in range(0, query_ref.shape[1], HEAD_SIZE):
        head = slice(start, start + HEAD_SIZE)
        for row in range(0, query_ref.shape[0], ATTENTION_ROWS):
            rows, stop = slice(row, row + ATTENTION_ROWS), row + ATTENTION_ROWS
            probs = attention_probs(query_ref[rows, head], key_ref[:stop, :], first_ref, row)
            out_ref[rows, head] = rows_times(probs.astype(low), value_ref[:stop, :]).astype(low)


def attention_back_body(
    query_ref,
    key_ref,
    value_ref,
    grad_ref,
    query_raw,
    key_raw,
    cosine_ref,
    sine_ref,
    gain_ref,
    first_ref,
    query_out,
    key_out,
    value_out,
    sums_ref,
    key_acc,
    value_acc,
):
    low = query_out.dtype
    scale = 1.0 / math.sqrt(HEAD_SIZE)
    key_acc[...] = jnp.zeros_like(key_acc)
    value_acc[...] = jnp.zeros_like(value_acc)
    query_sum = jnp.zeros((1, HEAD_SIZE), jnp.float32)
    for start in range(0, query_ref.shape[1], HEAD_SIZE):
        head = slice(start, start + HEAD_SIZE)
        for row in range(0, query_ref.shape[0], ATTENTION_ROWS):
            rows, stop = slice(row, row + ATTENTION_ROWS), row + ATTENTION_ROWS
            query, grad = query_ref[rows, head], grad_ref[rows, head]
            probs = attention_probs(query, key_ref[:stop, :], first_ref, row)
            prob_grad = contract_cols(grad, value_ref[:stop, :])
            inner = jnp.sum(probs * prob_grad, axis=-1, keepdims=True)
            score_grad = (probs * (prob_grad - inner)).astype(low)
            key_acc[:stop, :] += contract_rows(score_grad, query)
            value_acc[:stop, :] += contract_rows(probs.astype(low), grad)
            query_grad = (rows_times(score_grad, key_ref[:stop, :]) * scale).astype(low)
            raw_grad, gain_grad = head_back(
                query_grad.astype(jnp.float32),
                query_raw[rows, head],
                cosine_ref[rows, :],
                sine_ref[rows, :],
                gain_ref[0:1, :],
            )
            query_out[rows, head] = raw_grad.astype(low)
            query_sum += gain_grad
    key_sum = jnp.zeros((1, HEAD_SIZE), jnp.float32)
    for row in range(0, key_ref.shape[0], ATTENTION_ROWS):
        rows = slice(row, row + ATTENTION_ROWS)
        key_grad = (key_acc[rows, :] * scale).astype(low)
        raw_grad, gain_grad = head_back(
            key_grad.astype(jnp.float32),
            key_raw[rows, :],
            cosine_ref[rows, :],
            sine_ref[rows, :],
            gain_ref[1:2, :],
        )
        key_out[rows, :] = raw_grad.astype(low)
        key_sum += gain_grad
    value_out[...] = value_acc[...].astype(low)
    sums_ref[0:1, :] = query_sum
    sums_ref[1:2, :] = key_sum


def by_group(body, arrays, outs, groups, name, scratch=(), whole=()):
    tokens = arrays[0].shape[0]

    def columns(width):
        return pl.BlockSpec((tokens, width // groups), lambda group: (0, group))

    pair = tokens * tokens * arrays[0].shape[1]
    return pl.pallas_call(
        body,
        grid=(groups,),
        in_specs=[columns(array.shape[1]) for array in arrays]
        + [pl.BlockSpec(array.shape, lambda group: (0, 0)) for array in whole],
        out_specs=[
            columns(out.shape[1])
            if len(out.shape) == 2
            else pl.BlockSpec((None, *out.shape[1:]), lambda group: (group, 0, 0))
            for out in outs
        ],
        out_shape=list(outs),
        scratch_shapes=list(scratch),
        cost_estimate=pl.CostEstimate(
            flops=4 * pair, bytes_accessed=tokens * 4096, transcendentals=pair // 128
        ),
        name=name,
    )(*arrays, *whole)


def gains_body(shards, pieces, out_ref, came, total, late, sums):
    hops = Hops(shards)
    place = place_of(lax.axis_index("fsdp"), shards)
    peers = [{"fsdp": ring_place(place - at + shards, shards)} for at in range(1, shards)]
    hops.meet([*peers, hops.partner, hops.across])
    copies = [
        remote(
            pieces.at[at], came.at[at - 1], sums.at[0, at - 1], sums.at[1, at - 1], peers[at - 1]
        )
        for at in range(1, shards)
    ]
    for copy in copies:
        copy.start()
    value = pieces[0]
    for at in range(1, shards):
        copies[at - 1].wait_recv()
        value += came[at - 1]
    for stage, peer in enumerate((hops.partner, hops.across)):
        total[stage] = value
        copy = remote(
            total.at[stage],
            late.at[stage],
            sums.at[0, shards - 1 + stage],
            sums.at[1, shards - 1 + stage],
            peer,
        )
        copy.start()
        copy.wait()
        value += late[stage]
    own = lax.broadcasted_iota(jnp.int32, value.shape, 1) < value.shape[1] - HEAD_SIZE
    out_ref[...] = jnp.where(own, total[0], value)
    for copy in copies:
        copy.wait_send()


def gains_call(pieces):
    shards, rows, columns = pieces.shape
    return pl.pallas_call(
        functools.partial(gains_body, shards),
        in_specs=[pl.BlockSpec(memory_space=pltpu.VMEM)],
        out_specs=pl.BlockSpec(memory_space=pltpu.VMEM),
        out_shape=jax.ShapeDtypeStruct((rows, columns), pieces.dtype),
        scratch_shapes=[
            pltpu.VMEM((shards - 1, rows, columns), pieces.dtype),
            pltpu.VMEM((2, rows, columns), pieces.dtype),
            pltpu.VMEM((2, rows, columns), pieces.dtype),
            pltpu.SemaphoreType.DMA((2, shards + 1)),
        ],
        compiler_params=pltpu.CompilerParams(collective_id=3, has_side_effects=True),
        name="gain_sums",
    )(pieces)


def ring_device(
    shards,
    layer_input,
    out_grad,
    segment_ids,
    query_weight,
    key_weight,
    value_matrix,
    output_weight,
    gate_up_weight,
    down_weight,
    norm_gains,
    headnorm_gains,
    query_weight_mean,
    key_weight_first_moment,
    value_weight_first_moment,
    output_weight_mean,
    gate_up_weight_mean,
    down_weight_mean,
    norm_gains_mean,
    headnorm_gains_mean,
    query_weight_square,
    key_weight_second_moment,
    value_weight_second_moment,
    output_weight_square,
    gate_up_weight_square,
    down_weight_square,
    norm_gains_square,
    headnorm_gains_square,
):
    place = place_of(lax.axis_index("fsdp"), shards)
    core = lax.axis_index("tensor") % 2
    turn = jnp.stack([ring_place(place - at + shards, shards) for at in range(shards)])
    turn = turn.astype(jnp.int32)
    scalars = jnp.concatenate([turn, core[None].astype(jnp.int32)])
    back = (place - place_of(jnp.arange(shards), shards)) % shards

    gain_cols, head_cols = norm_gains.shape[1], headnorm_gains.shape[1]
    low = jnp.bfloat16
    packed_token_count, width = layer_input.shape
    query_cols, key_cols = query_weight.shape[1], key_weight.shape[1]
    local_groups = key_cols // HEAD_SIZE
    chunk_cols = down_weight.shape[1] // FF_CHUNKS
    states = [
        (query_weight, query_weight_mean, query_weight_square),
        (key_weight, key_weight_first_moment, key_weight_second_moment),
        (value_matrix, value_weight_first_moment, value_weight_second_moment),
        (output_weight, output_weight_mean, output_weight_square),
        (gate_up_weight, gate_up_weight_mean, gate_up_weight_square),
        (down_weight, down_weight_mean, down_weight_square),
        (norm_gains, norm_gains_mean, norm_gains_square),
        (headnorm_gains, headnorm_gains_mean, headnorm_gains_square),
    ]

    attention_block = jnp.concatenate(
        [
            query_weight.astype(low),
            key_weight.astype(low),
            value_matrix.astype(low),
            output_weight.astype(low),
        ],
        axis=1,
    )
    own_gains = jnp.concatenate([norm_gains, headnorm_gains], axis=1).astype(low)
    own_gains = jnp.pad(own_gains, ((0, 14), (0, -own_gains.shape[1] % 128)))
    inward_window = (query_cols + 2 * key_cols, 0)
    outward_window = (query_cols, (query_cols + 2 * key_cols) // query_cols)
    ff_block = jnp.stack(
        [
            jnp.concatenate(
                [
                    gate_up_weight[0, :, cols].astype(low),
                    gate_up_weight[1, :, cols].astype(low),
                    down_weight[:, cols].astype(low),
                ],
                axis=1,
            )
            for cols in (
                slice(chunk * chunk_cols, (chunk + 1) * chunk_cols) for chunk in range(FF_CHUNKS)
            )
        ]
    )
    token_positions = positions_of(segment_ids)
    first_key = (jnp.arange(packed_token_count, dtype=jnp.int32) - token_positions)[:, None]
    frequencies = ROPE_BASE ** (
        -2.0 * jnp.arange(HEAD_SIZE // 2).astype(jnp.float32) / HEAD_SIZE
    )
    angles = token_positions.astype(jnp.float32)[:, None] * frequencies[None, :]
    cosine = jnp.tile(jnp.cos(angles), (1, 2))
    sine = jnp.sin(angles)
    sine = jnp.concatenate([-sine, sine], axis=1)

    (
        attention_full,
        gains,
        ff_early,
        input_rows,
        grad_low,
        normed_one,
        query_raw,
        key_raw,
        query_heads,
        key_heads,
        value_heads,
        mixed,
        kept,
        sent,
    ) = gather_call(
        attention_block,
        own_gains,
        layer_input,
        out_grad,
        ff_block,
        cosine,
        sine,
        first_key,
        gain_cols,
        (query_cols, key_cols),
    )
    attention_full = attention_full.reshape(width, -1)
    gains = jnp.swapaxes(gains[:, :2].astype(jnp.float32), 0, 1)
    norm_gain = gains[:, :, :gain_cols].reshape(2, 1, -1)
    head_gain = gains[:, :, gain_cols : gain_cols + head_cols][:, back].reshape(2, -1)
    middle, norm_sum, down_sum, ff_sums, ff_late, _ = ff_call(
        sent, kept, input_rows, grad_low, norm_gain[1], ff_block, ff_early
    )
    ff_last = lax.psum_scatter(ff_late, "fsdp", scatter_dimension=0, tiled=False)
    middle_grad, middle_grad_low, gain_two_grad = row_call(
        second_back,
        scalars,
        [middle, grad_low, norm_sum],
        [norm_gain[1]],
        [jnp.float32, low],
        sums=1,
    )
    (mixed_grad,) = full_call(
        functools.partial(project_body, (query_cols,)),
        scalars,
        [middle_grad_low],
        attention_full,
        outward_window,
        [(query_cols, low)],
        [],
        "mixed_back",
    )
    query_proj_low, key_proj_low, value_grad_low, head_sums = by_group(
        attention_back_body,
        [query_heads, key_heads, value_heads, mixed_grad, query_raw, key_raw],
        [
            jax.ShapeDtypeStruct(query_heads.shape, low),
            jax.ShapeDtypeStruct(key_heads.shape, low),
            jax.ShapeDtypeStruct(key_heads.shape, low),
            jax.ShapeDtypeStruct((local_groups, 2, HEAD_SIZE), jnp.float32),
        ],
        local_groups,
        "attention_back",
        scratch=[pltpu.VMEM((packed_token_count, HEAD_SIZE), jnp.float32)] * 2,
        whole=[cosine, sine, head_gain, first_key],
    )
    kept, sent = full_call(
        back_body,
        scalars,
        [query_proj_low, key_proj_low, value_grad_low],
        attention_full,
        inward_window,
        [],
        [(width, low)],
        "projection_back",
    )
    norm_one_sum, attention_sums = tail_call(
        sent,
        kept,
        normed_one,
        middle_grad_low,
        [query_proj_low, key_proj_low, value_grad_low, mixed],
        (((0, 0), (0, 1)), ((0, 2), (1, 3))),
        shards,
    )
    (layer_output,) = row_call(layer_out, scalars, [middle, down_sum], [], [jnp.float32])
    input_grad, gain_one_grad = row_call(
        first_back,
        scalars,
        [middle_grad, input_rows, norm_one_sum],
        [norm_gain[0]],
        [jnp.float32],
        sums=1,
    )
    head_grads = jnp.sum(head_sums, axis=0).reshape(2, shards, head_cols)[:, turn]
    pieces = jnp.concatenate(
        [
            jnp.sum(gain_one_grad, axis=0).reshape(shards, 1, gain_cols),
            jnp.sum(gain_two_grad, axis=0).reshape(shards, 1, gain_cols),
            jnp.pad(
                jnp.swapaxes(head_grads, 0, 1).reshape(shards, 1, 2 * head_cols),
                ((0, 0), (0, 0), (0, HEAD_SIZE - 2 * head_cols)),
            ),
        ],
        axis=2,
    )
    gain_sums = gains_call(pieces)
    ff_updates = adam_update(
        [ff_sums[0], ff_sums[1], ff_last], [(0, 0), (0, 1), (1, None)], states[4:6]
    )
    inner_updates = adam_update([attention_sums[0]], [(0, None), (1, None)], states[0:2])
    outer_updates = adam_update([attention_sums[1]], [(0, None), (1, None)], states[2:4])
    gain_shards = [
        gain_sums[:, : 2 * gain_cols].reshape(2, gain_cols),
        gain_sums[:, 2 * gain_cols : 2 * gain_cols + 2 * head_cols].reshape(2, head_cols),
    ]
    updates = [inner_updates[:4], inner_updates[4:], outer_updates[:4], outer_updates[4:]]
    updates += [ff_updates[:4], ff_updates[4:]]
    for (weight, mean, square), grad in zip(states[6:], gain_shards):
        updates.append([grad, *adam_step(weight, grad, mean, square, GAIN_RATE, 0.0)])
    return tuple([layer_output, input_grad] + [update[kind] for kind in range(4) for update in updates])


def solution(mesh):
    shards, parts = mesh.shape["fsdp"], mesh.shape["tensor"]
    ringed = parts == 4 and shards == 8
    return jax.shard_map(
        functools.partial(ring_device, shards) if ringed else plain_device,
        mesh=mesh,
        in_specs=(
            P("fsdp", None),
            P("fsdp", None),
            P("fsdp"),
            P("fsdp", "tensor"),
            P("fsdp", "tensor"),
            P("fsdp", "tensor"),
            P("fsdp", "tensor"),
            P(None, "fsdp", "tensor"),
            P("fsdp", "tensor"),
            P(None, "fsdp"),
            P(None, "fsdp"),
            P("fsdp", "tensor"),
            P("fsdp", "tensor"),
            P("fsdp", "tensor"),
            P("fsdp", "tensor"),
            P(None, "fsdp", "tensor"),
            P("fsdp", "tensor"),
            P(None, "fsdp"),
            P(None, "fsdp"),
            P("fsdp", "tensor"),
            P("fsdp", "tensor"),
            P("fsdp", "tensor"),
            P("fsdp", "tensor"),
            P(None, "fsdp", "tensor"),
            P("fsdp", "tensor"),
            P(None, "fsdp"),
            P(None, "fsdp"),
        ),
        out_specs=(
            P("fsdp", None),
            P("fsdp", None),
            P("fsdp", "tensor"),
            P("fsdp", "tensor"),
            P("fsdp", "tensor"),
            P("fsdp", "tensor"),
            P(None, "fsdp", "tensor"),
            P("fsdp", "tensor"),
            P(None, "fsdp"),
            P(None, "fsdp"),
            P("fsdp", "tensor"),
            P("fsdp", "tensor"),
            P("fsdp", "tensor"),
            P("fsdp", "tensor"),
            P(None, "fsdp", "tensor"),
            P("fsdp", "tensor"),
            P(None, "fsdp"),
            P(None, "fsdp"),
            P("fsdp", "tensor"),
            P("fsdp", "tensor"),
            P("fsdp", "tensor"),
            P("fsdp", "tensor"),
            P(None, "fsdp", "tensor"),
            P("fsdp", "tensor"),
            P(None, "fsdp"),
            P(None, "fsdp"),
            P("fsdp", "tensor"),
            P("fsdp", "tensor"),
            P("fsdp", "tensor"),
            P("fsdp", "tensor"),
            P(None, "fsdp", "tensor"),
            P("fsdp", "tensor"),
            P(None, "fsdp"),
            P(None, "fsdp"),
        ),
        check_vma=False,
    )
```

```python
import functools
import math

import jax
import jax.numpy as jnp
from jax import lax
from jax.experimental import pallas as pl
from jax.experimental.pallas import tpu as pltpu
from jax.sharding import PartitionSpec as P

HEAD_SIZE = 128
MODEL_WIDTH = 2048
ADAM_STEP = 3


EPSILON = 1e-06
ROPE_BASE = 1000000.0
MASKED = -1e30
BETA_ONE = 0.9
BETA_TWO = 0.95
ADAM_EPSILON = 1e-08
MATRIX_RATE = 0.02
GAIN_RATE = 0.1
WEIGHT_DECAY = 0.1


def root_mean_scale(values):
    return values * lax.rsqrt(jnp.mean(values * values, axis=-1, keepdims=True) + EPSILON)


def positions_of(segments):
    earlier = jnp.sum((segments[None, :] < segments[:, None]).astype(jnp.int32), axis=1)
    return jnp.arange(segments.shape[0], dtype=jnp.int32) - earlier


def rotary_embedding(values, token_positions):
    head_width = values.shape[-1]
    half_width = head_width // 2
    frequencies = ROPE_BASE ** (-2.0 * jnp.arange(half_width).astype(values.dtype) / head_width)
    angles = token_positions.astype(values.dtype)[:, None] * frequencies[None, :]
    cosine = jnp.cos(angles)[:, None, :]
    sine_part = jnp.sin(angles)[:, None, :]
    first_half = values[..., :half_width]
    second_half = values[..., half_width:]
    return jnp.concatenate(
        [
            first_half * cosine - second_half * sine_part,
            second_half * cosine + first_half * sine_part,
        ],
        axis=-1,
    )


def contract_rows(left, right):
    return lax.dot_general(
        left, right, (((0,), (0,)), ((), ())), preferred_element_type=jnp.float32
    )


def contract_cols(left, right):
    return lax.dot_general(
        left, right, (((1,), (1,)), ((), ())), preferred_element_type=jnp.float32
    )


def gained_norm(values, gain):
    return root_mean_scale(values) * gain


def swiglu(gate_proj, up_proj):
    return jax.nn.silu(gate_proj) * up_proj


def adam_step(weight, gradient, mean_state, square_state, learn_rate, decay_rate):
    mean_next = BETA_ONE * mean_state + (1.0 - BETA_ONE) * gradient
    square_next = BETA_TWO * square_state + (1.0 - BETA_TWO) * gradient * gradient
    mean_hat = mean_next / (1.0 - BETA_ONE**ADAM_STEP)
    square_hat = square_next / (1.0 - BETA_TWO**ADAM_STEP)
    weight_next = weight - learn_rate * (
        mean_hat / (jnp.sqrt(square_hat) + ADAM_EPSILON) + decay_rate * weight
    )
    return (weight_next - weight, mean_next, square_next)


def plain_device(
    layer_input,
    out_grad,
    segment_ids,
    query_weight,
    key_weight,
    value_matrix,
    output_weight,
    gate_up_weight,
    down_weight,
    norm_gains,
    headnorm_gains,
    query_weight_mean,
    key_weight_first_moment,
    value_weight_first_moment,
    output_weight_mean,
    gate_up_weight_mean,
    down_weight_mean,
    norm_gains_mean,
    headnorm_gains_mean,
    query_weight_square,
    key_weight_second_moment,
    value_weight_second_moment,
    output_weight_square,
    gate_up_weight_square,
    down_weight_square,
    norm_gains_square,
    headnorm_gains_square,
):
    params = (
        query_weight,
        key_weight,
        value_matrix,
        output_weight,
        gate_up_weight,
        down_weight,
        norm_gains,
        headnorm_gains,
    )
    means = (
        query_weight_mean,
        key_weight_first_moment,
        value_weight_first_moment,
        output_weight_mean,
        gate_up_weight_mean,
        down_weight_mean,
        norm_gains_mean,
        headnorm_gains_mean,
    )
    squares = (
        query_weight_square,
        key_weight_second_moment,
        value_weight_second_moment,
        output_weight_square,
        gate_up_weight_square,
        down_weight_square,
        norm_gains_square,
        headnorm_gains_square,
    )
    gain_rows = norm_gains.shape[1]
    gains_low = lax.all_gather(
        jnp.concatenate([norm_gains, headnorm_gains], axis=1).astype(jnp.bfloat16),
        "fsdp",
        axis=0,
    )
    norm_full = jnp.swapaxes(gains_low[:, :, :gain_rows], 0, 1).reshape(2, -1)
    head_full = jnp.swapaxes(gains_low[:, :, gain_rows:], 0, 1).reshape(2, -1)
    query_cols = query_weight.shape[1]
    key_cols = key_weight.shape[1]
    attn_low = jnp.concatenate(
        [query_weight, key_weight, value_matrix, output_weight], axis=1
    ).astype(jnp.bfloat16)
    attn_full = lax.all_gather(attn_low, "fsdp", axis=0, tiled=True)
    query_full = attn_full[:, :query_cols]
    key_full = attn_full[:, query_cols : query_cols + key_cols]
    value_full = attn_full[:, query_cols + key_cols : query_cols + 2 * key_cols]
    output_full = attn_full[:, query_cols + 2 * key_cols :]
    gate_up_full = lax.all_gather(gate_up_weight.astype(jnp.bfloat16), "fsdp", axis=1, tiled=True)
    down_full = lax.all_gather(down_weight.astype(jnp.bfloat16), "fsdp", axis=0, tiled=True)
    norm_gain = norm_full.astype(jnp.float32)
    head_gain = head_full.astype(jnp.float32)
    packed_token_count = layer_input.shape[0]
    local_query = query_full.shape[1] // HEAD_SIZE
    local_groups = key_full.shape[1] // HEAD_SIZE
    query_group_width = local_query // local_groups
    score_scale = 1.0 / math.sqrt(HEAD_SIZE)
    token_positions = positions_of(segment_ids)
    token_index = jnp.arange(packed_token_count, dtype=jnp.int32)
    input_rows = layer_input.astype(jnp.float32)

    def head_map(projected, gain, heads):
        return rotary_embedding(
            root_mean_scale(projected.reshape(packed_token_count, heads, HEAD_SIZE)) * gain,
            token_positions,
        )

    normed_one = gained_norm(input_rows, norm_gain[0]).astype(jnp.bfloat16)
    query_proj = jnp.dot(normed_one, query_full, preferred_element_type=jnp.float32)
    key_projected = jnp.dot(normed_one, key_full, preferred_element_type=jnp.float32)
    value_projected = jnp.dot(normed_one, value_full, preferred_element_type=jnp.float32)
    query_heads = (
        head_map(query_proj, head_gain[0], local_query)
        .astype(jnp.bfloat16)
        .reshape(packed_token_count, local_groups, query_group_width, HEAD_SIZE)
    )
    per_head_keys = head_map(key_projected, head_gain[1], local_groups).astype(jnp.bfloat16)
    per_head_values = value_projected.astype(jnp.bfloat16).reshape(
        packed_token_count, local_groups, HEAD_SIZE
    )
    block_rows = min(512, packed_token_count)
    block_count = packed_token_count // block_rows

    def block_scores(row_start, row_stop):
        raw_scores = (
            jnp.einsum(
                "qhgd,khd->hgqk",
                query_heads[row_start:row_stop],
                per_head_keys[:row_stop],
                preferred_element_type=jnp.float32,
            )
            * score_scale
        )
        allowed = (segment_ids[row_start:row_stop, None] == segment_ids[None, :row_stop]) & (
            token_index[None, :row_stop] <= token_index[row_start:row_stop, None]
        )
        return jnp.where(allowed, raw_scores, MASKED)

    mixed_blocks = []
    log_sums = []
    for block_index in range(block_count):
        row_start = block_index * block_rows
        row_stop = row_start + block_rows
        scores = block_scores(row_start, row_stop)
        row_max = jnp.max(scores, axis=-1, keepdims=True)
        exponent = jnp.exp(scores - row_max)
        row_sum = jnp.sum(exponent, axis=-1, keepdims=True)
        weights_block = (exponent / row_sum).astype(jnp.bfloat16)
        log_sums.append(row_max + jnp.log(row_sum))
        mixed_blocks.append(
            jnp.einsum(
                "hgqk,khd->qhgd",
                weights_block,
                per_head_values[:row_stop],
                preferred_element_type=jnp.float32,
            )
        )
    mixed = (
        jnp.concatenate(mixed_blocks, axis=0)
        .reshape(packed_token_count, local_query * HEAD_SIZE)
        .astype(jnp.bfloat16)
    )
    attention_part = contract_cols(mixed, output_full)
    attention_out = lax.psum(attention_part.astype(jnp.bfloat16), "tensor").astype(jnp.float32)
    middle = input_rows + attention_out
    normed_two = gained_norm(middle, norm_gain[1]).astype(jnp.bfloat16)
    gate_proj = jnp.dot(normed_two, gate_up_full[0], preferred_element_type=jnp.float32)
    up_proj = jnp.dot(normed_two, gate_up_full[1], preferred_element_type=jnp.float32)
    hidden = swiglu(gate_proj, up_proj).astype(jnp.bfloat16)
    down_part = contract_cols(hidden, down_full)
    feedforward_out = lax.psum(down_part.astype(jnp.bfloat16), "tensor").astype(jnp.float32)
    layer_output = middle + feedforward_out
    query_back, key_back, value_back, output_back, gate_up_back, down_back = (
        query_full,
        key_full,
        value_full,
        output_full,
        gate_up_full,
        down_full,
    )
    grad_rows = out_grad.astype(jnp.float32)
    down_grad = contract_rows(out_grad, hidden)
    hidden_grad = jnp.dot(out_grad, down_back, preferred_element_type=jnp.float32)
    swiglu_out, swiglu_back = jax.vjp(swiglu, gate_proj, up_proj)
    gate_grad, up_grad = swiglu_back(hidden_grad)
    gate_grad_low = gate_grad.astype(jnp.bfloat16)
    up_grad_low = up_grad.astype(jnp.bfloat16)
    gate_up_grad = jnp.stack(
        [contract_rows(normed_two, gate_grad_low), contract_rows(normed_two, up_grad_low)]
    )
    normed_two_part = contract_cols(gate_grad_low, gate_up_back[0]) + contract_cols(
        up_grad_low, gate_up_back[1]
    )
    normed_two_grad = lax.psum(normed_two_part.astype(jnp.bfloat16), "tensor").astype(jnp.float32)
    norm_two_out, norm_two_back = jax.vjp(gained_norm, middle, norm_gain[1])
    middle_norm_grad, gain_two_grad = norm_two_back(normed_two_grad)
    middle_grad = grad_rows + middle_norm_grad
    middle_grad_low = middle_grad.astype(jnp.bfloat16)
    output_grad_w = contract_rows(middle_grad_low, mixed)
    mixed_grad = jnp.dot(middle_grad_low, output_back, preferred_element_type=jnp.float32).astype(
        jnp.bfloat16
    )
    mixed_grad = mixed_grad.reshape(packed_token_count, local_groups, query_group_width, HEAD_SIZE)
    query_grad_blocks = []
    key_grad_acc = jnp.zeros((packed_token_count, local_groups, HEAD_SIZE), jnp.float32)
    value_grad_acc = jnp.zeros((packed_token_count, local_groups, HEAD_SIZE), jnp.float32)
    for block_index in range(block_count):
        row_start = block_index * block_rows
        row_stop = row_start + block_rows
        scores = block_scores(row_start, row_stop)
        probs = jnp.exp(scores - log_sums[block_index])
        grad_block = mixed_grad[row_start:row_stop]
        prob_grad = jnp.einsum(
            "qhgd,khd->hgqk",
            grad_block,
            per_head_values[:row_stop],
            preferred_element_type=jnp.float32,
        )
        row_inner = jnp.sum(probs * prob_grad, axis=-1, keepdims=True)
        score_grad = (probs * (prob_grad - row_inner)).astype(jnp.bfloat16)
        query_grad_blocks.append(
            jnp.einsum(
                "hgqk,khd->qhgd",
                score_grad,
                per_head_keys[:row_stop],
                preferred_element_type=jnp.float32,
            )
            * score_scale
        )
        key_grad_acc = key_grad_acc.at[:row_stop].add(
            jnp.einsum(
                "hgqk,qhgd->khd",
                score_grad,
                query_heads[row_start:row_stop],
                preferred_element_type=jnp.float32,
            )
            * score_scale
        )
        value_grad_acc = value_grad_acc.at[:row_stop].add(
            jnp.einsum(
                "hgqk,qhgd->khd",
                probs.astype(jnp.bfloat16),
                grad_block,
                preferred_element_type=jnp.float32,
            )
        )
    query_grad_heads = (
        jnp.concatenate(query_grad_blocks, axis=0)
        .reshape(packed_token_count, local_query, HEAD_SIZE)
        .astype(jnp.bfloat16)
        .astype(jnp.float32)
    )
    key_grad_heads = key_grad_acc.astype(jnp.bfloat16).astype(jnp.float32)
    value_grad_low = value_grad_acc.astype(jnp.bfloat16).reshape(
        packed_token_count, local_groups * HEAD_SIZE
    )
    query_map_out, query_map_back = jax.vjp(
        lambda projected, gain: head_map(projected, gain, local_query), query_proj, head_gain[0]
    )
    query_proj_grad, head_query_grad = query_map_back(query_grad_heads)
    key_map_out, key_map_back = jax.vjp(
        lambda projected, gain: head_map(projected, gain, local_groups), key_projected, head_gain[1]
    )
    key_proj_grad, head_key_grad = key_map_back(key_grad_heads)
    query_proj_low = query_proj_grad.astype(jnp.bfloat16)
    key_proj_low = key_proj_grad.astype(jnp.bfloat16)
    query_grad_w = contract_rows(normed_one, query_proj_low)
    key_grad_w = contract_rows(normed_one, key_proj_low)
    value_grad_w = contract_rows(normed_one, value_grad_low)
    normed_one_part = (
        contract_cols(query_proj_low, query_back)
        + contract_cols(key_proj_low, key_back)
        + contract_cols(value_grad_low, value_back)
    )
    normed_one_grad = lax.psum(normed_one_part.astype(jnp.bfloat16), "tensor").astype(jnp.float32)
    head_query_total, head_key_total = lax.psum((head_query_grad, head_key_grad), "tensor")
    norm_one_out, norm_one_back = jax.vjp(gained_norm, input_rows, norm_gain[0])
    input_norm_grad, gain_one_grad = norm_one_back(normed_one_grad)
    input_grad = middle_grad + input_norm_grad
    norm_grads = jnp.stack([gain_one_grad, gain_two_grad])
    head_grads = jnp.stack([head_query_total, head_key_total])
    attn_grads = lax.psum_scatter(
        jnp.concatenate(
            [
                query_grad_w.astype(jnp.bfloat16),
                key_grad_w.astype(jnp.bfloat16),
                value_grad_w.astype(jnp.bfloat16),
                output_grad_w.astype(jnp.bfloat16),
            ],
            axis=1,
        ),
        "fsdp",
        scatter_dimension=0,
        tiled=True,
    ).astype(jnp.float32)
    shards = norm_grads.shape[1] // gain_rows
    gains_grad = lax.psum_scatter(
        jnp.concatenate(
            [norm_grads.reshape(2, shards, gain_rows), head_grads.reshape(2, shards, -1)], axis=2
        ),
        "fsdp",
        scatter_dimension=1,
        tiled=False,
    )
    shard_grads = (
        attn_grads[:, :query_cols],
        attn_grads[:, query_cols : query_cols + key_cols],
        attn_grads[:, query_cols + key_cols : query_cols + 2 * key_cols],
        attn_grads[:, query_cols + 2 * key_cols :],
        lax.psum_scatter(
            gate_up_grad.astype(jnp.bfloat16), "fsdp", scatter_dimension=1, tiled=True
        ).astype(jnp.float32),
        lax.psum_scatter(
            down_grad.astype(jnp.bfloat16), "fsdp", scatter_dimension=0, tiled=True
        ).astype(jnp.float32),
        gains_grad[:, :gain_rows],
        gains_grad[:, gain_rows:],
    )
    next_steps = []
    next_means = []
    next_squares = []
    for param_index in range(8):
        learn_rate = MATRIX_RATE if param_index < 6 else GAIN_RATE
        decay_rate = WEIGHT_DECAY if param_index < 6 else 0.0
        weight_step, mean_next, square_next = adam_step(
            params[param_index],
            shard_grads[param_index],
            means[param_index],
            squares[param_index],
            learn_rate,
            decay_rate,
        )
        next_steps.append(weight_step)
        next_means.append(mean_next)
        next_squares.append(square_next)
    results = (
        [layer_output, input_grad] + list(shard_grads) + next_steps + next_means + next_squares
    )
    return tuple(results)


FF_CHUNKS = 3
ROW_TILE = 128
ROW_GROUP = 16


def ring_place(place, shards):
    place = place % shards
    column = place // (shards // 2)
    return 2 * (place + column * (shards - 1 - 2 * place)) + column


def place_of(index, shards):
    row, column = index // 2, index % 2
    return row + column * (shards - 1 - 2 * row)


def row_scale(values):
    return lax.rsqrt(jnp.mean(values * values, axis=-1, keepdims=True) + EPSILON)


def row_call(body, scalars, arrays, gains, outs, sums=0, cost=8, matrix=None, columns=0, at=0):
    tokens, width = arrays[0].shape
    tiles = tokens // ROW_TILE
    row = pl.BlockSpec((ROW_TILE, width), lambda tile, *_: (tile, 0))
    whole = pl.BlockSpec((1, width), lambda tile, *_: (0, 0))
    return pl.pallas_call(
        body,
        grid_spec=pltpu.PrefetchScalarGridSpec(
            num_scalar_prefetch=1,
            grid=(tiles,),
            in_specs=[row] * len(arrays)
            + [whole] * len(gains)
            + ([] if matrix is None else [pl.BlockSpec((width, columns), lambda *_: (0, at))]),
            out_specs=[row] * len(outs)
            + (
                []
                if matrix is None
                else [pl.BlockSpec((ROW_TILE, columns), lambda tile, *_: (tile, 0))]
            )
            + [pl.BlockSpec((8, width), lambda tile, *_: (0, 0))] * sums,
        ),
        out_shape=[jax.ShapeDtypeStruct((tokens, width), kind) for kind in outs]
        + ([] if matrix is None else [jax.ShapeDtypeStruct((tokens, columns), jnp.bfloat16)])
        + [jax.ShapeDtypeStruct((8, width), jnp.float32)] * sums,
        cost_estimate=pl.CostEstimate(
            flops=cost * tokens * width, bytes_accessed=3 * cost * tokens * width // 2, transcendentals=0
        ),
        name=body.__name__,
    )(scalars, *arrays, *gains, *([] if matrix is None else [matrix]))


def row_groups(ref, body):
    @pl.loop(0, ref.shape[0] // ROW_GROUP)
    def _(step):
        body(pl.ds(pl.multiple_of(step * ROW_GROUP, ROW_GROUP), ROW_GROUP))


def count_of(scalars):
    return (len(scalars) if isinstance(scalars, list) else scalars.shape[0]) - 1


def turned_in(scalars, x_ref, g_ref, gain_ref, xr_ref, gr_ref, n_ref):
    shards = count_of(scalars)
    width = x_ref.shape[1] // shards
    sources = [pl.ds(pl.multiple_of(scalars[at] * width, 128), width) for at in range(shards)]

    def body(rows):
        scale = row_scale(x_ref[rows, :].astype(jnp.float32))
        for at in range(shards):
            target = slice(at * width, (at + 1) * width)
            values = x_ref[rows, sources[at]]
            xr_ref[rows, target] = values
            gr_ref[rows, target] = g_ref[rows, sources[at]]
            n_ref[rows, target] = (
                values.astype(jnp.float32) * scale * gain_ref[:, target]
            ).astype(n_ref.dtype)

    row_groups(x_ref, body)


def put_back(scalars, out_ref, rows, value):
    shards = count_of(scalars)
    width = value.shape[1] // shards
    for at in range(shards):
        out_ref[rows, pl.ds(pl.multiple_of(scalars[at] * width, 128), width)] = value[
            :, at * width : (at + 1) * width
        ]


def layer_out(scalars, mid_ref, came_ref, out_ref):
    def body(rows):
        put_back(
            scalars,
            out_ref,
            rows,
            mid_ref[rows, :].astype(jnp.float32) + came_ref[rows, :].astype(jnp.float32),
        )

    row_groups(mid_ref, body)


LANES = 128


def norm_back(rows, values_ref, grad_ref, gain_ref, base_ref, sum_ref, put):
    width = values_ref.shape[1]

    def lanes(ref, start):
        return ref[rows, start : start + LANES].astype(jnp.float32)

    squares = products = 0.0
    for start in range(0, width, LANES):
        values = lanes(values_ref, start)
        squares += values * values
        products += lanes(grad_ref, start) * gain_ref[:, start : start + LANES] * values
    mean = jnp.sum(squares, axis=-1, keepdims=True) * (1.0 / width)
    scale = lax.rsqrt(mean + EPSILON)
    slope = scale * scale * scale * (jnp.sum(products, axis=-1, keepdims=True) * (1.0 / width))
    for start in range(0, width, LANES):
        values, grad = lanes(values_ref, start), lanes(grad_ref, start)
        share = grad * (values * scale)
        sum_ref[:, start : start + LANES] += jnp.sum(share.reshape(-1, 8, LANES), axis=0)
        inner = grad * gain_ref[:, start : start + LANES]
        put(start, lanes(base_ref, start) + (scale * inner - slope * values))


def clear_first(sum_ref):
    @pl.when(pl.program_id(0) == 0)
    def _():
        sum_ref[...] = jnp.zeros_like(sum_ref)


def second_back(
    scalars, mid_ref, g_ref, came_ref, gain_ref, whole, low_ref, out_ref, sum_ref
):
    clear_first(sum_ref)

    def body(rows):
        def put(start, value):
            low_ref[rows, start : start + LANES] = value.astype(low_ref.dtype)

        norm_back(rows, mid_ref, came_ref, gain_ref, g_ref, sum_ref, put)

    row_groups(mid_ref, body)
    out_ref[...] = rows_times(low_ref[...], whole[...]).astype(out_ref.dtype)


def first_back(scalars, dx_ref, x_ref, came_ref, gain_ref, out_ref, sum_ref):
    clear_first(sum_ref)
    width = x_ref.shape[1] // count_of(scalars)

    def body(rows):
        def put(start, value):
            at, inside = start // width, start % width
            target = pl.multiple_of(scalars[at] * width + inside, LANES)
            out_ref[rows, pl.ds(target, LANES)] = value

        norm_back(rows, x_ref, came_ref, gain_ref, dx_ref, sum_ref, put)

    row_groups(x_ref, body)


def full_call(body, scalars, lefts, matrix, window, outs, halves, name, extras=()):
    tokens = lefts[0].shape[0]
    tiles = tokens // FULL_TILE
    half = tiles // 2
    columns, at = window

    def turned(step, scalars):
        return (lax.rem(step + scalars[scalars.shape[0] - 1] * half, tiles), 0)

    def kernel(scalars, *refs):
        left_refs, whole = refs[: len(lefts)], refs[len(lefts)]
        extra_refs = refs[len(lefts) + 1 : len(lefts) + 1 + len(extras)]
        rest = refs[len(lefts) + 1 + len(extras) :]
        out_refs, half_refs = rest[: len(outs)], rest[len(outs) :]
        step = pl.program_id(0)
        values = body(left_refs, whole, extra_refs, out_refs)
        for place, value in enumerate(values):
            kept, sent = half_refs[2 * place : 2 * place + 2]

            @pl.when(step < half)
            def _():
                kept[...] = value.astype(kept.dtype)

            @pl.when(step >= half)
            def _():
                sent[...] = value.astype(sent.dtype)

    def row_spec(width):
        return pl.BlockSpec((FULL_TILE, width), turned)

    half_out = []
    for width, _ in halves:
        half_out.append(
            pl.BlockSpec((FULL_TILE, width), lambda step, _: (jnp.minimum(step, half - 1), 0))
        )
        half_out.append(
            pl.BlockSpec((FULL_TILE, width), lambda step, _: (jnp.maximum(step - half, 0), 0))
        )
    work = 2 * tokens * matrix.shape[0] * columns
    return pl.pallas_call(
        kernel,
        grid_spec=pltpu.PrefetchScalarGridSpec(
            num_scalar_prefetch=1,
            grid=(tiles,),
            in_specs=[row_spec(left.shape[1]) for left in lefts]
            + [pl.BlockSpec((matrix.shape[0], columns), lambda step, _: (0, at))]
            + [pl.BlockSpec(extra.shape, lambda step, _: (0, 0)) for extra in extras],
            out_specs=[row_spec(width) for width, _ in outs] + half_out,
        ),
        out_shape=[jax.ShapeDtypeStruct((tokens, width), kind) for width, kind in outs]
        + [
            jax.ShapeDtypeStruct((tokens // 2, width), kind)
            for width, kind in halves
            for _ in range(2)
        ],
        cost_estimate=pl.CostEstimate(flops=work, bytes_accessed=work // 250, transcendentals=0),
        name=name,
    )(scalars, *lefts, matrix, *extras)


def rows_times(left, right):
    return jnp.dot(left, right, preferred_element_type=jnp.float32)


def back_body(lefts, whole, extras, outs):
    start, value = 0, None
    for left in lefts:
        stop = start + left.shape[1]
        term = contract_cols(left[...], whole[:, start:stop])
        value = term if value is None else value + term
        start = stop
    return [value]


def adam_body(places, count, *refs):
    arrays = len({place[0] for place in places})
    grad_refs, refs = refs[:count], refs[count:]
    states, outs = refs[: 3 * arrays], refs[3 * arrays :]
    start = 0
    for array, plane in places:
        at = (Ellipsis,) if plane is None else (plane,)
        weight, mean, square = (states[3 * array + kind][at] for kind in range(3))
        stop = start + weight.shape[-1]
        grad = grad_refs[0][:, start:stop]
        for part in range(1, count):
            other = grad_refs[part][:, start:stop].astype(jnp.float32)
            grad = jnp.where(pl.program_id(0) == part, other, grad)
        step, mean_next, square_next = adam_step(
            weight, grad, mean, square, MATRIX_RATE, WEIGHT_DECAY
        )
        for kind, result in enumerate((grad, step, mean_next, square_next)):
            outs[4 * array + kind][at] = result
        start = stop


def adam_update(grads, places, states):
    parts = len(grads)
    rows, columns = grads[0].shape
    tile = min(128, rows)

    def window(array):
        lead = array.shape[:-2]
        shape = lead + (tile, array.shape[-1] // parts)
        return pl.BlockSpec(shape, lambda part, at: (0,) * len(lead) + (at, part))

    def grad_index(own, part, at):
        return (jnp.where(part == own, at, 0), 0)

    flat = [array for group in states for array in group]
    out_like = [group[0] for group in states for _ in range(4)]
    return pl.pallas_call(
        functools.partial(adam_body, places, parts),
        grid=(parts, rows // tile),
        in_specs=[
            pl.BlockSpec((tile, columns), functools.partial(grad_index, own))
            for own in range(parts)
        ]
        + [window(array) for array in flat],
        out_specs=[window(array) for array in out_like],
        out_shape=[jax.ShapeDtypeStruct(array.shape, jnp.float32) for array in out_like],
        cost_estimate=pl.CostEstimate(
            flops=20 * parts * rows * columns,
            bytes_accessed=32 * parts * rows * columns,
            transcendentals=0,
        ),
        name="adam_update",
    )(*grads, *flat)


class Hops:
    def __init__(self, shards):
        self.shards = shards
        place = place_of(lax.axis_index("fsdp"), shards)
        self.neighbours = [
            {"fsdp": ring_place(place + shards + step, shards)} for step in (1, -1)
        ]
        tensor = lax.axis_index("tensor")
        self.core = lax.rem(tensor, 2)
        chip = tensor // 2
        self.partner = {"tensor": 2 * chip + 1 - self.core}
        self.across = {"tensor": 2 * (1 - chip) + self.core}

    def meet(self, others):
        barrier = pltpu.get_barrier_semaphore()
        for other in others:
            pl.semaphore_signal(
                barrier, inc=1, device_id=other, device_id_type=pl.DeviceIdType.MESH
            )
        pl.semaphore_wait(barrier, len(others))


def remote(source, target, sent, arrived, device):
    return pltpu.make_async_remote_copy(
        src_ref=source,
        dst_ref=target,
        send_sem=sent,
        recv_sem=arrived,
        device_id=device,
        device_id_type=pl.DeviceIdType.MESH,
    )


HALVES = 2


def half_rows(ref, half):
    rows = ref.shape[0] // HALVES
    return ref.at[pl.ds(half * rows, rows)]


class RingGather:
    def __init__(self, hops, own, slots, sems, forward):
        legs = hops.shards // 2
        reach = (legs, legs - 1) if forward else (legs - 1, legs)
        self.reach = [reach if half % 2 == 0 else reach[::-1] for half in range(HALVES)]
        self.hops, self.own, self.slots, self.sems = hops, own, slots, sems

    def copy(self, way, step, half):
        shards = self.hops.shards
        source, target = (step - 1, step) if way == 0 else (shards - step + 1, shards - step)
        return remote(
            half_rows(self.own if step == 1 else self.slots.at[source], half),
            half_rows(self.slots.at[target], half),
            self.sems[0].at[way, step - 1, half],
            self.sems[1].at[way, step - 1, half],
            self.hops.neighbours[way],
        )

    def hop(self, step):
        for half in range(HALVES):
            for way in range(2):
                if 1 < step <= self.reach[half][way] + 1:
                    self.copy(way, step - 1, half).wait_recv()
                if step <= self.reach[half][way]:
                    self.copy(way, step, half).start()

    def close(self):
        for half in range(HALVES):
            for way in range(2):
                for step in range(1, self.reach[half][way] + 1):
                    self.copy(way, step, half).wait_send()


def by_rows(count, body):
    @pl.loop(0, count // ROW_STEP)
    def _(step):
        body(pl.ds(pl.multiple_of(step * ROW_STEP, ROW_STEP), ROW_STEP))


class RingScatter:
    SLOTS = 3

    def __init__(self, hops, partial, sent, came, sems, credits, jobs, plan):
        self.hops, self.partial, self.sent, self.came = hops, partial, sent, came
        self.sems, self.credits, self.jobs = sems, credits, jobs
        self.total = [sum(job[way] for job in jobs) for way in range(2)]
        self.number = [{}, {}]
        for job, step in plan:
            for way in range(2):
                if step <= jobs[job][way]:
                    self.number[way][job, step] = len(self.number[way])

    def copy(self, way, number, half):
        slot = number % self.SLOTS
        return remote(
            half_rows(self.sent.at[way, slot], half),
            half_rows(self.came.at[way, slot], half),
            self.sems[0].at[way, slot, half],
            self.sems[1].at[way, slot, half],
            self.hops.neighbours[way],
        )

    def add(self, way, job, hop, half, out):
        number = self.number[way][job, hop]
        self.copy(way, number, half).wait_recv()
        slot = number % self.SLOTS
        count = out.shape[0] // HALVES

        @pl.loop(0, count // ROW_STEP)
        def _(step):
            rows = pl.ds(pl.multiple_of(half * count + step * ROW_STEP, ROW_STEP), ROW_STEP)
            out[rows, :] = (
                out[rows, :].astype(jnp.float32) + self.came[way, slot, rows].astype(jnp.float32)
            ).astype(out.dtype)

        if number + self.SLOTS < self.total[way]:
            pl.semaphore_signal(
                self.credits.at[way, half],
                inc=1,
                device_id=self.hops.neighbours[1 - way],
                device_id_type=pl.DeviceIdType.MESH,
            )

    def prepare(self, job, hop):
        for way in range(2):
            distance = self.jobs[job][way] - hop + 1
            if distance < 1:
                continue
            number = self.number[way][job, hop]
            if number >= self.SLOTS:
                for half in range(HALVES):
                    self.copy(way, number - self.SLOTS, half).wait_send()
            self.partial(
                job,
                self.hops.shards - distance if way == 0 else distance,
                self.sent.at[way, number % self.SLOTS],
            )

    def hop(self, job, hop):
        for half in range(HALVES):
            for way in range(2):
                if hop > self.jobs[job][way]:
                    continue
                number = self.number[way][job, hop]
                if hop > 1:
                    self.add(way, job, hop - 1, half, self.sent.at[way, number % self.SLOTS])
                if number >= self.SLOTS:
                    pl.semaphore_wait(self.credits.at[way, half], 1)
                self.copy(way, number, half).start()

    def last(self, job, own):
        for half in range(HALVES):
            for way in range(2):
                self.add(way, job, self.jobs[job][way], half, own)

    def close(self):
        for way in range(2):
            for number in range(max(0, self.total[way] - self.SLOTS), self.total[way]):
                for half in range(HALVES):
                    self.copy(way, number, half).wait_send()


class CoreSum:
    def __init__(self, hops, sent, kept, first, chip, second, out, sems):
        self.hops, self.sent, self.kept, self.first = hops, sent, kept, first
        self.chip, self.second, self.out, self.sems = chip, second, out, sems
        self.half = chip.shape[0]

    def copy(self, stage):
        rows = self.out.at[pl.ds(pl.multiple_of(self.hops.core * self.half, 128), self.half)]
        source, target, device = (
            (self.sent, self.first, self.hops.partner),
            (self.chip, self.second, self.hops.across),
            (self.chip, rows, self.hops.partner),
        )[stage]
        return remote(source, target, self.sems.at[0, stage], self.sems.at[1, stage], device)

    def local(self):
        rows = self.out.at[pl.ds(pl.multiple_of(self.hops.core * self.half, 128), self.half)]
        return pltpu.make_async_copy(self.chip, rows, self.sems.at[0, 3])

    def add(self, left, right):
        def body(rows):
            self.chip[rows, :] = (
                left[rows, :].astype(jnp.float32) + right[rows, :].astype(jnp.float32)
            ).astype(jnp.bfloat16)

        by_rows(self.half, body)

    def start(self):
        self.copy(0).start()

    def to_chip(self):
        self.copy(0).wait_recv()
        self.add(self.kept, self.first)
        self.copy(1).start()

    def to_all(self):
        self.copy(1).wait()
        self.add(self.chip, self.second)
        self.copy(2).start()
        self.local().start()

    def done(self):
        self.copy(0).wait_send()
        self.copy(2).wait()
        self.local().wait()


RING_LIMIT = 66500000


FULL_TILE = 256


def gather_body(shards, gain_cols, query_cols, key_cols, *refs):
    (own_ref, small_ref, x_ref, g_ref, gate_up_ref, down_ref) = refs[:6]
    (cosine_ref, sine_ref, first_ref) = refs[6:9]
    (out_ref, few_ref, early_ref, ff_ref, xr_ref, gr_ref, n_ref) = refs[9:16]
    (query_raw, key_raw, query_ref, key_ref, value_ref, mixed_ref) = refs[16:22]
    (kept_ref, sent_ref) = refs[22:24]
    (few, gain, head_gain, whole) = refs[24:28]
    (big_sent, big_came, ff_sent, ff_came, few_sent, few_came, local) = refs[28:]
    hops = Hops(shards)
    place = place_of(lax.axis_index("fsdp"), shards)
    ahead = [{"fsdp": ring_place(place + at, shards)} for at in range(1, shards)]
    hops.meet(ahead)
    smalls = [
        remote(small_ref, few.at[at], few_sent.at[at - 1], few_came.at[at - 1], ahead[at - 1])
        for at in range(1, shards)
    ]
    for copy in smalls:
        copy.start()
    big = RingGather(hops, own_ref, out_ref, (big_sent, big_came), True)
    early = RingGather(hops, ff_ref.at[0], early_ref, (ff_sent, ff_came), True)
    big.hop(1)
    copies = [
        pltpu.make_async_copy(own_ref, out_ref.at[0], local.at[0]),
        pltpu.make_async_copy(small_ref, few.at[0], local.at[1]),
    ]
    for copy in copies:
        copy.start()
    for copy in copies:
        copy.wait()
    for copy in smalls:
        copy.wait_recv()
    put = pltpu.make_async_copy(few, few_ref, local.at[1])
    put.start()
    turn = [ring_place(place - at + shards, shards) for at in range(shards)]
    heads = jnp.zeros((few.shape[1], HEAD_SIZE), jnp.float32)
    for at in range(shards):
        gain[:, at * gain_cols : (at + 1) * gain_cols] = few[at, 0:1, :gain_cols].astype(
            jnp.float32
        )
        heads += pltpu.roll(
            few[at, :, gain_cols : gain_cols + HEAD_SIZE].astype(jnp.float32),
            turn[at] * (HEAD_SIZE // shards),
            1,
        )
    head_gain[...] = heads
    scalars = turn + [hops.core]
    tokens, width = x_ref.shape
    tiles = tokens // ROW_TILE
    legs = shards // 2

    def turned_part(part):
        def index(tile):
            return (tile + part * (tiles // legs), 0)

        pltpu.emit_pipeline(
            lambda *refs: turned_in(scalars, *refs[:2], gain, *refs[2:]),
            grid=(tiles // legs,),
            in_specs=[pl.BlockSpec((ROW_TILE, width), index)] * 2,
            out_specs=[pl.BlockSpec((ROW_TILE, width), index)] * 3,
        )(x_ref, g_ref, xr_ref, gr_ref, n_ref)

    def cast_part(part):
        rows, columns = ff_ref.shape[1], ff_ref.shape[2] // 3
        tile = rows // 2

        def body(gate_up, down, out):
            out[:, :columns] = gate_up[0].astype(out.dtype)
            out[:, columns : 2 * columns] = gate_up[1].astype(out.dtype)
            out[:, 2 * columns :] = down[...].astype(out.dtype)

        pltpu.emit_pipeline(
            body,
            grid=(rows // tile,),
            in_specs=[
                pl.BlockSpec((2, tile, columns), lambda at: (0, at, part)),
                pl.BlockSpec((tile, columns), lambda at: (at, part)),
            ],
            out_specs=[pl.BlockSpec((tile, 3 * columns), lambda at: (at, 0))],
        )(gate_up_ref, down_ref, ff_ref.at[part])

    for part in range(legs):
        if part < ff_ref.shape[0]:
            cast_part(part)
        if part == legs - 1:
            early.hop(1)
        turned_part(part)
        if part + 2 <= legs:
            big.hop(part + 2)
    big.hop(legs + 1)
    loads = [
        pltpu.make_async_copy(
            out_ref.at[at],
            whole.at[pl.ds(at * out_ref.shape[1], out_ref.shape[1])],
            local.at[2 + at],
        )
        for at in range(shards)
    ]
    for copy in loads:
        copy.start()
    for copy in loads:
        copy.wait()
    inward = query_cols + 2 * key_cols

    def project_part(part):
        def index(tile):
            return (tile + part * (tokens // FULL_TILE // 2), 0)

        def spec(array):
            return pl.BlockSpec((FULL_TILE, array.shape[1]), index)

        outs = [query_raw, key_raw, query_ref, key_ref, value_ref]
        lefts = [n_ref, cosine_ref, sine_ref]
        pltpu.emit_pipeline(
            lambda *refs: turn_body(
                query_cols, key_cols, refs[:3], whole.at[:, pl.ds(0, inward)], [head_gain], refs[3:]
            )
            and None,
            grid=(tokens // FULL_TILE // 2,),
            in_specs=[spec(left) for left in lefts],
            out_specs=[spec(out) for out in outs],
        )(*lefts, *outs)

    groups = key_cols // HEAD_SIZE

    def attention_part(group):
        def spec(array):
            return pl.BlockSpec((tokens, array.shape[1] // groups), lambda _: (0, group))

        arrays = [query_ref, key_ref, value_ref, mixed_ref]
        pltpu.emit_pipeline(
            lambda query, key, value, out: attention_body(query, key, value, first_ref, out),
            grid=(1,),
            in_specs=[spec(array) for array in arrays[:3]],
            out_specs=[spec(mixed_ref)],
        )(*arrays)

    half = tokens // 2

    def out_part(core, out):
        rows = mixed_ref.at[pl.ds(pl.multiple_of(core * half, half), half)]

        def body(left, value):
            value[...] = contract_cols(left[...], whole[:, inward:]).astype(value.dtype)

        pltpu.emit_pipeline(
            body,
            grid=(half // FULL_TILE,),
            in_specs=[pl.BlockSpec((FULL_TILE, query_cols), lambda tile: (tile, 0))],
            out_specs=[pl.BlockSpec((FULL_TILE, width), lambda tile: (tile, 0))],
        )(rows, out)

    project_part(0)
    early.hop(2)
    project_part(1)
    attention_part(0)
    early.hop(3)
    for group in range(1, groups):
        attention_part(group)
    early.hop(4)
    out_part(1 - hops.core, sent_ref)
    out_part(hops.core, kept_ref)
    early.hop(5)
    big.close()
    early.close()
    for copy in smalls:
        copy.wait_send()
    put.wait()


def cast_body(*refs):
    start = 0
    for ref in refs[:-1]:
        stop = start + ref.shape[1]
        refs[-1][:, start:stop] = ref[...].astype(refs[-1].dtype)
        start = stop


def side_by_side(arrays):
    rows = arrays[0].shape[0]
    columns = sum(array.shape[1] for array in arrays)
    tile = rows // 2
    return pl.pallas_call(
        cast_body,
        grid=(rows // tile,),
        in_specs=[pl.BlockSpec((tile, array.shape[1]), lambda at: (at, 0)) for array in arrays],
        out_specs=pl.BlockSpec((tile, columns), lambda at: (at, 0)),
        out_shape=jax.ShapeDtypeStruct((rows, columns), jnp.bfloat16),
        name="side_by_side",
    )(*arrays)


def gather_call(own, small, rows, grads, gate_up, down, cosine, sine, first, gain_cols, cuts):
    tokens, width = rows.shape
    shards = width // own.shape[0]
    legs = shards // 2
    query_cols, key_cols = cuts
    low = jnp.bfloat16
    chunk = (down.shape[0], 3 * down.shape[1] // FF_CHUNKS)
    anywhere = pl.BlockSpec(memory_space=pl.ANY)

    def like(columns, kind=low, count=tokens):
        return jax.ShapeDtypeStruct((count, columns), kind)

    return pl.pallas_call(
        functools.partial(gather_body, shards, gain_cols, query_cols, key_cols),
        in_specs=[anywhere] * 8 + [pl.BlockSpec(memory_space=pltpu.VMEM)],
        out_specs=[anywhere] * 15,
        out_shape=[
            jax.ShapeDtypeStruct((shards, *shape), low)
            for shape in (own.shape, small.shape, chunk)
        ]
        + [jax.ShapeDtypeStruct((FF_CHUNKS, *chunk), low)]
        + [like(width)] * 3
        + [like(query_cols, jnp.float32), like(key_cols, jnp.float32)]
        + [like(query_cols), like(key_cols), like(key_cols), like(query_cols)]
        + [like(width, low, tokens // 2)] * 2,
        scratch_shapes=[
            pltpu.VMEM((shards, *small.shape), small.dtype),
            pltpu.VMEM((1, width), jnp.float32),
            pltpu.VMEM((small.shape[0], HEAD_SIZE), jnp.float32),
            pltpu.VMEM((width, own.shape[1]), low),
        ]
        + [pltpu.SemaphoreType.DMA((2, legs, HALVES))] * 4
        + [
            pltpu.SemaphoreType.DMA((shards - 1,)),
            pltpu.SemaphoreType.DMA((shards - 1,)),
            pltpu.SemaphoreType.DMA((2 + shards,)),
        ],
        compiler_params=pltpu.CompilerParams(
            collective_id=0, has_side_effects=True, vmem_limit_bytes=56 * 1024 * 1024
        ),
        name="gather_ring",
    )(own, small, rows, grads, gate_up, down, cosine, sine, first)


FF_TILE = 256
ROW_STEP = 32


def ff_kernel(shards, parts, *refs):
    (sent_ref, kept_ref, x_ref, grad_ref, gain_ref, own_ref, early_ref) = refs[:7]
    (mid_ref, normsum_ref, downkept_ref, downsent_ref, grads_ref, late_ref, whole_ref) = refs[7:14]
    (acts, whole, pairs, norm_acc, r_sent, r_came, total, late) = refs[14:22]
    (out_half, kept_half, chip, first) = refs[22:26]
    seconds = refs[26:28]
    (x_tile, mid_tile) = refs[28:30]
    (ag_sent, ag_came, rs_sent, rs_came, credits, sums, local) = refs[30:]
    place = place_of(lax.axis_index("fsdp"), shards)
    hops = Hops(shards)
    hops.meet([*hops.neighbours, hops.partner, hops.across])
    core = hops.core
    tokens, wide = x_ref.shape
    half = tokens // 2
    columns = pairs.shape[2]
    width = wide // shards
    legs = shards // 2
    gathers = [
        RingGather(
            hops,
            own_ref.at[part],
            whole_ref.at[part - 1],
            (ag_sent.at[part - 1], ag_came.at[part - 1]),
            part % 2 == 0,
        )
        for part in range(1, parts)
    ]

    def chunk_block(part, at):
        if at == 0:
            return own_ref.at[part]
        return early_ref.at[at] if part == 0 else whole_ref.at[part - 1, at]

    def partial(job, at, out):
        @pl.loop(0, 3)
        def _(pair):
            left = acts[pair // 2, :, at * width : (at + 1) * width]
            right = pairs[3 * job + pair]
            out[:, pl.ds(pl.multiple_of(pair * columns, 128), columns)] = contract_rows(
                left, right
            ).astype(out.dtype)

    scatter = RingScatter(
        hops,
        partial,
        r_sent,
        r_came,
        (rs_sent, rs_came),
        credits,
        [(legs, legs - 1) if part % 2 == 0 else (legs - 1, legs) for part in range(parts - 1)],
        [(part, step) for part in range(parts - 1) for step in range(1, legs + 1)],
    )
    attention = CoreSum(
        hops, sent_ref, kept_half, first, chip, seconds[0], acts.at[0], sums.at[0]
    )
    attention.start()
    take_kept = pltpu.make_async_copy(kept_ref, kept_half, local.at[0])
    take_grad = pltpu.make_async_copy(grad_ref, acts.at[1], local.at[1])
    take_kept.start()
    take_grad.start()
    gathers[0].hop(1)
    take_kept.wait()
    attention.to_chip()
    gathers[0].hop(2)
    gathers[0].hop(3)
    gathers[0].hop(4)
    gathers[1].hop(1)
    attention.to_all()
    attention.done()

    @pl.loop(0, tokens // FF_TILE)
    def _(tile):
        rows = pl.ds(pl.multiple_of(tile * FF_TILE, FF_TILE), FF_TILE)
        take = pltpu.make_async_copy(x_ref.at[rows], x_tile, local.at[2])
        take.start()
        take.wait()
        middle = x_tile[...].astype(jnp.float32) + acts[0, rows, :].astype(jnp.float32)
        mid_tile[...] = middle.astype(mid_tile.dtype)
        put = pltpu.make_async_copy(mid_tile, mid_ref.at[rows], local.at[2])
        put.start()
        acts[0, rows, :] = (middle * row_scale(middle) * gain_ref[...]).astype(jnp.bfloat16)
        put.wait()

    take_grad.wait()

    def load(part):
        copies = [
            pltpu.make_async_copy(
                chunk_block(part, at), whole.at[pl.ds(at * width, width)], local.at[3 + at]
            )
            for at in range(shards)
        ]
        for copy in copies:
            copy.start()
        for copy in copies:
            copy.wait()

    def tiles(part, start, stop):
        @pl.loop(start, stop)
        def _(tile):
            rows = pl.ds(pl.multiple_of(tile * FF_TILE, FF_TILE), FF_TILE)
            norm = acts[0, rows, :]
            grad = acts[1, rows, :]
            gate_proj = rows_times(norm, whole[:, :columns])
            up_proj = rows_times(norm, whole[:, columns : 2 * columns])
            hidden_grad = rows_times(grad, whole[:, 2 * columns :])
            gate = 1.0 / (1.0 + jnp.exp(-gate_proj))
            swish = gate_proj * gate
            gate_grad = (
                hidden_grad * up_proj * (gate * (1.0 + gate_proj * (1.0 - gate)))
            ).astype(jnp.bfloat16)
            up_grad = (hidden_grad * swish).astype(jnp.bfloat16)
            pairs[3 * part, rows, :] = gate_grad
            pairs[3 * part + 1, rows, :] = up_grad
            pairs[3 * part + 2, rows, :] = (swish * up_proj).astype(jnp.bfloat16)
            value = contract_cols(gate_grad, whole[:, :columns]) + contract_cols(
                up_grad, whole[:, columns : 2 * columns]
            )
            if part > 0:
                value += norm_acc[rows, :]
            norm_acc[rows, :] = value

    count = tokens // FF_TILE
    mine = pl.ds(pl.multiple_of(core * half, 128), half)
    other = pl.ds(pl.multiple_of((1 - core) * half, 128), half)
    norm_sum = CoreSum(
        hops, out_half, norm_acc.at[mine], first, chip, seconds[1], normsum_ref, sums.at[1]
    )
    puts = [
        pltpu.make_async_copy(total, grads_ref.at[part], local.at[2]) for part in range(parts - 1)
    ]

    def own_block(part):
        if part > 0:
            puts[part - 1].wait()
        partial(part, 0, total)

    def finish(part):
        scatter.last(part, total)
        puts[part].start()

    lates = [
        pltpu.make_async_copy(
            late.at[at % 2],
            late_ref.at[ring_place(place - at + shards, shards)],
            local.at[3 + shards + at % 2],
        )
        for at in range(shards)
    ]

    def leave(at):
        if at > 1:
            lates[at - 2].wait()
        partial(parts - 1, at, late.at[at % 2])
        lates[at].start()

    load(0)
    tiles(0, 0, 2)
    gathers[0].hop(5)
    tiles(0, 2, count)
    gathers[1].hop(2)
    load(1)
    tiles(1, 0, 2)
    gathers[1].hop(3)
    tiles(1, 2, count)
    scatter.prepare(0, 1)
    gathers[1].hop(4)
    scatter.hop(0, 1)
    scatter.prepare(0, 2)
    gathers[1].hop(5)
    load(2)
    tiles(2, 0, 2)
    scatter.hop(0, 2)
    scatter.prepare(0, 3)
    tiles(2, 2, count)

    def cast_half(rows):
        out_half[rows, :] = norm_acc[
            pl.ds(pl.multiple_of((1 - core) * half + rows.start, ROW_STEP), ROW_STEP), :
        ].astype(jnp.bfloat16)

    by_rows(half, cast_half)
    norm_sum.start()
    scatter.hop(0, 3)
    scatter.prepare(0, 4)
    norm_sum.to_chip()
    scatter.prepare(1, 1)
    leave(0)
    scatter.hop(0, 4)
    scatter.hop(1, 1)
    own_block(0)
    scatter.prepare(1, 2)
    leave(1)
    finish(0)
    scatter.hop(1, 2)
    scatter.prepare(1, 3)
    leave(2)
    leave(3)
    for part in range(parts):
        copies = [
            pltpu.make_async_copy(
                chunk_block(part, at).at[:, pl.ds(2 * columns, columns)],
                whole.at[pl.ds(at * width, width), pl.ds(part * columns, columns)],
                local.at[3 + at],
            )
            for at in range(shards)
        ]
        for copy in copies:
            copy.start()
        for copy in copies:
            copy.wait()
    def down_tile(tile, offset):
        rows = pl.ds(pl.multiple_of(offset + tile * FF_TILE, FF_TILE), FF_TILE)
        value = contract_cols(pairs[2, rows, :], whole[:, :columns])
        for part in range(1, parts):
            value += contract_cols(
                pairs[3 * part + 2, rows, :], whole[:, part * columns : (part + 1) * columns]
            )
        return value.astype(jnp.bfloat16)

    scatter.hop(1, 3)
    scatter.prepare(1, 4)
    leave(4)

    @pl.loop(0, half // FF_TILE)
    def _(tile):
        rows = pl.ds(pl.multiple_of(tile * FF_TILE, FF_TILE), FF_TILE)
        kept_half[rows, :] = down_tile(tile, core * half)

    put_kept = pltpu.make_async_copy(kept_half, downkept_ref, local.at[0])
    put_kept.start()
    scatter.hop(1, 4)
    norm_sum.to_all()
    own_block(1)
    leave(5)
    finish(1)
    norm_sum.done()

    @pl.loop(0, half // FF_TILE)
    def _(tile):
        rows = pl.ds(pl.multiple_of(tile * FF_TILE, FF_TILE), FF_TILE)
        out_half[rows, :] = down_tile(tile, (1 - core) * half)

    put_sent = pltpu.make_async_copy(out_half, downsent_ref, local.at[1])
    put_sent.start()
    for at in range(6, shards):
        leave(at)
    put_kept.wait()
    put_sent.wait()
    puts[parts - 2].wait()
    for copy in lates[-2:]:
        copy.wait()
    for gather in gathers:
        gather.close()
    scatter.close()


def ff_call(sent, kept, rows, grad, gain, own, early):
    parts, width, columns3 = own.shape
    tokens, wide = rows.shape
    shards = wide // width
    columns = columns3 // 3
    half = tokens // 2
    legs = shards // 2
    low = jnp.bfloat16
    anywhere = pl.BlockSpec(memory_space=pl.ANY)
    slots = RingScatter.SLOTS
    return pl.pallas_call(
        functools.partial(ff_kernel, shards, parts),
        in_specs=[anywhere] * 4 + [pl.BlockSpec(memory_space=pltpu.VMEM)] + [anywhere] * 2,
        out_specs=[anywhere] * 7,
        out_shape=[
            jax.ShapeDtypeStruct((tokens, wide), low),
            jax.ShapeDtypeStruct((tokens, wide), low),
            jax.ShapeDtypeStruct((half, wide), low),
            jax.ShapeDtypeStruct((half, wide), low),
            jax.ShapeDtypeStruct((parts - 1, width, columns3), jnp.float32),
            jax.ShapeDtypeStruct((shards, width, columns3), low),
            jax.ShapeDtypeStruct((parts - 1, shards, width, columns3), low),
        ],
        scratch_shapes=[
            pltpu.VMEM((2, tokens, wide), low),
            pltpu.VMEM((wide, columns3), low),
            pltpu.VMEM((3 * parts, tokens, columns), low),
            pltpu.VMEM((tokens, wide), jnp.float32),
            pltpu.VMEM((2, slots, width, columns3), low),
            pltpu.VMEM((2, slots, width, columns3), low),
            pltpu.VMEM((width, columns3), jnp.float32),
            pltpu.VMEM((2, width, columns3), low),
        ]
        + [pltpu.VMEM((half, wide), low)] * 6
        + [
            pltpu.VMEM((FF_TILE, wide), low),
            pltpu.VMEM((FF_TILE, wide), low),
            pltpu.SemaphoreType.DMA((parts - 1, 2, legs, HALVES)),
            pltpu.SemaphoreType.DMA((parts - 1, 2, legs, HALVES)),
            pltpu.SemaphoreType.DMA((2, slots, HALVES)),
            pltpu.SemaphoreType.DMA((2, slots, HALVES)),
            pltpu.SemaphoreType.REGULAR((2, HALVES)),
            pltpu.SemaphoreType.DMA((2, 2, 4)),
            pltpu.SemaphoreType.DMA((5 + shards,)),
        ],
        compiler_params=pltpu.CompilerParams(
            collective_id=1, has_side_effects=True, vmem_limit_bytes=RING_LIMIT
        ),
        name="ff_ring",
    )(sent, kept, rows, grad, gain, own, early)


def tail_kernel(shards, jobs, *refs):
    (sent_ref, kept_ref, norm_ref, grad_ref, downsent_ref, downkept_ref) = refs[:6]
    rights = refs[6:10]
    (sum_ref, downsum_ref, grads_ref, acts, r_sent, r_came, total) = refs[10:17]
    (kept_half, chip, first, second) = refs[17:21]
    (down_half, down_chip, down_first, down_second) = refs[21:25]
    (rs_sent, rs_came, credits, sums, local) = refs[25:]
    hops = Hops(shards)
    hops.meet([*hops.neighbours, hops.partner, hops.across])
    wide = norm_ref.shape[1]
    width = wide // shards
    legs = shards // 2

    def partial(job, at, out):
        start = 0
        for left, right in jobs[job]:
            stop = start + rights[right].shape[1]
            out[:, start:stop] = contract_rows(
                acts[left, :, at * width : (at + 1) * width], rights[right][...]
            ).astype(out.dtype)
            start = stop

    scatter = RingScatter(
        hops,
        partial,
        r_sent,
        r_came,
        (rs_sent, rs_came),
        credits,
        [(legs, legs - 1) if job % 2 == 0 else (legs - 1, legs) for job in range(len(jobs))],
        [(job, step) for step in range(1, legs + 1) for job in range(len(jobs))],
    )
    take = [
        pltpu.make_async_copy(ref, target, local.at[at])
        for at, (ref, target) in enumerate(
            [
                (kept_ref, kept_half),
                (norm_ref, acts.at[0]),
                (grad_ref, acts.at[1]),
                (downkept_ref, down_half),
            ]
        )
    ]
    norm_sum = CoreSum(
        hops, sent_ref, kept_half, first, chip, second, sum_ref, sums.at[0]
    )
    puts = [pltpu.make_async_copy(total, grads_ref.at[job], local.at[0]) for job in range(2)]
    down_sum = CoreSum(
        hops, downsent_ref, down_half, down_first, down_chip, down_second, downsum_ref, sums.at[1]
    )
    norm_sum.start()
    down_sum.start()
    for copy in take:
        copy.start()
    for copy in take:
        copy.wait()
    scatter.prepare(0, 1)
    scatter.hop(0, 1)
    scatter.prepare(1, 1)
    scatter.hop(1, 1)
    norm_sum.to_chip()
    down_sum.to_chip()
    for step in range(2, legs + 1):
        for job in range(2):
            scatter.prepare(job, step)
            scatter.hop(job, step)
    norm_sum.to_all()
    for job in range(2):
        if job > 0:
            puts[job - 1].wait()
        partial(job, 0, total)
        scatter.last(job, total)
        puts[job].start()
    norm_sum.done()
    down_sum.to_all()
    down_sum.done()
    puts[1].wait()
    scatter.close()


def tail_call(sent, kept, norm, grad, down_sent, down_kept, rights, jobs, shards):
    tokens, wide = norm.shape
    half, width, legs = tokens // 2, wide // shards, shards // 2
    columns = sum(rights[right].shape[1] for _, right in jobs[0])
    low = jnp.bfloat16
    anywhere = pl.BlockSpec(memory_space=pl.ANY)
    slots = RingScatter.SLOTS
    return pl.pallas_call(
        functools.partial(tail_kernel, shards, jobs),
        in_specs=[anywhere] * 6 + [pl.BlockSpec(memory_space=pltpu.VMEM)] * len(rights),
        out_specs=[anywhere] * 3,
        out_shape=[
            jax.ShapeDtypeStruct((tokens, wide), low),
            jax.ShapeDtypeStruct((tokens, wide), low),
            jax.ShapeDtypeStruct((len(jobs), width, columns), jnp.float32),
        ],
        scratch_shapes=[
            pltpu.VMEM((2, tokens, wide), low),
            pltpu.VMEM((2, slots, width, columns), low),
            pltpu.VMEM((2, slots, width, columns), low),
            pltpu.VMEM((width, columns), jnp.float32),
        ]
        + [pltpu.VMEM((half, wide), low)] * 8
        + [
            pltpu.SemaphoreType.DMA((2, slots, HALVES)),
            pltpu.SemaphoreType.DMA((2, slots, HALVES)),
            pltpu.SemaphoreType.REGULAR((2, HALVES)),
            pltpu.SemaphoreType.DMA((2, 2, 4)),
            pltpu.SemaphoreType.DMA((4,)),
        ],
        compiler_params=pltpu.CompilerParams(
            collective_id=2, has_side_effects=True, vmem_limit_bytes=48 * 1024 * 1024
        ),
        name="tail_ring",
    )(sent, kept, norm, grad, down_sent, down_kept, *rights)


ATTENTION_ROWS = 256


def head_turn(raw, cosine, sine, gain):
    scaled = raw * row_scale(raw) * gain
    return scaled * cosine + pltpu.roll(scaled, HEAD_SIZE // 2, 1) * sine


def head_back(grad, raw, cosine, sine, gain):
    turned = grad * cosine - pltpu.roll(grad, HEAD_SIZE // 2, 1) * sine
    scale = row_scale(raw)
    unit = raw * scale
    inner = turned * gain
    raw_grad = scale * (inner - unit * jnp.mean(inner * unit, axis=-1, keepdims=True))
    return raw_grad, jnp.sum(turned * unit, axis=0, keepdims=True)


def turn_body(query_cols, key_cols, lefts, whole, extras, outs):
    normed, cosine_ref, sine_ref = lefts
    query_raw, key_raw, query_out, key_out, value_out = outs
    cosine, sine = cosine_ref[...], sine_ref[...]
    raw = rows_times(normed[...], whole[:, : query_cols + key_cols])
    query_raw[...] = raw[:, :query_cols]
    key_raw[...] = raw[:, query_cols:]
    value_out[...] = rows_times(normed[...], whole[:, query_cols + key_cols :]).astype(
        value_out.dtype
    )
    for out, base, gain in ((query_out, 0, 0), (key_out, query_cols, 1)):
        for start in range(0, out.shape[1], HEAD_SIZE):
            out[:, start : start + HEAD_SIZE] = head_turn(
                raw[:, base + start : base + start + HEAD_SIZE],
                cosine,
                sine,
                extras[0][gain : gain + 1, :],
            ).astype(out.dtype)
    return []


def attention_probs(query, keys, first_ref, row_start):
    rows, stop = query.shape[0], keys.shape[0]
    scores = contract_cols(query, keys) * (1.0 / math.sqrt(HEAD_SIZE))
    column = lax.broadcasted_iota(jnp.int32, (rows, stop), 1)
    row = lax.broadcasted_iota(jnp.int32, (rows, stop), 0) + row_start
    first = first_ref[row_start : row_start + rows, :]
    scores = jnp.where((column <= row) & (column >= first), scores, MASKED)
    exponent = jnp.exp(scores - jnp.max(scores, axis=-1, keepdims=True))
    return exponent * (1.0 / jnp.sum(exponent, axis=-1, keepdims=True))


def attention_body(query_ref, key_ref, value_ref, first_ref, out_ref):
    low = out_ref.dtype
    for start in range(0, query_ref.shape[1], HEAD_SIZE):
        head = slice(start, start + HEAD_SIZE)
        for row in range(0, query_ref.shape[0], ATTENTION_ROWS):
            rows, stop = slice(row, row + ATTENTION_ROWS), row + ATTENTION_ROWS
            probs = attention_probs(query_ref[rows, head], key_ref[:stop, :], first_ref, row)
            out_ref[rows, head] = rows_times(probs.astype(low), value_ref[:stop, :]).astype(low)


def attention_back_body(
    query_ref,
    key_ref,
    value_ref,
    grad_ref,
    query_raw,
    key_raw,
    cosine_ref,
    sine_ref,
    gain_ref,
    first_ref,
    query_out,
    key_out,
    value_out,
    sums_ref,
    key_acc,
    value_acc,
):
    low = query_out.dtype
    scale = 1.0 / math.sqrt(HEAD_SIZE)
    key_acc[...] = jnp.zeros_like(key_acc)
    value_acc[...] = jnp.zeros_like(value_acc)
    query_sum = jnp.zeros((1, HEAD_SIZE), jnp.float32)
    for start in range(0, query_ref.shape[1], HEAD_SIZE):
        head = slice(start, start + HEAD_SIZE)
        for row in range(0, query_ref.shape[0], ATTENTION_ROWS):
            rows, stop = slice(row, row + ATTENTION_ROWS), row + ATTENTION_ROWS
            query, grad = query_ref[rows, head], grad_ref[rows, head]
            probs = attention_probs(query, key_ref[:stop, :], first_ref, row)
            prob_grad = contract_cols(grad, value_ref[:stop, :])
            inner = jnp.sum(probs * prob_grad, axis=-1, keepdims=True)
            score_grad = (probs * (prob_grad - inner)).astype(low)
            key_acc[:stop, :] += contract_rows(score_grad, query)
            value_acc[:stop, :] += contract_rows(probs.astype(low), grad)
            query_grad = (rows_times(score_grad, key_ref[:stop, :]) * scale).astype(low)
            raw_grad, gain_grad = head_back(
                query_grad.astype(jnp.float32),
                query_raw[rows, head],
                cosine_ref[rows, :],
                sine_ref[rows, :],
                gain_ref[0:1, :],
            )
            query_out[rows, head] = raw_grad.astype(low)
            query_sum += gain_grad
    key_sum = jnp.zeros((1, HEAD_SIZE), jnp.float32)
    for row in range(0, key_ref.shape[0], ATTENTION_ROWS):
        rows = slice(row, row + ATTENTION_ROWS)
        key_grad = (key_acc[rows, :] * scale).astype(low)
        raw_grad, gain_grad = head_back(
            key_grad.astype(jnp.float32),
            key_raw[rows, :],
            cosine_ref[rows, :],
            sine_ref[rows, :],
            gain_ref[1:2, :],
        )
        key_out[rows, :] = raw_grad.astype(low)
        key_sum += gain_grad
    value_out[...] = value_acc[...].astype(low)
    sums_ref[0:1, :] = query_sum
    sums_ref[1:2, :] = key_sum


def by_group(body, arrays, outs, groups, name, scratch=(), whole=()):
    tokens = arrays[0].shape[0]

    def columns(width):
        return pl.BlockSpec((tokens, width // groups), lambda group: (0, group))

    pair = tokens * tokens * arrays[0].shape[1]
    return pl.pallas_call(
        body,
        grid=(groups,),
        in_specs=[columns(array.shape[1]) for array in arrays]
        + [pl.BlockSpec(array.shape, lambda group: (0, 0)) for array in whole],
        out_specs=[
            columns(out.shape[1])
            if len(out.shape) == 2
            else pl.BlockSpec((None, *out.shape[1:]), lambda group: (group, 0, 0))
            for out in outs
        ],
        out_shape=list(outs),
        scratch_shapes=list(scratch),
        cost_estimate=pl.CostEstimate(
            flops=4 * pair, bytes_accessed=tokens * 4096, transcendentals=pair // 128
        ),
        name=name,
    )(*arrays, *whole)


def gains_body(shards, pieces, out_ref, came, total, late, sums):
    hops = Hops(shards)
    place = place_of(lax.axis_index("fsdp"), shards)
    peers = [{"fsdp": ring_place(place - at + shards, shards)} for at in range(1, shards)]
    hops.meet([*peers, hops.partner, hops.across])
    copies = [
        remote(
            pieces.at[at], came.at[at - 1], sums.at[0, at - 1], sums.at[1, at - 1], peers[at - 1]
        )
        for at in range(1, shards)
    ]
    for copy in copies:
        copy.start()
    value = pieces[0]
    for at in range(1, shards):
        copies[at - 1].wait_recv()
        value += came[at - 1]
    for stage, peer in enumerate((hops.partner, hops.across)):
        total[stage] = value
        copy = remote(
            total.at[stage],
            late.at[stage],
            sums.at[0, shards - 1 + stage],
            sums.at[1, shards - 1 + stage],
            peer,
        )
        copy.start()
        copy.wait()
        value += late[stage]
    own = lax.broadcasted_iota(jnp.int32, value.shape, 1) < value.shape[1] - HEAD_SIZE
    out_ref[...] = jnp.where(own, total[0], value)
    for copy in copies:
        copy.wait_send()


def gains_call(pieces):
    shards, rows, columns = pieces.shape
    return pl.pallas_call(
        functools.partial(gains_body, shards),
        in_specs=[pl.BlockSpec(memory_space=pltpu.VMEM)],
        out_specs=pl.BlockSpec(memory_space=pltpu.VMEM),
        out_shape=jax.ShapeDtypeStruct((rows, columns), pieces.dtype),
        scratch_shapes=[
            pltpu.VMEM((shards - 1, rows, columns), pieces.dtype),
            pltpu.VMEM((2, rows, columns), pieces.dtype),
            pltpu.VMEM((2, rows, columns), pieces.dtype),
            pltpu.SemaphoreType.DMA((2, shards + 1)),
        ],
        compiler_params=pltpu.CompilerParams(collective_id=3, has_side_effects=True),
        name="gain_sums",
    )(pieces)


def ring_device(
    shards,
    layer_input,
    out_grad,
    segment_ids,
    query_weight,
    key_weight,
    value_matrix,
    output_weight,
    gate_up_weight,
    down_weight,
    norm_gains,
    headnorm_gains,
    query_weight_mean,
    key_weight_first_moment,
    value_weight_first_moment,
    output_weight_mean,
    gate_up_weight_mean,
    down_weight_mean,
    norm_gains_mean,
    headnorm_gains_mean,
    query_weight_square,
    key_weight_second_moment,
    value_weight_second_moment,
    output_weight_square,
    gate_up_weight_square,
    down_weight_square,
    norm_gains_square,
    headnorm_gains_square,
):
    place = place_of(lax.axis_index("fsdp"), shards)
    core = lax.axis_index("tensor") % 2
    turn = jnp.stack([ring_place(place - at + shards, shards) for at in range(shards)])
    turn = turn.astype(jnp.int32)
    scalars = jnp.concatenate([turn, core[None].astype(jnp.int32)])
    back = (place - place_of(jnp.arange(shards), shards)) % shards

    gain_cols, head_cols = norm_gains.shape[1], headnorm_gains.shape[1]
    low = jnp.bfloat16
    packed_token_count, width = layer_input.shape
    query_cols, key_cols = query_weight.shape[1], key_weight.shape[1]
    local_groups = key_cols // HEAD_SIZE
    states = [
        (query_weight, query_weight_mean, query_weight_square),
        (key_weight, key_weight_first_moment, key_weight_second_moment),
        (value_matrix, value_weight_first_moment, value_weight_second_moment),
        (output_weight, output_weight_mean, output_weight_square),
        (gate_up_weight, gate_up_weight_mean, gate_up_weight_square),
        (down_weight, down_weight_mean, down_weight_square),
        (norm_gains, norm_gains_mean, norm_gains_square),
        (headnorm_gains, headnorm_gains_mean, headnorm_gains_square),
    ]

    attention_block = side_by_side([query_weight, key_weight, value_matrix, output_weight])
    own_gains = jnp.concatenate([norm_gains, headnorm_gains], axis=1).astype(low)
    own_gains = jnp.pad(own_gains, ((0, 14), (0, -own_gains.shape[1] % 128)))
    inward_window = (query_cols + 2 * key_cols, 0)
    outward_window = (query_cols, (query_cols + 2 * key_cols) // query_cols)
    token_positions = positions_of(segment_ids)
    first_key = (jnp.arange(packed_token_count, dtype=jnp.int32) - token_positions)[:, None]
    frequencies = ROPE_BASE ** (
        -2.0 * jnp.arange(HEAD_SIZE // 2).astype(jnp.float32) / HEAD_SIZE
    )
    angles = token_positions.astype(jnp.float32)[:, None] * frequencies[None, :]
    cosine = jnp.tile(jnp.cos(angles), (1, 2))
    sine = jnp.sin(angles)
    sine = jnp.concatenate([-sine, sine], axis=1)

    (
        attention_full,
        gains,
        ff_early,
        ff_block,
        input_rows,
        grad_low,
        normed_one,
        query_raw,
        key_raw,
        query_heads,
        key_heads,
        value_heads,
        mixed,
        kept,
        sent,
    ) = gather_call(
        attention_block,
        own_gains,
        layer_input,
        out_grad,
        gate_up_weight,
        down_weight,
        cosine,
        sine,
        first_key,
        gain_cols,
        (query_cols, key_cols),
    )
    attention_full = attention_full.reshape(width, -1)
    gains = jnp.swapaxes(gains[:, :2].astype(jnp.float32), 0, 1)
    norm_gain = gains[:, :, :gain_cols].reshape(2, 1, -1)
    head_gain = gains[:, :, gain_cols : gain_cols + head_cols][:, back].reshape(2, -1)
    middle, norm_sum, down_kept, down_sent, ff_sums, ff_late, _ = ff_call(
        sent, kept, input_rows, grad_low, norm_gain[1], ff_block, ff_early
    )
    ff_last = lax.psum_scatter(ff_late, "fsdp", scatter_dimension=0, tiled=False)
    middle_grad_low, mixed_grad, gain_two_grad = row_call(
        second_back,
        scalars,
        [middle, grad_low, norm_sum],
        [norm_gain[1]],
        [low],
        sums=1,
        matrix=attention_full,
        columns=outward_window[0],
        at=outward_window[1],
    )
    query_proj_low, key_proj_low, value_grad_low, head_sums = by_group(
        attention_back_body,
        [query_heads, key_heads, value_heads, mixed_grad, query_raw, key_raw],
        [
            jax.ShapeDtypeStruct(query_heads.shape, low),
            jax.ShapeDtypeStruct(key_heads.shape, low),
            jax.ShapeDtypeStruct(key_heads.shape, low),
            jax.ShapeDtypeStruct((local_groups, 2, HEAD_SIZE), jnp.float32),
        ],
        local_groups,
        "attention_back",
        scratch=[pltpu.VMEM((packed_token_count, HEAD_SIZE), jnp.float32)] * 2,
        whole=[cosine, sine, head_gain, first_key],
    )
    kept, sent = full_call(
        back_body,
        scalars,
        [query_proj_low, key_proj_low, value_grad_low],
        attention_full,
        inward_window,
        [],
        [(width, low)],
        "projection_back",
    )
    norm_one_sum, down_sum, attention_sums = tail_call(
        sent,
        kept,
        normed_one,
        middle_grad_low,
        down_sent,
        down_kept,
        [query_proj_low, key_proj_low, value_grad_low, mixed],
        (((0, 0), (0, 1)), ((0, 2), (1, 3))),
        shards,
    )
    (layer_output,) = row_call(layer_out, scalars, [middle, down_sum], [], [jnp.float32])
    input_grad, gain_one_grad = row_call(
        first_back,
        scalars,
        [middle_grad_low, input_rows, norm_one_sum],
        [norm_gain[0]],
        [jnp.float32],
        sums=1,
    )
    head_grads = jnp.sum(head_sums, axis=0).reshape(2, shards, head_cols)[:, turn]
    pieces = jnp.concatenate(
        [
            jnp.sum(gain_one_grad, axis=0).reshape(shards, 1, gain_cols),
            jnp.sum(gain_two_grad, axis=0).reshape(shards, 1, gain_cols),
            jnp.pad(
                jnp.swapaxes(head_grads, 0, 1).reshape(shards, 1, 2 * head_cols),
                ((0, 0), (0, 0), (0, HEAD_SIZE - 2 * head_cols)),
            ),
        ],
        axis=2,
    )
    gain_sums = gains_call(pieces)
    ff_updates = adam_update(
        [ff_sums[0], ff_sums[1], ff_last], [(0, 0), (0, 1), (1, None)], states[4:6]
    )
    inner_updates = adam_update([attention_sums[0]], [(0, None), (1, None)], states[0:2])
    outer_updates = adam_update([attention_sums[1]], [(0, None), (1, None)], states[2:4])
    gain_shards = [
        gain_sums[:, : 2 * gain_cols].reshape(2, gain_cols),
        gain_sums[:, 2 * gain_cols : 2 * gain_cols + 2 * head_cols].reshape(2, head_cols),
    ]
    updates = [inner_updates[:4], inner_updates[4:], outer_updates[:4], outer_updates[4:]]
    updates += [ff_updates[:4], ff_updates[4:]]
    for (weight, mean, square), grad in zip(states[6:], gain_shards):
        updates.append([grad, *adam_step(weight, grad, mean, square, GAIN_RATE, 0.0)])
    return tuple([layer_output, input_grad] + [update[kind] for kind in range(4) for update in updates])


def solution(mesh):
    shards, parts = mesh.shape["fsdp"], mesh.shape["tensor"]
    ringed = parts == 4 and shards == 8
    return jax.shard_map(
        functools.partial(ring_device, shards) if ringed else plain_device,
        mesh=mesh,
        in_specs=(
            P("fsdp", None),
            P("fsdp", None),
            P("fsdp"),
            P("fsdp", "tensor"),
            P("fsdp", "tensor"),
            P("fsdp", "tensor"),
            P("fsdp", "tensor"),
            P(None, "fsdp", "tensor"),
            P("fsdp", "tensor"),
            P(None, "fsdp"),
            P(None, "fsdp"),
            P("fsdp", "tensor"),
            P("fsdp", "tensor"),
            P("fsdp", "tensor"),
            P("fsdp", "tensor"),
            P(None, "fsdp", "tensor"),
            P("fsdp", "tensor"),
            P(None, "fsdp"),
            P(None, "fsdp"),
            P("fsdp", "tensor"),
            P("fsdp", "tensor"),
            P("fsdp", "tensor"),
            P("fsdp", "tensor"),
            P(None, "fsdp", "tensor"),
            P("fsdp", "tensor"),
            P(None, "fsdp"),
            P(None, "fsdp"),
        ),
        out_specs=(
            P("fsdp", None),
            P("fsdp", None),
            P("fsdp", "tensor"),
            P("fsdp", "tensor"),
            P("fsdp", "tensor"),
            P("fsdp", "tensor"),
            P(None, "fsdp", "tensor"),
            P("fsdp", "tensor"),
            P(None, "fsdp"),
            P(None, "fsdp"),
            P("fsdp", "tensor"),
            P("fsdp", "tensor"),
            P("fsdp", "tensor"),
            P("fsdp", "tensor"),
            P(None, "fsdp", "tensor"),
            P("fsdp", "tensor"),
            P(None, "fsdp"),
            P(None, "fsdp"),
            P("fsdp", "tensor"),
            P("fsdp", "tensor"),
            P("fsdp", "tensor"),
            P("fsdp", "tensor"),
            P(None, "fsdp", "tensor"),
            P("fsdp", "tensor"),
            P(None, "fsdp"),
            P(None, "fsdp"),
            P("fsdp", "tensor"),
            P("fsdp", "tensor"),
            P("fsdp", "tensor"),
            P("fsdp", "tensor"),
            P(None, "fsdp", "tensor"),
            P("fsdp", "tensor"),
            P(None, "fsdp"),
            P(None, "fsdp"),
        ),
        check_vma=False,
    )
```
